16 devices in a mesh: dp: 4 (over z, y), kv: 4 (over x, core).
Axes of the slice: x: 2, y: 2, z: 2, core: 2. Of those that a mesh axis runs over, the one named last changes fastest.
Arguments:
- x_in: bfloat16 [1024, 640], P('dp'), parts along dimension 0
- positions: int32 [1024], P('dp'), parts along dimension 0
- k_cache: bfloat16 [1024, 512, 256], P('dp', 'kv'), parts along dimension 0
- v_cache: bfloat16 [1024, 512, 256], P('dp', 'kv'), parts along dimension 0
- slot_pos: int32 [1024, 512], P('dp', 'kv'), parts along dimension 0
- norm_scale: bfloat16 [640], replicated
- w_q: bfloat16 [640, 1024], replicated
- w_k: bfloat16 [640, 256], replicated
- w_v: bfloat16 [640, 256], replicated
- w_o: bfloat16 [1024, 640], replicated
- b_o: bfloat16 [640], replicated
Outputs:
- output 1: bfloat16 [1024, 640], P('dp'), parts along dimension 0
- output 2: bfloat16 [1024, 512, 256], P('dp', 'kv'), parts along dimension 0
- output 3: bfloat16 [1024, 512, 256], P('dp', 'kv'), parts along dimension 0
- output 4: int32 [1024, 512], P('dp', 'kv'), parts along dimension 0
There are 4 independent parts. The reference program is written for one: setup_inputs(seed, part) draws one part's arguments, and reference() takes and returns one part's arrays. A program takes and returns all parts, laid end to end along the dimension named above; an argument that names none is the same for every part.
All inputs are finite; a program needn't handle non-finite values.
Results may differ from the reference program's by a relative error of at most 0.00593895.
Values sent between devices are 32-bit elements.
A program may use at most 1 GiB of HBM per device.

```python
import math
import jax
import jax.numpy as jnp
from jax import lax

BATCH = 256
D_MODEL = 640
HEADS = 4
WINDOW = 512
HEAD_DIM = 256
ROPE_DIM = 128
ROW_BLOCK = 8
POS_SPAN = 8
MAX_POS = POS_SPAN * WINDOW
ROPE_BASE = 10000.0
EPS = 1e-6
SCORE_SCALE = HEAD_DIM ** -0.5


def draw_positions(pos_key):
    key_young, key_old, key_bits = jax.random.split(pos_key, 3)
    row_ids = jnp.arange(BATCH)
    log_window = int(math.log2(WINDOW))
    shift_bits = jax.random.randint(key_bits, (BATCH,), 3, log_window + 1)
    young_cap = jnp.minimum(jnp.left_shift(jnp.ones((BATCH,), jnp.int32), shift_bits), WINDOW)
    young_pos = jax.random.randint(key_young, (BATCH,), 0, young_cap)
    old_pos = jax.random.randint(key_old, (BATCH,), WINDOW, MAX_POS)
    positions = jnp.where(row_ids % 2 == 0, young_pos, old_pos)
    positions = jnp.where(row_ids == 0, 0, positions)
    positions = jnp.where(row_ids == 1, MAX_POS - 1, positions)
    return positions.astype(jnp.int32)


def slot_history(positions):
    slot_index = jnp.arange(WINDOW, dtype=jnp.int32)
    last_pos = positions[:, None] - 1
    latest = last_pos - jnp.mod(last_pos - slot_index[None, :], WINDOW)
    return jnp.where(latest >= 0, latest, -1).astype(jnp.int32)


def slot_waves():
    slot_index = jnp.arange(WINDOW, dtype=jnp.float32)
    harmonic = jnp.arange(1.0, 4.0, dtype=jnp.float32)
    angles = 2.0 * math.pi * harmonic[:, None] * slot_index[None, :] / WINDOW
    return jnp.concatenate([jnp.cos(angles), jnp.sin(angles)], axis=0)


def setup_inputs(seed: int = 0, part: int = 0) -> dict:
    part_key = jax.random.fold_in(jax.random.key(seed), part)
    key_list = jax.random.split(part_key, 8)
    shared = jax.random.split(jax.random.key(seed + 1), 7)
    positions = draw_positions(key_list[0])
    slot_pos = slot_history(positions)
    wave_table = slot_waves()
    k_coeffs = jax.random.normal(key_list[1], (BATCH, 6, HEAD_DIM), jnp.float32)
    k_noise = jax.random.normal(key_list[2], (BATCH, WINDOW, HEAD_DIM), jnp.float32)
    k_cache = 0.5 * jnp.einsum('bjd,js->bsd', k_coeffs, wave_table) + 0.8 * k_noise
    v_coeffs = jax.random.normal(key_list[3], (BATCH, 6, HEAD_DIM), jnp.float32)
    v_mean = jax.random.normal(key_list[4], (BATCH, 1, HEAD_DIM), jnp.float32)
    v_noise = jax.random.normal(key_list[5], (BATCH, WINDOW, HEAD_DIM), jnp.float32)
    v_cache = 0.7 * jnp.einsum('bjd,js->bsd', v_coeffs, wave_table) + 0.3 * v_mean + 0.5 * v_noise
    x_in = jax.random.normal(key_list[6], (BATCH, D_MODEL), jnp.float32)
    q_width = HEADS * HEAD_DIM
    norm_scale = 0.3 * jax.random.normal(shared[0], (D_MODEL,), jnp.float32)
    w_q = jax.random.normal(shared[1], (D_MODEL, q_width), jnp.float32) * D_MODEL ** -0.5
    w_k = jax.random.normal(shared[2], (D_MODEL, HEAD_DIM), jnp.float32) * D_MODEL ** -0.5
    w_v = jax.random.normal(shared[3], (D_MODEL, HEAD_DIM), jnp.float32) * D_MODEL ** -0.5
    w_o = jax.random.normal(shared[4], (q_width, D_MODEL), jnp.float32) * 2.0 * q_width ** -0.5
    b_o = 0.3 * jax.random.normal(shared[5], (D_MODEL,), jnp.float32)
    return {
        'x_in': x_in.astype(jnp.bfloat16),
        'positions': positions,
        'k_cache': k_cache.astype(jnp.bfloat16),
        'v_cache': v_cache.astype(jnp.bfloat16),
        'slot_pos': slot_pos,
        'norm_scale': norm_scale.astype(jnp.bfloat16),
        'w_q': w_q.astype(jnp.bfloat16),
        'w_k': w_k.astype(jnp.bfloat16),
        'w_v': w_v.astype(jnp.bfloat16),
        'w_o': w_o.astype(jnp.bfloat16),
        'b_o': b_o.astype(jnp.bfloat16),
    }


def rms_norm(x_in, norm_scale):
    x_f32 = x_in.astype(jnp.float32)
    mean_sq = jnp.mean(x_f32 * x_f32, axis=-1, keepdims=True)
    return (x_f32 * lax.rsqrt(mean_sq + EPS) * (1.0 + norm_scale.astype(jnp.float32))).astype(jnp.bfloat16)


def rope_tables(positions):
    rope_half = ROPE_DIM // 2
    inv_freq = ROPE_BASE ** (-jnp.arange(rope_half, dtype=jnp.float32) / rope_half)
    angles = positions.astype(jnp.float32)[:, None] * inv_freq[None, :]
    return jnp.cos(angles), jnp.sin(angles)


def rotate(tensor, cos_t, sin_t):
    rope_half = ROPE_DIM // 2
    rot_first = tensor[..., :rope_half]
    rot_second = tensor[..., rope_half:ROPE_DIM]
    return jnp.concatenate([rot_first * cos_t - rot_second * sin_t, rot_second * cos_t + rot_first * sin_t, tensor[..., ROPE_DIM:]], axis=-1)


def reference(x_in, positions, k_cache, v_cache, slot_pos, norm_scale, w_q, w_k, w_v, w_o, b_o):
    normed = rms_norm(x_in, norm_scale)
    cos_t, sin_t = rope_tables(positions)
    q_full = jnp.dot(normed, w_q, preferred_element_type=jnp.float32).reshape(BATCH, HEADS, HEAD_DIM)
    q_rot = rotate(q_full, cos_t[:, None, :], sin_t[:, None, :]).astype(jnp.bfloat16)
    k_new = rotate(jnp.dot(normed, w_k, preferred_element_type=jnp.float32), cos_t, sin_t).astype(jnp.bfloat16)
    v_new = jnp.dot(normed, w_v, preferred_element_type=jnp.float32).astype(jnp.bfloat16)
    row_ids = jnp.arange(BATCH)
    slot_now = jnp.mod(positions, WINDOW)
    k_out = k_cache.at[row_ids, slot_now].set(k_new)
    v_out = v_cache.at[row_ids, slot_now].set(v_new)
    slot_pos_out = slot_pos.at[row_ids, slot_now].set(positions)
    slot_age = positions[:, None] - slot_pos_out
    usable = (slot_pos_out >= 0) & (slot_age >= 0) & (slot_age < WINDOW)
    num_blocks = BATCH // ROW_BLOCK

    def attend(block_in):
        q_block, k_block, v_block, mask_block = block_in
        scores = jnp.einsum('bhd,bsd->bhs', q_block.astype(jnp.float32), k_block.astype(jnp.float32)) * SCORE_SCALE
        scores = jnp.where(mask_block[:, None, :], scores, -jnp.inf)
        attn_probs = jax.nn.softmax(scores, axis=-1)
        return jnp.einsum('bhs,bsd->bhd', attn_probs, v_block.astype(jnp.float32))

    attended = lax.map(attend, (
        q_rot.reshape(num_blocks, ROW_BLOCK, HEADS, HEAD_DIM),
        k_out.reshape(num_blocks, ROW_BLOCK, WINDOW, HEAD_DIM),
        v_out.reshape(num_blocks, ROW_BLOCK, WINDOW, HEAD_DIM),
        usable.reshape(num_blocks, ROW_BLOCK, WINDOW)))
    attn_rows = attended.reshape(BATCH, HEADS * HEAD_DIM).astype(jnp.bfloat16)
    x_out = (x_in.astype(jnp.float32) + jnp.dot(attn_rows, w_o, preferred_element_type=jnp.float32) + b_o.astype(jnp.float32)).astype(jnp.bfloat16)
    return (x_out, k_out, v_out, slot_pos_out)
```

```python
import functools
import numpy as np
import jax
import jax.numpy as jnp
from jax import lax
from jax.experimental import pallas as pl
from jax.experimental.pallas import tpu as pltpu
from jax.sharding import PartitionSpec as P

HEADS = 4
HEAD_DIM = 256
ROPE_DIM = 128
ROPE_BASE = 10000.0
EPS = 1e-6
NEG_LARGE = -1e30
SCORE_SCALE = HEAD_DIM ** -0.5

UNIT = 8
CHUNK_UNITS = 4
ROWS = UNIT * HEADS
PACKET = 2 * ROWS + 8
PIECES = 2
AHEAD = 3
MESH = pl.DeviceIdType.MESH
F32 = jnp.float32
BF16 = jnp.bfloat16


def attend_kernel(window, pos_h, freq_h, x_h, ns_h, wk_h, wv_h, wq_h, sp_h, wo_h, bo_h, k_h, v_h,
                  *rest):
    k_vm, v_vm = rest[:PIECES], rest[PIECES:2 * PIECES]
    (x_new, k_new, v_new, sp_new,
                  pos, freq, x_in, ns, wk, wv, wq, sp, wo, bo,
                  pos_b, x_f, q_s, pk, rc1, cm, rc2, o_s, ag,
                  in_sem, k_sem, v_sem, s1, r1, s2, r2, sa, ra, sb, rb, sc, rc) = rest[2 * PIECES:]
    me = lax.axis_index('kv')
    x_side, core = me // 2, me % 2
    over = {'kv': 2 * (1 - x_side) + core}
    beside = {'kv': 2 * x_side + 1 - core}
    over_i = 2 * (1 - x_side) + core
    batch, slots = sp.shape
    chunk = UNIT * CHUNK_UNITS
    chunks = batch // chunk
    half = chunks // 2

    barrier = pltpu.get_barrier_semaphore()
    pl.semaphore_signal(barrier, inc=1, device_id=over, device_id_type=MESH)
    pl.semaphore_signal(barrier, inc=1, device_id=beside, device_id_type=MESH)

    smalls = [pltpu.make_async_copy(src, dst, in_sem.at[n]) for n, (src, dst) in enumerate((
        (pos_h, pos), (freq_h, freq), (x_h, x_in), (ns_h, ns), (wk_h, wk), (wv_h, wv), (wq_h, wq), (sp_h, sp), (wo_h, wo), (bo_h, bo)))]

    span = chunks // PIECES

    def cache_copy(j, piece):
        rows, held = pl.ds(j * chunk, chunk), pl.ds((j - piece * span) * chunk, chunk)
        return (pltpu.make_async_copy(k_h.at[rows], k_vm[piece].at[held], k_sem.at[j]),
                pltpu.make_async_copy(v_h.at[rows], v_vm[piece].at[held], v_sem.at[j]))

    for small in smalls[:8]:
        small.start()
    for j in range(AHEAD):
        for copy in cache_copy(j, j // span):
            copy.start()
    for small in smalls[8:]:
        small.start()

    smalls[0].wait()
    smalls[1].wait()
    for r in range(batch // 128):
        row = pos[r:r + 1, :].astype(F32)
        pos_b[pl.ds(128 * r, 128), :] = jnp.transpose(jnp.broadcast_to(row, (128, 128)))
    angles = pos_b[...] * freq[...]
    low = lax.broadcasted_iota(jnp.int32, (batch, 128), 1) < ROPE_DIM // 2
    cos_t = jnp.cos(angles)
    sin_t = jnp.sin(angles)
    sin_t = jnp.where(low, -sin_t, sin_t)

    def rotate(first):
        return first * cos_t + pltpu.roll(first, ROPE_DIM // 2, 1) * sin_t

    smalls[2].wait()
    smalls[3].wait()
    x32 = x_in[...].astype(F32)
    x_f[...] = x32
    mean_sq = jnp.mean(x32 * x32, axis=-1, keepdims=True)
    normed = (x32 * lax.rsqrt(mean_sq + EPS) * (1.0 + ns[...].astype(F32))).astype(BF16)
    smalls[4].wait()
    smalls[5].wait()
    k_row = jnp.dot(normed, wk[...], preferred_element_type=F32)
    k_new[:, :128] = rotate(k_row[:, :128]).astype(BF16).astype(F32)
    k_new[:, 128:] = k_row[:, 128:].astype(BF16).astype(F32)
    v_new[...] = jnp.dot(normed, wv[...], preferred_element_type=F32).astype(BF16).astype(F32)
    smalls[6].wait()
    for h in range(HEADS):
        q_row = jnp.dot(normed, wq[:, h * HEAD_DIM:(h + 1) * HEAD_DIM], preferred_element_type=F32)
        q_s[:, h, :, :128] = rotate(q_row[:, :128]).reshape(batch // UNIT, UNIT, 128)
        q_s[:, h, :, 128:] = q_row[:, 128:].reshape(batch // UNIT, UNIT, 128)
    smalls[7].wait()
    pl.semaphore_wait(barrier, 2)

    lane = lax.broadcasted_iota(jnp.int32, (UNIT, 128), 1)
    row_seq = lax.broadcasted_iota(jnp.int32, (ROWS, 128), 0) % UNIT

    def scores_of(u, piece):
        keys = k_vm[piece][pl.ds(u * UNIT - piece * span * chunk, UNIT)].reshape(UNIT * slots, HEAD_DIM)
        q_b = q_s[u].reshape(ROWS, HEAD_DIM).astype(BF16)
        return q_b, lax.dot_general(q_b, keys, (((1,), (1,)), ((), ())), preferred_element_type=F32)

    def weights_of(u, q_b, all_scores):
        seqs = pl.ds(u * UNIT, UNIT)
        scores = all_scores[:, :slots]
        for s in range(1, UNIT):
            scores = jnp.where(row_seq == s, all_scores[:, s * slots:(s + 1) * slots], scores)
        p_now = pos_b[seqs, :].astype(jnp.int32)
        slot = (p_now & (window - 1)) - me * slots
        hit = lane == slot
        held = jnp.where(hit, p_now, sp[seqs, :])
        sp_new[seqs, :] = held
        age = p_now - held
        usable = (held >= 0) & (age >= 0) & (age < window)
        fresh = jnp.sum(q_b.astype(F32).reshape(HEADS, UNIT, HEAD_DIM) * k_new[seqs, :][None], axis=-1, keepdims=True)
        scores = jnp.where(hit[None], fresh, scores.reshape(HEADS, UNIT, slots)) * SCORE_SCALE
        scores = jnp.where(usable[None], scores, NEG_LARGE)
        top = jnp.max(scores, axis=-1, keepdims=True)
        weights = jnp.where(usable[None], jnp.exp(scores - top), 0.0)
        total = jnp.sum(weights, axis=-1, keepdims=True)
        fresh_weight = jnp.sum(jnp.where(hit[None], weights, 0.0), axis=-1, keepdims=True)
        kept = jnp.where(hit[None], 0.0, weights).reshape(ROWS, slots)
        spread = jnp.concatenate([jnp.where(row_seq == s, kept, 0.0).astype(BF16) for s in range(UNIT)], axis=1)
        return top, total, fresh_weight, spread

    def sums_of(u, piece, fresh_weight, spread):
        values = v_vm[piece][pl.ds(u * UNIT - piece * span * chunk, UNIT)].reshape(UNIT * slots, HEAD_DIM)
        sums = jnp.dot(spread, values, preferred_element_type=F32).reshape(HEADS, UNIT, HEAD_DIM)
        sums = sums + fresh_weight.astype(BF16).astype(F32) * v_new[pl.ds(u * UNIT, UNIT), :][None]
        return sums.reshape(ROWS, HEAD_DIM)

    def attend(j, piece):
        units = [j * CHUNK_UNITS + i for i in range(CHUNK_UNITS)]
        scored = [scores_of(u, piece) for u in units]
        weighed = [weights_of(u, *pair) for u, pair in zip(units, scored)]
        for i, u in enumerate(units):
            top, total, fresh_weight, spread = weighed[i]
            sums = sums_of(u, piece, fresh_weight, spread)
            pk[j, i, 0:ROWS, :] = sums[:, :128]
            pk[j, i, ROWS:2 * ROWS, :] = sums[:, 128:]
            tile = jnp.zeros((UNIT, 128), F32)
            for h in range(HEADS):
                tile = jnp.where(lane == h, top[h], jnp.where(lane == HEADS + h, total[h], tile))
            pk[j, i, 2 * ROWS:, :] = tile

    def merge(a, b):
        ta, tb = a[2 * ROWS:, :], b[2 * ROWS:, :]
        tile = jnp.maximum(ta, tb)
        ea, eb = jnp.exp(ta - tile), jnp.exp(tb - tile)
        parts, totals = [], []
        for h in range(HEADS):
            fa, fb = ea[:, h:h + 1], eb[:, h:h + 1]
            totals.append(fa * ta[:, HEADS + h:HEADS + h + 1] + fb * tb[:, HEADS + h:HEADS + h + 1])
            parts.append([fa * a[o + h * UNIT:o + (h + 1) * UNIT, :] + fb * b[o + h * UNIT:o + (h + 1) * UNIT, :] for o in (0, ROWS)])
        return tile, parts, totals

    def first_copy(j):
        return pltpu.make_async_remote_copy(pk.at[j, pl.ds(2 * (1 - core), 2)], rc1.at[j], s1.at[j], r1.at[j], device_id=beside, device_id_type=MESH)

    def second_copy(j):
        return pltpu.make_async_remote_copy(cm.at[j, 1 - x_side], rc2.at[j], s2.at[j], r2.at[j], device_id=over, device_id_type=MESH)

    def first_merge(j):
        first_copy(j).wait_recv()
        for i in range(2):
            tile, parts, totals = merge(pk[j, 2 * core + i], rc1[j, i])
            for h in range(HEADS):
                cm[j, i, h * UNIT:(h + 1) * UNIT, :] = parts[h][0]
                cm[j, i, ROWS + h * UNIT:ROWS + (h + 1) * UNIT, :] = parts[h][1]
                tile = jnp.where(lane == HEADS + h, totals[h], tile)
            cm[j, i, 2 * ROWS:, :] = tile
        second_copy(j).start()

    def second_merge(j):
        second_copy(j).wait_recv()
        _, parts, totals = merge(cm[j, x_side], rc2[j])
        rows = pl.ds(j * UNIT, UNIT)
        for h in range(HEADS):
            inverse = 1.0 / totals[h]
            o_s[rows, h * HEAD_DIM:h * HEAD_DIM + 128] = parts[h][0] * inverse
            o_s[rows, h * HEAD_DIM + 128:(h + 1) * HEAD_DIM] = parts[h][1] * inverse

    own_unit = 2 * core + x_side

    def gather_copy(g, owner, target, send, recv):
        rows = ag.at[owner, pl.ds(g * half * UNIT, half * UNIT)]
        return pltpu.make_async_remote_copy(rows, rows, send.at[g], recv.at[g], device_id=target, device_id_type=MESH)

    def project(g):
        o_b = o_s[pl.ds(g * half * UNIT, half * UNIT), :].astype(BF16)
        rows = jnp.concatenate([x_f[pl.ds((g * half + i) * chunk + own_unit * UNIT, UNIT), :] for i in range(half)], axis=0)
        ag[me, pl.ds(g * half * UNIT, half * UNIT), :] = rows + jnp.dot(o_b, wo[...], preferred_element_type=F32) + bo[...].astype(F32)
        gather_copy(g, me, over, sa, ra).start()
        gather_copy(g, me, beside, sb, rb).start()

    def forward(g):
        gather_copy(g, me, over, sa, ra).wait_recv()
        gather_copy(g, over_i, beside, sc, rc).start()

    def step(piece, j, carry):
        for ahead in range(PIECES):
            @pl.when((j + AHEAD < chunks) & ((j + AHEAD) // span == ahead))
            def _():
                for copy in cache_copy(j + AHEAD, ahead):
                    copy.start()
        for copy in cache_copy(j, piece):
            copy.wait()
        attend(j, piece)
        first_copy(j).start()

        @pl.when(j >= 1)
        def _():
            first_merge(j - 1)

        @pl.when(j >= 3)
        def _():
            second_merge(j - 3)

        @pl.when(j == half + 2)
        def _():
            smalls[8].wait()
            smalls[9].wait()
            project(0)

        return carry

    for piece in range(PIECES):
        lax.fori_loop(piece * span, (piece + 1) * span, functools.partial(step, piece), 0)
    second_merge(chunks - 3)
    forward(0)
    first_merge(chunks - 1)
    second_merge(chunks - 2)
    second_merge(chunks - 1)
    project(1)
    forward(1)
    for g in range(2):
        gather_copy(g, me, beside, sb, rb).wait_recv()
        gather_copy(g, me, beside, sc, rc).wait_recv()
    for c in range(2):
        for j in range(chunks):
            rows = [ag[2 * s + c, j * UNIT:(j + 1) * UNIT, :] for s in range(2)]
            x_new[j * chunk + 2 * UNIT * c:j * chunk + 2 * UNIT * (c + 1), :] = jnp.concatenate(rows, axis=0).astype(BF16)

    def drain(j, carry):
        first_copy(j).wait_send()
        second_copy(j).wait_send()
        return carry

    lax.fori_loop(0, chunks, drain, 0)
    for g in range(2):
        gather_copy(g, me, over, sa, ra).wait_send()
        gather_copy(g, me, beside, sb, rb).wait_send()
        gather_copy(g, over_i, beside, sc, rc).wait_send()


def write_kernel(window, pos, k_new, v_new, x_new, sp_new, *rest):
    k_vm, v_vm = rest[:PIECES], rest[PIECES:2 * PIECES]
    x_out, k_out, v_out, sp_out, k_ring, v_ring, sems, k_sem, v_sem = rest[2 * PIECES:]
    me = lax.axis_index('kv')
    part, slots, _ = k_vm[0].shape
    batch = part * PIECES
    depth, chunk = k_ring.shape[:2]
    chunks = batch // chunk
    span = chunks // PIECES
    others = (pltpu.make_async_copy(x_new, x_out, sems.at[0]), pltpu.make_async_copy(sp_new, sp_out, sems.at[1]))
    for copy in others:
        copy.start()
    tile_row = lax.broadcasted_iota(jnp.int32, (16, HEAD_DIM), 0)

    def copies(j):
        rows, ring = pl.ds(j * chunk, chunk), lax.rem(j, depth)
        return (pltpu.make_async_copy(k_ring.at[ring], k_out.at[rows], k_sem.at[ring]),
                pltpu.make_async_copy(v_ring.at[ring], v_out.at[rows], v_sem.at[ring]))

    def step(piece, j, carry):
        ring = lax.rem(j, depth)

        @pl.when(j >= depth)
        def _():
            for copy in copies(j - depth):
                copy.wait()

        def group(i, carry):
            for n in range(8):
                row = i * 8 + n
                b = j * chunk + row
                slot = (pos[b] & (window - 1)) - me * slots
                base = pl.multiple_of((jnp.clip(slot, 0, slots - 1) // 16) * 16, 16)
                for new, cache, out in ((k_new, k_vm[piece], k_ring), (v_new, v_vm[piece], v_ring)):
                    out[ring, row] = cache[b - piece * part]
                    fresh = jnp.broadcast_to(new[pl.ds(b, 1), :], (16, HEAD_DIM))
                    old = cache[b - piece * part, pl.ds(base, 16), :].astype(F32)
                    out[ring, row, pl.ds(base, 16), :] = jnp.where(tile_row == slot - base, fresh, old).astype(BF16)
            return carry
        lax.fori_loop(0, chunk // 8, group, 0)
        for copy in copies(j):
            copy.start()
        return carry

    for piece in range(PIECES):
        lax.fori_loop(piece * span, (piece + 1) * span, functools.partial(step, piece), 0)
    for j in range(chunks - depth, chunks):
        for copy in copies(j):
            copy.wait()
    for copy in others:
        copy.wait()


def solution(mesh):
    kv_size = mesh.shape['kv']
    row_spec = P('dp', None)
    cache_spec = P('dp', 'kv', None)
    slot_spec = P('dp', 'kv')
    vec_spec = P(None)
    mat_spec = P(None, None)
    half_dims = ROPE_DIM // 2
    freq_row = np.tile(ROPE_BASE ** (-np.arange(half_dims) / half_dims), 2).astype(np.float32)[None, :]

    def local_step(x_in, positions, k_cache, v_cache, slot_pos, norm_scale, w_q, w_k, w_v, w_o, b_o):
        batch, model = x_in.shape
        slots = k_cache.shape[1]
        window = slots * kv_size
        width = w_q.shape[1]
        chunks = batch // (UNIT * CHUNK_UNITS)
        hbm = pl.BlockSpec(memory_space=pltpu.HBM)
        vmem = pl.BlockSpec(memory_space=pltpu.VMEM)
        smem = pl.BlockSpec(memory_space=pltpu.SMEM)
        dma = pltpu.SemaphoreType.DMA
        per_chunk = [dma((chunks,))] * 4
        *held, x_new, k_new, v_new, sp_new = pl.pallas_call(
            functools.partial(attend_kernel, window),
            out_shape=(*([pltpu.VMEM((batch // PIECES, slots, HEAD_DIM), BF16)] * (2 * PIECES)), pltpu.VMEM((batch, model), BF16),
                       pltpu.VMEM((batch, HEAD_DIM), F32), pltpu.VMEM((batch, HEAD_DIM), F32), pltpu.VMEM((batch, slots), jnp.int32)),
            in_specs=[hbm] * 12,
            out_specs=(vmem,) * (2 * PIECES + 4),
            scratch_shapes=[
                pltpu.VMEM((batch // 128, 128), jnp.int32), pltpu.VMEM((1, 128), F32), pltpu.VMEM((batch, model), BF16), pltpu.VMEM((1, model), BF16),
                pltpu.VMEM((model, HEAD_DIM), BF16), pltpu.VMEM((model, HEAD_DIM), BF16), pltpu.VMEM((model, width), BF16),
                pltpu.VMEM((batch, slots), jnp.int32), pltpu.VMEM((width, model), BF16), pltpu.VMEM((1, model), BF16),
                pltpu.VMEM((batch, 128), F32), pltpu.VMEM((batch, model), F32), pltpu.VMEM((batch // UNIT, HEADS, UNIT, HEAD_DIM), F32),
                pltpu.VMEM((chunks, CHUNK_UNITS, PACKET, 128), F32), pltpu.VMEM((chunks, 2, PACKET, 128), F32),
                pltpu.VMEM((chunks, 2, PACKET, 128), F32), pltpu.VMEM((chunks, PACKET, 128), F32),
                pltpu.VMEM((chunks * UNIT, width), F32), pltpu.VMEM((kv_size, chunks * UNIT, model), F32),
                dma((10,)), dma((chunks,)), dma((chunks,)), *per_chunk, *([dma((2,))] * 6)],
            compiler_params=pltpu.CompilerParams(vmem_limit_bytes=16 << 20, collective_id=0, has_side_effects=True),
            name='attend',
        )(*[pltpu.with_memory_space_constraint(a, pltpu.HBM) for a in (
            positions.reshape(batch // 128, 128), jnp.asarray(freq_row), x_in, norm_scale.reshape(1, model), w_k, w_v, w_q, slot_pos,
            w_o, b_o.reshape(1, model), k_cache, v_cache)])
        x_out, k_out, v_out, slot_pos_out = pl.pallas_call(
            functools.partial(write_kernel, window),
            out_shape=(jax.ShapeDtypeStruct((batch, model), BF16), jax.ShapeDtypeStruct(k_cache.shape, BF16),
                       jax.ShapeDtypeStruct(v_cache.shape, BF16), jax.ShapeDtypeStruct((batch, slots), jnp.int32)),
            in_specs=[smem] + [vmem] * (2 * PIECES + 4),
            out_specs=(hbm,) * 4,
            scratch_shapes=[pltpu.VMEM((4, 16, slots, HEAD_DIM), BF16), pltpu.VMEM((4, 16, slots, HEAD_DIM), BF16), dma((2,)), dma((4,)), dma((4,))],
            compiler_params=pltpu.CompilerParams(vmem_limit_bytes=9 << 20),
            name='write',
        )(positions, k_new, v_new, x_new, sp_new, *held)
        return x_out, k_out, v_out, slot_pos_out

    return jax.shard_map(
        local_step,
        mesh=mesh,
        in_specs=(row_spec, P('dp'), cache_spec, cache_spec, slot_spec, vec_spec, mat_spec, mat_spec, mat_spec, mat_spec, vec_spec),
        out_specs=(row_spec, cache_spec, cache_spec, slot_spec),
        check_vma=False)
```

```python
import functools
import numpy as np
import jax
import jax.numpy as jnp
from jax import lax
from jax.experimental import pallas as pl
from jax.experimental.pallas import tpu as pltpu
from jax.sharding import PartitionSpec as P

HEADS = 4
HEAD_DIM = 256
ROPE_DIM = 128
ROPE_BASE = 10000.0
EPS = 1e-6
NEG_LARGE = -1e30
SCORE_SCALE = HEAD_DIM ** -0.5

UNIT = 8
CHUNK_UNITS = 4
ROWS = UNIT * HEADS
PACKET = 2 * ROWS + 8
PIECES = 2
AHEAD = 3
MESH = pl.DeviceIdType.MESH
F32 = jnp.float32
BF16 = jnp.bfloat16


def attend_kernel(window, pos_h, freq_h, x_h, ns_h, wk_h, wv_h, wq_h, sp_h, wo_h, bo_h, k_h, v_h,
                  *rest):
    k_vm, v_vm = rest[:PIECES], rest[PIECES:2 * PIECES]
    (x_new, k_new, v_new, sp_new,
                  pos, freq, x_in, ns, wk, wv, wq, sp, wo, bo,
                  pos_b, x_f, q_s, pk, rc1, cm, rc2, o_s, ag,
                  in_sem, k_sem, v_sem, s1, r1, s2, r2, sa, ra, sb, rb, sc, rc) = rest[2 * PIECES:]
    me = lax.axis_index('kv')
    x_side, core = me // 2, me % 2
    over = {'kv': 2 * (1 - x_side) + core}
    beside = {'kv': 2 * x_side + 1 - core}
    over_i = 2 * (1 - x_side) + core
    batch, slots = sp.shape
    chunk = UNIT * CHUNK_UNITS
    chunks = batch // chunk
    half = chunks // 2

    barrier = pltpu.get_barrier_semaphore()
    pl.semaphore_signal(barrier, inc=1, device_id=over, device_id_type=MESH)
    pl.semaphore_signal(barrier, inc=1, device_id=beside, device_id_type=MESH)

    smalls = [pltpu.make_async_copy(src, dst, in_sem.at[n]) for n, (src, dst) in enumerate((
        (pos_h, pos), (freq_h, freq), (x_h, x_in), (ns_h, ns), (wk_h, wk), (wv_h, wv), (wq_h, wq), (sp_h, sp), (wo_h, wo), (bo_h, bo)))]

    span = chunks // PIECES

    def cache_copy(j, piece):
        rows, held = pl.ds(j * chunk, chunk), pl.ds((j - piece * span) * chunk, chunk)
        return (pltpu.make_async_copy(k_h.at[rows], k_vm[piece].at[held], k_sem.at[j]),
                pltpu.make_async_copy(v_h.at[rows], v_vm[piece].at[held], v_sem.at[j]))

    def read_ahead(first, last):
        for j in range(first, last):
            for copy in cache_copy(j, j // span):
                copy.start()

    for small in smalls[:8]:
        small.start()
    read_ahead(0, AHEAD)

    smalls[0].wait()
    smalls[1].wait()
    for r in range(batch // 128):
        row = pos[r:r + 1, :].astype(F32)
        pos_b[pl.ds(128 * r, 128), :] = jnp.transpose(jnp.broadcast_to(row, (128, 128)))
    angles = pos_b[...] * freq[...]
    low = lax.broadcasted_iota(jnp.int32, (batch, 128), 1) < ROPE_DIM // 2
    cos_t = jnp.cos(angles)
    sin_t = jnp.sin(angles)
    sin_t = jnp.where(low, -sin_t, sin_t)

    def rotate(first):
        return first * cos_t + pltpu.roll(first, ROPE_DIM // 2, 1) * sin_t

    read_ahead(AHEAD, AHEAD + 1)
    smalls[2].wait()
    smalls[3].wait()
    x32 = x_in[...].astype(F32)
    x_f[...] = x32
    mean_sq = jnp.mean(x32 * x32, axis=-1, keepdims=True)
    normed = (x32 * lax.rsqrt(mean_sq + EPS) * (1.0 + ns[...].astype(F32)[None, :])).astype(BF16)
    smalls[4].wait()
    smalls[5].wait()
    k_row = jnp.dot(normed, wk[...], preferred_element_type=F32)
    k_new[:, :128] = rotate(k_row[:, :128]).astype(BF16).astype(F32)
    k_new[:, 128:] = k_row[:, 128:].astype(BF16).astype(F32)
    v_new[...] = jnp.dot(normed, wv[...], preferred_element_type=F32).astype(BF16).astype(F32)
    smalls[6].wait()
    read_ahead(AHEAD + 1, chunks)
    for small in smalls[8:]:
        small.start()
    for h in range(HEADS):
        q_row = jnp.dot(normed, wq[:, h * HEAD_DIM:(h + 1) * HEAD_DIM], preferred_element_type=F32)
        q_s[:, h, :, :128] = rotate(q_row[:, :128]).reshape(batch // UNIT, UNIT, 128)
        q_s[:, h, :, 128:] = q_row[:, 128:].reshape(batch // UNIT, UNIT, 128)
    smalls[7].wait()
    pl.semaphore_wait(barrier, 2)

    lane = lax.broadcasted_iota(jnp.int32, (UNIT, 128), 1)
    row_seq = lax.broadcasted_iota(jnp.int32, (ROWS, 128), 0) % UNIT

    def scores_of(u, piece):
        keys = k_vm[piece][pl.ds(u * UNIT - piece * span * chunk, UNIT)].reshape(UNIT * slots, HEAD_DIM)
        q_b = q_s[u].reshape(ROWS, HEAD_DIM).astype(BF16)
        return q_b, lax.dot_general(q_b, keys, (((1,), (1,)), ((), ())), preferred_element_type=F32)

    def weights_of(u, q_b, all_scores):
        seqs = pl.ds(u * UNIT, UNIT)
        scores = all_scores[:, :slots]
        for s in range(1, UNIT):
            scores = jnp.where(row_seq == s, all_scores[:, s * slots:(s + 1) * slots], scores)
        p_now = pos_b[seqs, :].astype(jnp.int32)
        slot = (p_now & (window - 1)) - me * slots
        hit = lane == slot
        held = jnp.where(hit, p_now, sp[seqs, :])
        sp_new[seqs, :] = held
        age = p_now - held
        usable = (held >= 0) & (age >= 0) & (age < window)
        fresh = jnp.sum(q_b.astype(F32).reshape(HEADS, UNIT, HEAD_DIM) * k_new[seqs, :][None], axis=-1, keepdims=True)
        scores = jnp.where(hit[None], fresh, scores.reshape(HEADS, UNIT, slots)) * SCORE_SCALE
        scores = jnp.where(usable[None], scores, NEG_LARGE)
        top = jnp.max(scores, axis=-1, keepdims=True)
        weights = jnp.where(usable[None], jnp.exp(scores - top), 0.0)
        total = jnp.sum(weights, axis=-1, keepdims=True)
        fresh_weight = jnp.sum(jnp.where(hit[None], weights, 0.0), axis=-1, keepdims=True)
        kept = jnp.where(hit[None], 0.0, weights).reshape(ROWS, slots)
        spread = jnp.concatenate([jnp.where(row_seq == s, kept, 0.0).astype(BF16) for s in range(UNIT)], axis=1)
        return top, total, fresh_weight, spread

    def sums_of(u, piece, fresh_weight, spread):
        values = v_vm[piece][pl.ds(u * UNIT - piece * span * chunk, UNIT)].reshape(UNIT * slots, HEAD_DIM)
        sums = jnp.dot(spread, values, preferred_element_type=F32).reshape(HEADS, UNIT, HEAD_DIM)
        sums = sums + fresh_weight.astype(BF16).astype(F32) * v_new[pl.ds(u * UNIT, UNIT), :][None]
        return sums.reshape(ROWS, HEAD_DIM)

    def attend(j, piece):
        units = [j * CHUNK_UNITS + i for i in range(CHUNK_UNITS)]
        scored = [scores_of(u, piece) for u in units]
        weighed = [weights_of(u, *pair) for u, pair in zip(units, scored)]
        for i, u in enumerate(units):
            top, total, fresh_weight, spread = weighed[i]
            sums = sums_of(u, piece, fresh_weight, spread)
            pk[j, i, 0:ROWS, :] = sums[:, :128]
            pk[j, i, ROWS:2 * ROWS, :] = sums[:, 128:]
            tile = jnp.zeros((UNIT, 128), F32)
            for h in range(HEADS):
                tile = jnp.where(lane == h, top[h], jnp.where(lane == HEADS + h, total[h], tile))
            pk[j, i, 2 * ROWS:, :] = tile

    def merge(a, b):
        ta, tb = a[2 * ROWS:, :], b[2 * ROWS:, :]
        tile = jnp.maximum(ta, tb)
        ea, eb = jnp.exp(ta - tile), jnp.exp(tb - tile)
        parts, totals = [], []
        for h in range(HEADS):
            fa, fb = ea[:, h:h + 1], eb[:, h:h + 1]
            totals.append(fa * ta[:, HEADS + h:HEADS + h + 1] + fb * tb[:, HEADS + h:HEADS + h + 1])
            parts.append([fa * a[o + h * UNIT:o + (h + 1) * UNIT, :] + fb * b[o + h * UNIT:o + (h + 1) * UNIT, :] for o in (0, ROWS)])
        return tile, parts, totals

    def first_copy(j):
        return pltpu.make_async_remote_copy(pk.at[j, pl.ds(2 * (1 - core), 2)], rc1.at[j], s1.at[j], r1.at[j], device_id=beside, device_id_type=MESH)

    def second_copy(j):
        return pltpu.make_async_remote_copy(cm.at[j, 1 - x_side], rc2.at[j], s2.at[j], r2.at[j], device_id=over, device_id_type=MESH)

    def first_merge(j):
        first_copy(j).wait_recv()
        for i in range(2):
            tile, parts, totals = merge(pk[j, 2 * core + i], rc1[j, i])
            for h in range(HEADS):
                cm[j, i, h * UNIT:(h + 1) * UNIT, :] = parts[h][0]
                cm[j, i, ROWS + h * UNIT:ROWS + (h + 1) * UNIT, :] = parts[h][1]
                tile = jnp.where(lane == HEADS + h, totals[h], tile)
            cm[j, i, 2 * ROWS:, :] = tile
        second_copy(j).start()

    def second_merge(j):
        second_copy(j).wait_recv()
        _, parts, totals = merge(cm[j, x_side], rc2[j])
        rows = pl.ds(j * UNIT, UNIT)
        for h in range(HEADS):
            inverse = 1.0 / totals[h]
            o_s[rows, h * HEAD_DIM:h * HEAD_DIM + 128] = parts[h][0] * inverse
            o_s[rows, h * HEAD_DIM + 128:(h + 1) * HEAD_DIM] = parts[h][1] * inverse

    own_unit = 2 * core + x_side

    def gather_copy(g, owner, target, send, recv):
        rows = ag.at[owner, pl.ds(g * half * UNIT, half * UNIT)]
        return pltpu.make_async_remote_copy(rows, rows, send.at[g], recv.at[g], device_id=target, device_id_type=MESH)

    def project(g):
        o_b = o_s[pl.ds(g * half * UNIT, half * UNIT), :].astype(BF16)
        rows = jnp.concatenate([x_f[pl.ds((g * half + i) * chunk + own_unit * UNIT, UNIT), :] for i in range(half)], axis=0)
        ag[me, pl.ds(g * half * UNIT, half * UNIT), :] = rows + jnp.dot(o_b, wo[...], preferred_element_type=F32) + bo[...].astype(F32)[None, :]
        gather_copy(g, me, over, sa, ra).start()
        gather_copy(g, me, beside, sb, rb).start()

    def forward(g):
        gather_copy(g, me, over, sa, ra).wait_recv()
        gather_copy(g, over_i, beside, sc, rc).start()

    def step(piece, j, carry):
        for copy in cache_copy(j, piece):
            copy.wait()
        attend(j, piece)
        first_copy(j).start()

        @pl.when(j >= 1)
        def _():
            first_merge(j - 1)

        @pl.when(j >= 3)
        def _():
            second_merge(j - 3)

        @pl.when(j == half + 2)
        def _():
            smalls[8].wait()
            smalls[9].wait()
            project(0)

        return carry

    for piece in range(PIECES):
        lax.fori_loop(piece * span, (piece + 1) * span, functools.partial(step, piece), 0)
    second_merge(chunks - 3)
    forward(0)
    first_merge(chunks - 1)
    second_merge(chunks - 2)
    second_merge(chunks - 1)
    project(1)
    forward(1)
    for g in range(2):
        gather_copy(g, me, beside, sb, rb).wait_recv()
        gather_copy(g, me, beside, sc, rc).wait_recv()
    for c in range(2):
        for j in range(chunks):
            rows = [ag[2 * s + c, j * UNIT:(j + 1) * UNIT, :] for s in range(2)]
            x_new[j * chunk + 2 * UNIT * c:j * chunk + 2 * UNIT * (c + 1), :] = jnp.concatenate(rows, axis=0).astype(BF16)

    def drain(j, carry):
        first_copy(j).wait_send()
        second_copy(j).wait_send()
        return carry

    lax.fori_loop(0, chunks, drain, 0)
    for g in range(2):
        gather_copy(g, me, over, sa, ra).wait_send()
        gather_copy(g, me, beside, sb, rb).wait_send()
        gather_copy(g, over_i, beside, sc, rc).wait_send()


def write_kernel(window, pos, k_new, v_new, x_new, sp_new, *rest):
    k_vm, v_vm = rest[:PIECES], rest[PIECES:2 * PIECES]
    x_out, k_out, v_out, sp_out, k_ring, v_ring, sems, k_sem, v_sem = rest[2 * PIECES:]
    me = lax.axis_index('kv')
    part, slots, _ = k_vm[0].shape
    batch = part * PIECES
    depth, chunk = k_ring.shape[:2]
    chunks = batch // chunk
    span = chunks // PIECES
    others = (pltpu.make_async_copy(x_new, x_out, sems.at[0]), pltpu.make_async_copy(sp_new, sp_out, sems.at[1]))
    for copy in others:
        copy.start()
    tile_row = lax.broadcasted_iota(jnp.int32, (16, HEAD_DIM), 0)

    def copies(j):
        rows, ring = pl.ds(j * chunk, chunk), lax.rem(j, depth)
        return (pltpu.make_async_copy(k_ring.at[ring], k_out.at[rows], k_sem.at[ring]),
                pltpu.make_async_copy(v_ring.at[ring], v_out.at[rows], v_sem.at[ring]))

    def step(piece, j, carry):
        ring = lax.rem(j, depth)

        @pl.when(j >= depth)
        def _():
            for copy in copies(j - depth):
                copy.wait()

        def group(i, carry):
            for n in range(8):
                row = i * 8 + n
                b = j * chunk + row
                slot = (pos[b] & (window - 1)) - me * slots
                base = pl.multiple_of((jnp.clip(slot, 0, slots - 1) // 16) * 16, 16)
                for new, cache, out in ((k_new, k_vm[piece], k_ring), (v_new, v_vm[piece], v_ring)):
                    out[ring, row] = cache[b - piece * part]
                    fresh = jnp.broadcast_to(new[pl.ds(b, 1), :], (16, HEAD_DIM))
                    old = cache[b - piece * part, pl.ds(base, 16), :].astype(F32)
                    out[ring, row, pl.ds(base, 16), :] = jnp.where(tile_row == slot - base, fresh, old).astype(BF16)
            return carry
        lax.fori_loop(0, chunk // 8, group, 0)
        for copy in copies(j):
            copy.start()
        return carry

    for piece in range(PIECES):
        lax.fori_loop(piece * span, (piece + 1) * span, functools.partial(step, piece), 0)
    for j in range(chunks - depth, chunks):
        for copy in copies(j):
            copy.wait()
    for copy in others:
        copy.wait()


def solution(mesh):
    kv_size = mesh.shape['kv']
    row_spec = P('dp', None)
    cache_spec = P('dp', 'kv', None)
    slot_spec = P('dp', 'kv')
    vec_spec = P(None)
    mat_spec = P(None, None)
    half_dims = ROPE_DIM // 2
    freq_row = np.tile(ROPE_BASE ** (-np.arange(half_dims) / half_dims), 2).astype(np.float32)[None, :]

    def local_step(x_in, positions, k_cache, v_cache, slot_pos, norm_scale, w_q, w_k, w_v, w_o, b_o):
        batch, model = x_in.shape
        slots = k_cache.shape[1]
        window = slots * kv_size
        width = w_q.shape[1]
        chunks = batch // (UNIT * CHUNK_UNITS)
        hbm = pl.BlockSpec(memory_space=pltpu.HBM)
        vmem = pl.BlockSpec(memory_space=pltpu.VMEM)
        smem = pl.BlockSpec(memory_space=pltpu.SMEM)
        dma = pltpu.SemaphoreType.DMA
        per_chunk = [dma((chunks,))] * 4
        *held, x_new, k_new, v_new, sp_new = pl.pallas_call(
            functools.partial(attend_kernel, window),
            out_shape=(*([pltpu.VMEM((batch // PIECES, slots, HEAD_DIM), BF16)] * (2 * PIECES)), pltpu.VMEM((batch, model), BF16),
                       pltpu.VMEM((batch, HEAD_DIM), F32), pltpu.VMEM((batch, HEAD_DIM), F32), pltpu.VMEM((batch, slots), jnp.int32)),
            in_specs=[hbm] * 12,
            out_specs=(vmem,) * (2 * PIECES + 4),
            scratch_shapes=[
                pltpu.VMEM((batch // 128, 128), jnp.int32), pltpu.VMEM((1, 128), F32), pltpu.VMEM((batch, model), BF16), pltpu.VMEM((model,), BF16),
                pltpu.VMEM((model, HEAD_DIM), BF16), pltpu.VMEM((model, HEAD_DIM), BF16), pltpu.VMEM((model, width), BF16),
                pltpu.VMEM((batch, slots), jnp.int32), pltpu.VMEM((width, model), BF16), pltpu.VMEM((model,), BF16),
                pltpu.VMEM((batch, 128), F32), pltpu.VMEM((batch, model), F32), pltpu.VMEM((batch // UNIT, HEADS, UNIT, HEAD_DIM), F32),
                pltpu.VMEM((chunks, CHUNK_UNITS, PACKET, 128), F32), pltpu.VMEM((chunks, 2, PACKET, 128), F32),
                pltpu.VMEM((chunks, 2, PACKET, 128), F32), pltpu.VMEM((chunks, PACKET, 128), F32),
                pltpu.VMEM((chunks * UNIT, width), F32), pltpu.VMEM((kv_size, chunks * UNIT, model), F32),
                dma((10,)), dma((chunks,)), dma((chunks,)), *per_chunk, *([dma((2,))] * 6)],
            compiler_params=pltpu.CompilerParams(vmem_limit_bytes=16 << 20, collective_id=0, has_side_effects=True),
            name='attend',
        )(*[pltpu.with_memory_space_constraint(a, pltpu.HBM) for a in (
            positions.reshape(batch // 128, 128), jnp.asarray(freq_row), x_in, norm_scale, w_k, w_v, w_q, slot_pos,
            w_o, b_o, k_cache, v_cache)])
        x_out, k_out, v_out, slot_pos_out = pl.pallas_call(
            functools.partial(write_kernel, window),
            out_shape=(jax.ShapeDtypeStruct((batch, model), BF16), jax.ShapeDtypeStruct(k_cache.shape, BF16),
                       jax.ShapeDtypeStruct(v_cache.shape, BF16), jax.ShapeDtypeStruct((batch, slots), jnp.int32)),
            in_specs=[smem] + [vmem] * (2 * PIECES + 4),
            out_specs=(hbm,) * 4,
            scratch_shapes=[pltpu.VMEM((4, 16, slots, HEAD_DIM), BF16), pltpu.VMEM((4, 16, slots, HEAD_DIM), BF16), dma((2,)), dma((4,)), dma((4,))],
            compiler_params=pltpu.CompilerParams(vmem_limit_bytes=9 << 20),
            name='write',
        )(positions, k_new, v_new, x_new, sp_new, *held)
        return x_out, k_out, v_out, slot_pos_out

    return jax.shard_map(
        local_step,
        mesh=mesh,
        in_specs=(row_spec, P('dp'), cache_spec, cache_spec, slot_spec, vec_spec, mat_spec, mat_spec, mat_spec, mat_spec, vec_spec),
        out_specs=(row_spec, cache_spec, cache_spec, slot_spec),
        check_vma=False)
```

```python
import functools
import numpy as np
import jax
import jax.numpy as jnp
from jax import lax
from jax.experimental import pallas as pl
from jax.experimental.pallas import tpu as pltpu
from jax.sharding import PartitionSpec as P

HEADS = 4
HEAD_DIM = 256
ROPE_DIM = 128
ROPE_BASE = 10000.0
EPS = 1e-6
NEG_LARGE = -1e30
SCORE_SCALE = HEAD_DIM ** -0.5

UNIT = 8
CHUNK_UNITS = 4
ROWS = UNIT * HEADS
PACKET = 2 * ROWS + 8
PIECES = 2
AHEAD = 3
MESH = pl.DeviceIdType.MESH
F32 = jnp.float32
BF16 = jnp.bfloat16


def attend_kernel(window, pos_h, freq_h, x_h, ns_h, wk_h, wv_h, wq_h, sp_h, k_h, v_h, *rest):
    k_vm, v_vm = rest[:PIECES], rest[PIECES:2 * PIECES]
    (pk, x_f, k_new, v_new, sp_new, pos, freq, x_in, ns, wk, wv, wq, sp, pos_b, q_s, in_sem, k_sem, v_sem) = rest[2 * PIECES:]
    me = lax.axis_index('kv')
    batch, slots = sp.shape
    chunk = UNIT * CHUNK_UNITS
    chunks = batch // chunk

    smalls = [pltpu.make_async_copy(src, dst, in_sem.at[n]) for n, (src, dst) in enumerate((
        (pos_h, pos), (freq_h, freq), (x_h, x_in), (ns_h, ns), (wk_h, wk), (wv_h, wv), (wq_h, wq), (sp_h, sp)))]

    span = chunks // PIECES

    def cache_copy(j, piece):
        rows, held = pl.ds(j * chunk, chunk), pl.ds((j - piece * span) * chunk, chunk)
        return (pltpu.make_async_copy(k_h.at[rows], k_vm[piece].at[held], k_sem.at[j]),
                pltpu.make_async_copy(v_h.at[rows], v_vm[piece].at[held], v_sem.at[j]))

    def read_ahead(first, last):
        for j in range(first, last):
            for copy in cache_copy(j, j // span):
                copy.start()

    for small in smalls:
        small.start()
    read_ahead(0, AHEAD)

    smalls[0].wait()
    smalls[1].wait()
    for r in range(batch // 128):
        row = pos[r:r + 1, :].astype(F32)
        pos_b[pl.ds(128 * r, 128), :] = jnp.transpose(jnp.broadcast_to(row, (128, 128)))
    angles = pos_b[...] * freq[...]
    low = lax.broadcasted_iota(jnp.int32, (batch, 128), 1) < ROPE_DIM // 2
    cos_t = jnp.cos(angles)
    sin_t = jnp.sin(angles)
    sin_t = jnp.where(low, -sin_t, sin_t)

    def rotate(first):
        return first * cos_t + pltpu.roll(first, ROPE_DIM // 2, 1) * sin_t

    read_ahead(AHEAD, AHEAD + 1)
    smalls[2].wait()
    smalls[3].wait()
    x32 = x_in[...].astype(F32)
    x_f[...] = x32
    mean_sq = jnp.mean(x32 * x32, axis=-1, keepdims=True)
    normed = (x32 * lax.rsqrt(mean_sq + EPS) * (1.0 + ns[...].astype(F32)[None, :])).astype(BF16)
    smalls[4].wait()
    smalls[5].wait()
    k_row = jnp.dot(normed, wk[...], preferred_element_type=F32)
    k_new[:, :128] = rotate(k_row[:, :128]).astype(BF16).astype(F32)
    k_new[:, 128:] = k_row[:, 128:].astype(BF16).astype(F32)
    v_new[...] = jnp.dot(normed, wv[...], preferred_element_type=F32).astype(BF16).astype(F32)
    smalls[6].wait()
    read_ahead(AHEAD + 1, chunks)
    for h in range(HEADS):
        q_row = jnp.dot(normed, wq[:, h * HEAD_DIM:(h + 1) * HEAD_DIM], preferred_element_type=F32)
        q_s[:, h, :, :128] = rotate(q_row[:, :128]).reshape(batch // UNIT, UNIT, 128)
        q_s[:, h, :, 128:] = q_row[:, 128:].reshape(batch // UNIT, UNIT, 128)
    smalls[7].wait()

    lane = lax.broadcasted_iota(jnp.int32, (UNIT, 128), 1)
    row_seq = lax.broadcasted_iota(jnp.int32, (ROWS, 128), 0) % UNIT

    def scores_of(u, piece):
        keys = k_vm[piece][pl.ds(u * UNIT - piece * span * chunk, UNIT)].reshape(UNIT * slots, HEAD_DIM)
        q_b = q_s[u].reshape(ROWS, HEAD_DIM).astype(BF16)
        return q_b, lax.dot_general(q_b, keys, (((1,), (1,)), ((), ())), preferred_element_type=F32)

    def weights_of(u, q_b, all_scores):
        seqs = pl.ds(u * UNIT, UNIT)
        scores = all_scores[:, :slots]
        for s in range(1, UNIT):
            scores = jnp.where(row_seq == s, all_scores[:, s * slots:(s + 1) * slots], scores)
        p_now = pos_b[seqs, :].astype(jnp.int32)
        slot = (p_now & (window - 1)) - me * slots
        hit = lane == slot
        held = jnp.where(hit, p_now, sp[seqs, :])
        sp_new[seqs, :] = held
        age = p_now - held
        usable = (held >= 0) & (age >= 0) & (age < window)
        fresh = jnp.sum(q_b.astype(F32).reshape(HEADS, UNIT, HEAD_DIM) * k_new[seqs, :][None], axis=-1, keepdims=True)
        scores = jnp.where(hit[None], fresh, scores.reshape(HEADS, UNIT, slots)) * SCORE_SCALE
        scores = jnp.where(usable[None], scores, NEG_LARGE)
        top = jnp.max(scores, axis=-1, keepdims=True)
        weights = jnp.where(usable[None], jnp.exp(scores - top), 0.0)
        total = jnp.sum(weights, axis=-1, keepdims=True)
        fresh_weight = jnp.sum(jnp.where(hit[None], weights, 0.0), axis=-1, keepdims=True)
        kept = jnp.where(hit[None], 0.0, weights).reshape(ROWS, slots)
        spread = jnp.concatenate([jnp.where(row_seq == s, kept, 0.0).astype(BF16) for s in range(UNIT)], axis=1)
        return top, total, fresh_weight, spread

    def sums_of(u, piece, fresh_weight, spread):
        values = v_vm[piece][pl.ds(u * UNIT - piece * span * chunk, UNIT)].reshape(UNIT * slots, HEAD_DIM)
        sums = jnp.dot(spread, values, preferred_element_type=F32).reshape(HEADS, UNIT, HEAD_DIM)
        sums = sums + fresh_weight.astype(BF16).astype(F32) * v_new[pl.ds(u * UNIT, UNIT), :][None]
        return sums.reshape(ROWS, HEAD_DIM)

    def attend(j, piece):
        units = [j * CHUNK_UNITS + i for i in range(CHUNK_UNITS)]
        scored = [scores_of(u, piece) for u in units]
        weighed = [weights_of(u, *pair) for u, pair in zip(units, scored)]
        for i, u in enumerate(units):
            top, total, fresh_weight, spread = weighed[i]
            sums = sums_of(u, piece, fresh_weight, spread)
            pk[j, i, 0:ROWS, :] = sums[:, :128]
            pk[j, i, ROWS:2 * ROWS, :] = sums[:, 128:]
            tile = jnp.zeros((UNIT, 128), F32)
            for h in range(HEADS):
                tile = jnp.where(lane == h, top[h], jnp.where(lane == HEADS + h, total[h], tile))
            pk[j, i, 2 * ROWS:, :] = tile

    def step(piece, j, carry):
        for copy in cache_copy(j, piece):
            copy.wait()
        attend(j, piece)
        return carry

    for piece in range(PIECES):
        lax.fori_loop(piece * span, (piece + 1) * span, functools.partial(step, piece), 0)


def exchange_kernel(wo_h, bo_h, pk, x_f, x_new, wo, bo, rc1, cm, rc2, o_s, ag, in_sem, s1, r1, s2, r2, sa, ra, sb, rb, sc, rc):
    me = lax.axis_index('kv')
    x_side, core = me // 2, me % 2
    over_i = 2 * (1 - x_side) + core
    over = {'kv': over_i}
    beside = {'kv': 2 * x_side + 1 - core}
    chunks = pk.shape[0]
    chunk = UNIT * CHUNK_UNITS
    half = chunks // 2
    barrier = pltpu.get_barrier_semaphore()
    pl.semaphore_signal(barrier, inc=1, device_id=over, device_id_type=MESH)
    pl.semaphore_signal(barrier, inc=1, device_id=beside, device_id_type=MESH)
    smalls = [pltpu.make_async_copy(src, dst, in_sem.at[n]) for n, (src, dst) in enumerate(((wo_h, wo), (bo_h, bo)))]
    for small in smalls:
        small.start()
    lane = lax.broadcasted_iota(jnp.int32, (UNIT, 128), 1)

    def merge(a, b):
        ta, tb = a[2 * ROWS:, :], b[2 * ROWS:, :]
        tile = jnp.maximum(ta, tb)
        ea, eb = jnp.exp(ta - tile), jnp.exp(tb - tile)
        parts, totals = [], []
        for h in range(HEADS):
            fa, fb = ea[:, h:h + 1], eb[:, h:h + 1]
            totals.append(fa * ta[:, HEADS + h:HEADS + h + 1] + fb * tb[:, HEADS + h:HEADS + h + 1])
            parts.append([fa * a[o + h * UNIT:o + (h + 1) * UNIT, :] + fb * b[o + h * UNIT:o + (h + 1) * UNIT, :] for o in (0, ROWS)])
        return tile, parts, totals

    def first_copy(j):
        return pltpu.make_async_remote_copy(pk.at[j, pl.ds(2 * (1 - core), 2)], rc1.at[j], s1.at[j], r1.at[j], device_id=beside, device_id_type=MESH)

    def second_copy(j):
        return pltpu.make_async_remote_copy(cm.at[j, 1 - x_side], rc2.at[j], s2.at[j], r2.at[j], device_id=over, device_id_type=MESH)

    def first_merge(j):
        first_copy(j).wait_recv()
        for i in range(2):
            tile, parts, totals = merge(pk[j, 2 * core + i], rc1[j, i])
            for h in range(HEADS):
                cm[j, i, h * UNIT:(h + 1) * UNIT, :] = parts[h][0]
                cm[j, i, ROWS + h * UNIT:ROWS + (h + 1) * UNIT, :] = parts[h][1]
                tile = jnp.where(lane == HEADS + h, totals[h], tile)
            cm[j, i, 2 * ROWS:, :] = tile
        second_copy(j).start()

    def second_merge(j):
        second_copy(j).wait_recv()
        _, parts, totals = merge(cm[j, x_side], rc2[j])
        rows = pl.ds(j * UNIT, UNIT)
        for h in range(HEADS):
            inverse = 1.0 / totals[h]
            o_s[rows, h * HEAD_DIM:h * HEAD_DIM + 128] = parts[h][0] * inverse
            o_s[rows, h * HEAD_DIM + 128:(h + 1) * HEAD_DIM] = parts[h][1] * inverse

    own_unit = 2 * core + x_side

    def gather_copy(g, owner, target, send, recv):
        rows = ag.at[owner, pl.ds(g * half * UNIT, half * UNIT)]
        return pltpu.make_async_remote_copy(rows, rows, send.at[g], recv.at[g], device_id=target, device_id_type=MESH)

    def project(g):
        o_b = o_s[pl.ds(g * half * UNIT, half * UNIT), :].astype(BF16)
        rows = jnp.concatenate([x_f[pl.ds((g * half + i) * chunk + own_unit * UNIT, UNIT), :] for i in range(half)], axis=0)
        ag[me, pl.ds(g * half * UNIT, half * UNIT), :] = rows + jnp.dot(o_b, wo[...], preferred_element_type=F32) + bo[...].astype(F32)[None, :]
        gather_copy(g, me, over, sa, ra).start()
        gather_copy(g, me, beside, sb, rb).start()

    def forward(g):
        gather_copy(g, me, over, sa, ra).wait_recv()
        gather_copy(g, over_i, beside, sc, rc).start()

    pl.semaphore_wait(barrier, 2)

    def send(j, carry):
        first_copy(j).start()
        return carry

    def first(j, carry):
        first_merge(j)
        return carry

    def second(j, carry):
        second_merge(j)
        return carry

    lax.fori_loop(0, chunks, send, 0)
    lax.fori_loop(0, chunks, first, 0)
    for small in smalls:
        small.wait()
    lax.fori_loop(0, half, second, 0)
    project(0)
    lax.fori_loop(half, chunks, second, 0)
    project(1)
    forward(0)
    forward(1)
    for g in range(2):
        gather_copy(g, me, beside, sb, rb).wait_recv()
        gather_copy(g, me, beside, sc, rc).wait_recv()
    for c in range(2):
        for j in range(chunks):
            rows = [ag[2 * s + c, j * UNIT:(j + 1) * UNIT, :] for s in range(2)]
            x_new[j * chunk + 2 * UNIT * c:j * chunk + 2 * UNIT * (c + 1), :] = jnp.concatenate(rows, axis=0).astype(BF16)

    def drain(j, carry):
        first_copy(j).wait_send()
        second_copy(j).wait_send()
        return carry

    lax.fori_loop(0, chunks, drain, 0)
    for g in range(2):
        gather_copy(g, me, over, sa, ra).wait_send()
        gather_copy(g, me, beside, sb, rb).wait_send()
        gather_copy(g, over_i, beside, sc, rc).wait_send()


def write_kernel(window, pos, k_new, v_new, x_new, sp_new, *rest):
    k_vm, v_vm = rest[:PIECES], rest[PIECES:2 * PIECES]
    x_out, k_out, v_out, sp_out, k_ring, v_ring, sems, k_sem, v_sem = rest[2 * PIECES:]
    me = lax.axis_index('kv')
    part, slots, _ = k_vm[0].shape
    batch = part * PIECES
    depth, chunk = k_ring.shape[:2]
    chunks = batch // chunk
    span = chunks // PIECES
    others = (pltpu.make_async_copy(x_new, x_out, sems.at[0]), pltpu.make_async_copy(sp_new, sp_out, sems.at[1]))
    for copy in others:
        copy.start()
    tile_row = lax.broadcasted_iota(jnp.int32, (16, HEAD_DIM), 0)

    def copies(j):
        rows, ring = pl.ds(j * chunk, chunk), lax.rem(j, depth)
        return (pltpu.make_async_copy(k_ring.at[ring], k_out.at[rows], k_sem.at[ring]),
                pltpu.make_async_copy(v_ring.at[ring], v_out.at[rows], v_sem.at[ring]))

    def step(piece, j, carry):
        ring = lax.rem(j, depth)

        @pl.when(j >= depth)
        def _():
            for copy in copies(j - depth):
                copy.wait()

        def group(i, carry):
            for n in range(8):
                row = i * 8 + n
                b = j * chunk + row
                slot = (pos[b] & (window - 1)) - me * slots
                base = pl.multiple_of((jnp.clip(slot, 0, slots - 1) // 16) * 16, 16)
                for new, cache, out in ((k_new, k_vm[piece], k_ring), (v_new, v_vm[piece], v_ring)):
                    out[ring, row] = cache[b - piece * part]
                    fresh = jnp.broadcast_to(new[pl.ds(b, 1), :], (16, HEAD_DIM))
                    old = cache[b - piece * part, pl.ds(base, 16), :].astype(F32)
                    out[ring, row, pl.ds(base, 16), :] = jnp.where(tile_row == slot - base, fresh, old).astype(BF16)
            return carry
        lax.fori_loop(0, chunk // 8, group, 0)
        for copy in copies(j):
            copy.start()
        return carry

    for piece in range(PIECES):
        lax.fori_loop(piece * span, (piece + 1) * span, functools.partial(step, piece), 0)
    for j in range(chunks - depth, chunks):
        for copy in copies(j):
            copy.wait()
    for copy in others:
        copy.wait()


def solution(mesh):
    kv_size = mesh.shape['kv']
    row_spec = P('dp', None)
    cache_spec = P('dp', 'kv', None)
    slot_spec = P('dp', 'kv')
    vec_spec = P(None)
    mat_spec = P(None, None)
    half_dims = ROPE_DIM // 2
    freq_row = np.tile(ROPE_BASE ** (-np.arange(half_dims) / half_dims), 2).astype(np.float32)[None, :]

    def local_step(x_in, positions, k_cache, v_cache, slot_pos, norm_scale, w_q, w_k, w_v, w_o, b_o):
        batch, model = x_in.shape
        slots = k_cache.shape[1]
        window = slots * kv_size
        width = w_q.shape[1]
        chunks = batch // (UNIT * CHUNK_UNITS)
        hbm = pl.BlockSpec(memory_space=pltpu.HBM)
        vmem = pl.BlockSpec(memory_space=pltpu.VMEM)
        smem = pl.BlockSpec(memory_space=pltpu.SMEM)
        dma = pltpu.SemaphoreType.DMA
        per_chunk = [dma((chunks,))] * 4
        at_hbm = functools.partial(pltpu.with_memory_space_constraint, memory_space=pltpu.HBM)
        *held, pk, x_f, k_new, v_new, sp_new = pl.pallas_call(
            functools.partial(attend_kernel, window),
            out_shape=(*([pltpu.VMEM((batch // PIECES, slots, HEAD_DIM), BF16)] * (2 * PIECES)),
                       pltpu.VMEM((chunks, CHUNK_UNITS, PACKET, 128), F32), pltpu.VMEM((batch, model), F32),
                       pltpu.VMEM((batch, HEAD_DIM), F32), pltpu.VMEM((batch, HEAD_DIM), F32), pltpu.VMEM((batch, slots), jnp.int32)),
            in_specs=[hbm] * 10,
            out_specs=(vmem,) * (2 * PIECES + 5),
            scratch_shapes=[
                pltpu.VMEM((batch // 128, 128), jnp.int32), pltpu.VMEM((1, 128), F32), pltpu.VMEM((batch, model), BF16), pltpu.VMEM((model,), BF16),
                pltpu.VMEM((model, HEAD_DIM), BF16), pltpu.VMEM((model, HEAD_DIM), BF16), pltpu.VMEM((model, width), BF16),
                pltpu.VMEM((batch, slots), jnp.int32),
                pltpu.VMEM((batch, 128), F32), pltpu.VMEM((batch // UNIT, HEADS, UNIT, HEAD_DIM), F32),
                dma((8,)), dma((chunks,)), dma((chunks,))],
            compiler_params=pltpu.CompilerParams(vmem_limit_bytes=14 << 20),
            name='attend',
        )(*map(at_hbm, (positions.reshape(batch // 128, 128), jnp.asarray(freq_row), x_in, norm_scale, w_k, w_v, w_q, slot_pos, k_cache, v_cache)))
        x_new = pl.pallas_call(
            exchange_kernel,
            out_shape=pltpu.VMEM((batch, model), BF16),
            in_specs=[hbm] * 2 + [vmem] * 2,
            out_specs=vmem,
            scratch_shapes=[
                pltpu.VMEM((width, model), BF16), pltpu.VMEM((model,), BF16), pltpu.VMEM((chunks, 2, PACKET, 128), F32),
                pltpu.VMEM((chunks, 2, PACKET, 128), F32), pltpu.VMEM((chunks, PACKET, 128), F32),
                pltpu.VMEM((chunks * UNIT, width), F32), pltpu.VMEM((kv_size, chunks * UNIT, model), F32),
                dma((2,)), *per_chunk, *([dma((2,))] * 6)],
            compiler_params=pltpu.CompilerParams(vmem_limit_bytes=10 << 20, collective_id=0, has_side_effects=True),
            name='exchange',
        )(at_hbm(w_o), at_hbm(b_o), pk, x_f)
        x_out, k_out, v_out, slot_pos_out = pl.pallas_call(
            functools.partial(write_kernel, window),
            out_shape=(jax.ShapeDtypeStruct((batch, model), BF16), jax.ShapeDtypeStruct(k_cache.shape, BF16),
                       jax.ShapeDtypeStruct(v_cache.shape, BF16), jax.ShapeDtypeStruct((batch, slots), jnp.int32)),
            in_specs=[smem] + [vmem] * (2 * PIECES + 4),
            out_specs=(hbm,) * 4,
            scratch_shapes=[pltpu.VMEM((4, 16, slots, HEAD_DIM), BF16), pltpu.VMEM((4, 16, slots, HEAD_DIM), BF16), dma((2,)), dma((4,)), dma((4,))],
            compiler_params=pltpu.CompilerParams(vmem_limit_bytes=9 << 20),
            name='write',
        )(positions, k_new, v_new, x_new, sp_new, *held)
        return x_out, k_out, v_out, slot_pos_out

    return jax.shard_map(
        local_step,
        mesh=mesh,
        in_specs=(row_spec, P('dp'), cache_spec, cache_spec, slot_spec, vec_spec, mat_spec, mat_spec, mat_spec, mat_spec, vec_spec),
        out_specs=(row_spec, cache_spec, cache_spec, slot_spec),
        check_vma=False)
```

```python
import functools
import numpy as np
import jax
import jax.numpy as jnp
from jax import lax
from jax.experimental import pallas as pl
from jax.experimental.pallas import tpu as pltpu
from jax.sharding import PartitionSpec as P

HEADS = 4
HEAD_DIM = 256
ROPE_DIM = 128
ROPE_BASE = 10000.0
EPS = 1e-6
NEG_LARGE = -1e30
SCORE_SCALE = HEAD_DIM ** -0.5

UNIT = 8
CHUNK_UNITS = 4
ROWS = UNIT * HEADS
PACKET = 2 * ROWS + 8
PIECES = 2
AHEAD = 2
MESH = pl.DeviceIdType.MESH
F32 = jnp.float32
BF16 = jnp.bfloat16


def attend_kernel(window, pos_h, freq_h, x_h, ns_h, wk_h, wv_h, wq_h, sp_h, wo_h, bo_h, k_h, v_h,
                  *rest):
    k_vm, v_vm = rest[:PIECES], rest[PIECES:2 * PIECES]
    (x_new, k_new, v_new, sp_new,
                  pos, freq, x_in, ns, wk, wv, wq, sp, wo, bo,
                  pos_b, x_f, q_s, pk, rc1, cm, rc2, o_s, ag,
                  in_sem, k_sem, v_sem, s1, r1, s2, r2, sa, ra, sb, rb, sc, rc) = rest[2 * PIECES:]
    me = lax.axis_index('kv')
    x_side, core = me // 2, me % 2
    over = {'kv': 2 * (1 - x_side) + core}
    beside = {'kv': 2 * x_side + 1 - core}
    over_i = 2 * (1 - x_side) + core
    batch, slots = sp.shape
    chunk = UNIT * CHUNK_UNITS
    chunks = batch // chunk
    half = chunks // 2

    barrier = pltpu.get_barrier_semaphore()
    pl.semaphore_signal(barrier, inc=1, device_id=over, device_id_type=MESH)
    pl.semaphore_signal(barrier, inc=1, device_id=beside, device_id_type=MESH)

    smalls = [pltpu.make_async_copy(src, dst, in_sem.at[n]) for n, (src, dst) in enumerate((
        (pos_h, pos), (freq_h, freq), (x_h, x_in), (ns_h, ns), (wk_h, wk), (wv_h, wv), (wq_h, wq), (sp_h, sp), (wo_h, wo), (bo_h, bo)))]

    span = chunks // PIECES

    def cache_copy(j, piece):
        rows, held = pl.ds(j * chunk, chunk), pl.ds((j - piece * span) * chunk, chunk)
        return (pltpu.make_async_copy(k_h.at[rows], k_vm[piece].at[held], k_sem.at[j]),
                pltpu.make_async_copy(v_h.at[rows], v_vm[piece].at[held], v_sem.at[j]))

    def read_ahead(first, last):
        for j in range(first, last):
            for copy in cache_copy(j, j // span):
                copy.start()

    for small in smalls[:8]:
        small.start()
    read_ahead(0, AHEAD)

    smalls[0].wait()
    smalls[1].wait()
    for r in range(batch // 128):
        row = pos[r:r + 1, :].astype(F32)
        pos_b[pl.ds(128 * r, 128), :] = jnp.transpose(jnp.broadcast_to(row, (128, 128)))
    angles = pos_b[...] * freq[...]
    low = lax.broadcasted_iota(jnp.int32, (batch, 128), 1) < ROPE_DIM // 2
    cos_t = jnp.cos(angles)
    sin_t = jnp.sin(angles)
    sin_t = jnp.where(low, -sin_t, sin_t)

    def rotate(first):
        return first * cos_t + pltpu.roll(first, ROPE_DIM // 2, 1) * sin_t

    smalls[2].wait()
    smalls[3].wait()
    x32 = x_in[...].astype(F32)
    x_f[...] = x32
    mean_sq = jnp.mean(x32 * x32, axis=-1, keepdims=True)
    normed = (x32 * lax.rsqrt(mean_sq + EPS) * (1.0 + ns[...].astype(F32)[None, :])).astype(BF16)
    smalls[4].wait()
    smalls[5].wait()
    k_row = jnp.dot(normed, wk[...], preferred_element_type=F32)
    k_new[:, :128] = rotate(k_row[:, :128]).astype(BF16).astype(F32)
    k_new[:, 128:] = k_row[:, 128:].astype(BF16).astype(F32)
    v_new[...] = jnp.dot(normed, wv[...], preferred_element_type=F32).astype(BF16).astype(F32)
    smalls[6].wait()
    for small in smalls[8:]:
        small.start()
    for h in range(HEADS):
        q_row = jnp.dot(normed, wq[:, h * HEAD_DIM:(h + 1) * HEAD_DIM], preferred_element_type=F32)
        q_s[:, h, :, :128] = rotate(q_row[:, :128]).reshape(batch // UNIT, UNIT, 128)
        q_s[:, h, :, 128:] = q_row[:, 128:].reshape(batch // UNIT, UNIT, 128)
    smalls[7].wait()
    pl.semaphore_wait(barrier, 2)

    lane = lax.broadcasted_iota(jnp.int32, (UNIT, 128), 1)
    row_seq = lax.broadcasted_iota(jnp.int32, (ROWS, 128), 0) % UNIT

    def scores_of(u, piece):
        keys = k_vm[piece][pl.ds(u * UNIT - piece * span * chunk, UNIT)].reshape(UNIT * slots, HEAD_DIM)
        q_b = q_s[u].reshape(ROWS, HEAD_DIM).astype(BF16)
        return q_b, lax.dot_general(q_b, keys, (((1,), (1,)), ((), ())), preferred_element_type=F32)

    def weights_of(u, q_b, all_scores):
        seqs = pl.ds(u * UNIT, UNIT)
        scores = all_scores[:, :slots]
        for s in range(1, UNIT):
            scores = jnp.where(row_seq == s, all_scores[:, s * slots:(s + 1) * slots], scores)
        p_now = pos_b[seqs, :].astype(jnp.int32)
        slot = (p_now & (window - 1)) - me * slots
        hit = lane == slot
        held = jnp.where(hit, p_now, sp[seqs, :])
        sp_new[seqs, :] = held
        age = p_now - held
        usable = (held >= 0) & (age >= 0) & (age < window)
        fresh = jnp.sum(q_b.astype(F32).reshape(HEADS, UNIT, HEAD_DIM) * k_new[seqs, :][None], axis=-1, keepdims=True)
        scores = jnp.where(hit[None], fresh, scores.reshape(HEADS, UNIT, slots)) * SCORE_SCALE
        scores = jnp.where(usable[None], scores, NEG_LARGE)
        top = jnp.max(scores, axis=-1, keepdims=True)
        weights = jnp.where(usable[None], jnp.exp(scores - top), 0.0)
        total = jnp.sum(weights, axis=-1, keepdims=True)
        fresh_weight = jnp.sum(jnp.where(hit[None], weights, 0.0), axis=-1, keepdims=True)
        kept = jnp.where(hit[None], 0.0, weights).reshape(ROWS, slots)
        spread = jnp.concatenate([jnp.where(row_seq == s, kept, 0.0).astype(BF16) for s in range(UNIT)], axis=1)
        return top, total, fresh_weight, spread

    def sums_of(u, piece, fresh_weight, spread):
        values = v_vm[piece][pl.ds(u * UNIT - piece * span * chunk, UNIT)].reshape(UNIT * slots, HEAD_DIM)
        sums = jnp.dot(spread, values, preferred_element_type=F32).reshape(HEADS, UNIT, HEAD_DIM)
        sums = sums + fresh_weight.astype(BF16).astype(F32) * v_new[pl.ds(u * UNIT, UNIT), :][None]
        return sums.reshape(ROWS, HEAD_DIM)

    def attend(j, piece):
        units = [j * CHUNK_UNITS + i for i in range(CHUNK_UNITS)]
        scored = [scores_of(u, piece) for u in units]
        weighed = [weights_of(u, *pair) for u, pair in zip(units, scored)]
        for i, u in enumerate(units):
            top, total, fresh_weight, spread = weighed[i]
            sums = sums_of(u, piece, fresh_weight, spread)
            pk[j, i, 0:ROWS, :] = sums[:, :128]
            pk[j, i, ROWS:2 * ROWS, :] = sums[:, 128:]
            tile = jnp.zeros((UNIT, 128), F32)
            for h in range(HEADS):
                tile = jnp.where(lane == h, top[h], jnp.where(lane == HEADS + h, total[h], tile))
            pk[j, i, 2 * ROWS:, :] = tile

    def merge(a, b):
        ta, tb = a[2 * ROWS:, :], b[2 * ROWS:, :]
        tile = jnp.maximum(ta, tb)
        ea, eb = jnp.exp(ta - tile), jnp.exp(tb - tile)
        parts, totals = [], []
        for h in range(HEADS):
            fa, fb = ea[:, h:h + 1], eb[:, h:h + 1]
            totals.append(fa * ta[:, HEADS + h:HEADS + h + 1] + fb * tb[:, HEADS + h:HEADS + h + 1])
            parts.append([fa * a[o + h * UNIT:o + (h + 1) * UNIT, :] + fb * b[o + h * UNIT:o + (h + 1) * UNIT, :] for o in (0, ROWS)])
        return tile, parts, totals

    def first_copy(j):
        return pltpu.make_async_remote_copy(pk.at[j, pl.ds(2 * (1 - core), 2)], rc1.at[j], s1.at[j], r1.at[j], device_id=beside, device_id_type=MESH)

    def second_copy(j):
        return pltpu.make_async_remote_copy(cm.at[j, 1 - x_side], rc2.at[j], s2.at[j], r2.at[j], device_id=over, device_id_type=MESH)

    def first_merge(j):
        first_copy(j).wait_recv()
        for i in range(2):
            tile, parts, totals = merge(pk[j, 2 * core + i], rc1[j, i])
            for h in range(HEADS):
                cm[j, i, h * UNIT:(h + 1) * UNIT, :] = parts[h][0]
                cm[j, i, ROWS + h * UNIT:ROWS + (h + 1) * UNIT, :] = parts[h][1]
                tile = jnp.where(lane == HEADS + h, totals[h], tile)
            cm[j, i, 2 * ROWS:, :] = tile
        second_copy(j).start()

    def second_merge(j):
        second_copy(j).wait_recv()
        _, parts, totals = merge(cm[j, x_side], rc2[j])
        rows = pl.ds(j * UNIT, UNIT)
        for h in range(HEADS):
            inverse = 1.0 / totals[h]
            o_s[rows, h * HEAD_DIM:h * HEAD_DIM + 128] = parts[h][0] * inverse
            o_s[rows, h * HEAD_DIM + 128:(h + 1) * HEAD_DIM] = parts[h][1] * inverse

    own_unit = 2 * core + x_side

    def gather_copy(g, owner, target, send, recv):
        rows = ag.at[owner, pl.ds(g * half * UNIT, half * UNIT)]
        return pltpu.make_async_remote_copy(rows, rows, send.at[g], recv.at[g], device_id=target, device_id_type=MESH)

    def project(g):
        o_b = o_s[pl.ds(g * half * UNIT, half * UNIT), :].astype(BF16)
        rows = jnp.concatenate([x_f[pl.ds((g * half + i) * chunk + own_unit * UNIT, UNIT), :] for i in range(half)], axis=0)
        ag[me, pl.ds(g * half * UNIT, half * UNIT), :] = rows + jnp.dot(o_b, wo[...], preferred_element_type=F32) + bo[...].astype(F32)[None, :]
        gather_copy(g, me, over, sa, ra).start()
        gather_copy(g, me, beside, sb, rb).start()

    def forward(g):
        gather_copy(g, me, over, sa, ra).wait_recv()
        gather_copy(g, over_i, beside, sc, rc).start()

    def step(piece, j, carry):
        for copy in cache_copy(j, piece):
            copy.wait()
        attend(j, piece)
        first_copy(j).start()

        @pl.when(j >= 1)
        def _():
            first_merge(j - 1)

        @pl.when(j >= 3)
        def _():
            second_merge(j - 3)

        @pl.when(j == half + 2)
        def _():
            smalls[8].wait()
            smalls[9].wait()
            project(0)

        for ahead in range(PIECES):
            @pl.when((j + AHEAD < chunks) & ((j + AHEAD) // span == ahead))
            def _():
                for copy in cache_copy(j + AHEAD, ahead):
                    copy.start()

        return carry

    for piece in range(PIECES):
        lax.fori_loop(piece * span, (piece + 1) * span, functools.partial(step, piece), 0)
    second_merge(chunks - 3)
    forward(0)
    first_merge(chunks - 1)
    second_merge(chunks - 2)
    second_merge(chunks - 1)
    project(1)
    forward(1)
    for g in range(2):
        gather_copy(g, me, beside, sb, rb).wait_recv()
        gather_copy(g, me, beside, sc, rc).wait_recv()
    for c in range(2):
        for j in range(chunks):
            rows = [ag[2 * s + c, j * UNIT:(j + 1) * UNIT, :] for s in range(2)]
            x_new[j * chunk + 2 * UNIT * c:j * chunk + 2 * UNIT * (c + 1), :] = jnp.concatenate(rows, axis=0).astype(BF16)

    def drain(j, carry):
        first_copy(j).wait_send()
        second_copy(j).wait_send()
        return carry

    lax.fori_loop(0, chunks, drain, 0)
    for g in range(2):
        gather_copy(g, me, over, sa, ra).wait_send()
        gather_copy(g, me, beside, sb, rb).wait_send()
        gather_copy(g, over_i, beside, sc, rc).wait_send()


def write_kernel(window, pos, k_new, v_new, x_new, sp_new, *rest):
    k_vm, v_vm = rest[:PIECES], rest[PIECES:2 * PIECES]
    x_out, k_out, v_out, sp_out, k_ring, v_ring, sems, k_sem, v_sem = rest[2 * PIECES:]
    me = lax.axis_index('kv')
    part, slots, _ = k_vm[0].shape
    batch = part * PIECES
    depth, chunk = k_ring.shape[:2]
    chunks = batch // chunk
    span = chunks // PIECES
    others = (pltpu.make_async_copy(x_new, x_out, sems.at[0]), pltpu.make_async_copy(sp_new, sp_out, sems.at[1]))
    for copy in others:
        copy.start()
    tile_row = lax.broadcasted_iota(jnp.int32, (16, HEAD_DIM), 0)

    def copies(j):
        rows, ring = pl.ds(j * chunk, chunk), lax.rem(j, depth)
        return (pltpu.make_async_copy(k_ring.at[ring], k_out.at[rows], k_sem.at[ring]),
                pltpu.make_async_copy(v_ring.at[ring], v_out.at[rows], v_sem.at[ring]))

    def step(piece, j, carry):
        ring = lax.rem(j, depth)

        @pl.when(j >= depth)
        def _():
            for copy in copies(j - depth):
                copy.wait()

        def group(i, carry):
            for n in range(8):
                row = i * 8 + n
                b = j * chunk + row
                slot = (pos[b] & (window - 1)) - me * slots
                base = pl.multiple_of((jnp.clip(slot, 0, slots - 1) // 16) * 16, 16)
                for new, cache, out in ((k_new, k_vm[piece], k_ring), (v_new, v_vm[piece], v_ring)):
                    out[ring, row] = cache[b - piece * part]
                    fresh = jnp.broadcast_to(new[pl.ds(b, 1), :], (16, HEAD_DIM))
                    old = cache[b - piece * part, pl.ds(base, 16), :].astype(F32)
                    out[ring, row, pl.ds(base, 16), :] = jnp.where(tile_row == slot - base, fresh, old).astype(BF16)
            return carry
        lax.fori_loop(0, chunk // 8, group, 0)
        for copy in copies(j):
            copy.start()
        return carry

    for piece in range(PIECES):
        lax.fori_loop(piece * span, (piece + 1) * span, functools.partial(step, piece), 0)
    for j in range(chunks - depth, chunks):
        for copy in copies(j):
            copy.wait()
    for copy in others:
        copy.wait()


def solution(mesh):
    kv_size = mesh.shape['kv']
    row_spec = P('dp', None)
    cache_spec = P('dp', 'kv', None)
    slot_spec = P('dp', 'kv')
    vec_spec = P(None)
    mat_spec = P(None, None)
    half_dims = ROPE_DIM // 2
    freq_row = np.tile(ROPE_BASE ** (-np.arange(half_dims) / half_dims), 2).astype(np.float32)[None, :]

    def local_step(x_in, positions, k_cache, v_cache, slot_pos, norm_scale, w_q, w_k, w_v, w_o, b_o):
        batch, model = x_in.shape
        slots = k_cache.shape[1]
        window = slots * kv_size
        width = w_q.shape[1]
        chunks = batch // (UNIT * CHUNK_UNITS)
        hbm = pl.BlockSpec(memory_space=pltpu.HBM)
        vmem = pl.BlockSpec(memory_space=pltpu.VMEM)
        smem = pl.BlockSpec(memory_space=pltpu.SMEM)
        dma = pltpu.SemaphoreType.DMA
        per_chunk = [dma((chunks,))] * 4
        *held, x_new, k_new, v_new, sp_new = pl.pallas_call(
            functools.partial(attend_kernel, window),
            out_shape=(*([pltpu.VMEM((batch // PIECES, slots, HEAD_DIM), BF16)] * (2 * PIECES)), pltpu.VMEM((batch, model), BF16),
                       pltpu.VMEM((batch, HEAD_DIM), F32), pltpu.VMEM((batch, HEAD_DIM), F32), pltpu.VMEM((batch, slots), jnp.int32)),
            in_specs=[hbm] * 12,
            out_specs=(vmem,) * (2 * PIECES + 4),
            scratch_shapes=[
                pltpu.VMEM((batch // 128, 128), jnp.int32), pltpu.VMEM((1, 128), F32), pltpu.VMEM((batch, model), BF16), pltpu.VMEM((model,), BF16),
                pltpu.VMEM((model, HEAD_DIM), BF16), pltpu.VMEM((model, HEAD_DIM), BF16), pltpu.VMEM((model, width), BF16),
                pltpu.VMEM((batch, slots), jnp.int32), pltpu.VMEM((width, model), BF16), pltpu.VMEM((model,), BF16),
                pltpu.VMEM((batch, 128), F32), pltpu.VMEM((batch, model), F32), pltpu.VMEM((batch // UNIT, HEADS, UNIT, HEAD_DIM), F32),
                pltpu.VMEM((chunks, CHUNK_UNITS, PACKET, 128), F32), pltpu.VMEM((chunks, 2, PACKET, 128), F32),
                pltpu.VMEM((chunks, 2, PACKET, 128), F32), pltpu.VMEM((chunks, PACKET, 128), F32),
                pltpu.VMEM((chunks * UNIT, width), F32), pltpu.VMEM((kv_size, chunks * UNIT, model), F32),
                dma((10,)), dma((chunks,)), dma((chunks,)), *per_chunk, *([dma((2,))] * 6)],
            compiler_params=pltpu.CompilerParams(vmem_limit_bytes=16 << 20, collective_id=0, has_side_effects=True),
            name='attend',
        )(*[pltpu.with_memory_space_constraint(a, pltpu.HBM) for a in (
            positions.reshape(batch // 128, 128), jnp.asarray(freq_row), x_in, norm_scale, w_k, w_v, w_q, slot_pos,
            w_o, b_o, k_cache, v_cache)])
        x_out, k_out, v_out, slot_pos_out = pl.pallas_call(
            functools.partial(write_kernel, window),
            out_shape=(jax.ShapeDtypeStruct((batch, model), BF16), jax.ShapeDtypeStruct(k_cache.shape, BF16),
                       jax.ShapeDtypeStruct(v_cache.shape, BF16), jax.ShapeDtypeStruct((batch, slots), jnp.int32)),
            in_specs=[smem] + [vmem] * (2 * PIECES + 4),
            out_specs=(hbm,) * 4,
            scratch_shapes=[pltpu.VMEM((4, 16, slots, HEAD_DIM), BF16), pltpu.VMEM((4, 16, slots, HEAD_DIM), BF16), dma((2,)), dma((4,)), dma((4,))],
            compiler_params=pltpu.CompilerParams(vmem_limit_bytes=9 << 20),
            name='write',
        )(positions, k_new, v_new, x_new, sp_new, *held)
        return x_out, k_out, v_out, slot_pos_out

    return jax.shard_map(
        local_step,
        mesh=mesh,
        in_specs=(row_spec, P('dp'), cache_spec, cache_spec, slot_spec, vec_spec, mat_spec, mat_spec, mat_spec, mat_spec, vec_spec),
        out_specs=(row_spec, cache_spec, cache_spec, slot_spec),
        check_vma=False)
```

```python
import functools
import numpy as np
import jax
import jax.numpy as jnp
from jax import lax
from jax.experimental import pallas as pl
from jax.experimental.pallas import tpu as pltpu
from jax.sharding import PartitionSpec as P

HEADS = 4
HEAD_DIM = 256
ROPE_DIM = 128
ROPE_BASE = 10000.0
EPS = 1e-6
NEG_LARGE = -1e30
SCORE_SCALE = HEAD_DIM ** -0.5

UNIT = 8
CHUNK_UNITS = 4
ROWS = UNIT * HEADS
PACKET = 2 * ROWS + 8
PIECES = 2
FIRST_LAG = 2
SECOND_LAG = 5
RING = 4
AHEAD = 2
MESH = pl.DeviceIdType.MESH
F32 = jnp.float32
BF16 = jnp.bfloat16


def attend_kernel(window, pos_h, freq_h, x_h, ns_h, wk_h, wv_h, wq_h, sp_h, wo_h, bo_h, k_h, v_h,
                  *rest):
    k_vm, v_vm = rest[:PIECES], rest[PIECES:2 * PIECES]
    (x_own, k_new, v_new, sp_new,
                  pos, freq, x_in, ns, wk, wv, wq, sp, wo, bo,
                  pos_b, x_f, q_s, pk, rc1, cm, rc2, o_s,
                  in_sem, k_sem, v_sem, s1, r1, s2, r2) = rest[2 * PIECES:]
    me = lax.axis_index('kv')
    x_side, core = me // 2, me % 2
    over = {'kv': 2 * (1 - x_side) + core}
    beside = {'kv': 2 * x_side + 1 - core}
    batch, slots = sp.shape
    chunk = UNIT * CHUNK_UNITS
    chunks = batch // chunk

    barrier = pltpu.get_barrier_semaphore()
    pl.semaphore_signal(barrier, inc=1, device_id=over, device_id_type=MESH)
    pl.semaphore_signal(barrier, inc=1, device_id=beside, device_id_type=MESH)

    smalls = [pltpu.make_async_copy(src, dst, in_sem.at[n]) for n, (src, dst) in enumerate((
        (pos_h, pos), (freq_h, freq), (x_h, x_in), (ns_h, ns), (wk_h, wk), (wv_h, wv), (wq_h, wq), (sp_h, sp), (wo_h, wo), (bo_h, bo)))]

    span = chunks // PIECES

    def cache_copy(j, piece):
        rows, held = pl.ds(j * chunk, chunk), pl.ds((j - piece * span) * chunk, chunk)
        return (pltpu.make_async_copy(k_h.at[rows], k_vm[piece].at[held], k_sem.at[j]),
                pltpu.make_async_copy(v_h.at[rows], v_vm[piece].at[held], v_sem.at[j]))

    def read_ahead(first, last):
        for j in range(first, last):
            for copy in cache_copy(j, j // span):
                copy.start()

    for small in smalls[:8]:
        small.start()
    read_ahead(0, AHEAD)

    smalls[0].wait()
    smalls[1].wait()
    for r in range(batch // 128):
        row = pos[r:r + 1, :].astype(F32)
        pos_b[pl.ds(128 * r, 128), :] = jnp.transpose(jnp.broadcast_to(row, (128, 128)))
    angles = pos_b[...] * freq[...]
    low = lax.broadcasted_iota(jnp.int32, (batch, 128), 1) < ROPE_DIM // 2
    cos_t = jnp.cos(angles)
    sin_t = jnp.sin(angles)
    sin_t = jnp.where(low, -sin_t, sin_t)

    def rotate(first):
        return first * cos_t + pltpu.roll(first, ROPE_DIM // 2, 1) * sin_t

    smalls[2].wait()
    smalls[3].wait()
    x32 = x_in[...].astype(F32)
    x_f[...] = x32
    mean_sq = jnp.mean(x32 * x32, axis=-1, keepdims=True)
    normed = (x32 * lax.rsqrt(mean_sq + EPS) * (1.0 + ns[...].astype(F32)[None, :])).astype(BF16)
    smalls[4].wait()
    smalls[5].wait()
    k_row = jnp.dot(normed, wk[...], preferred_element_type=F32)
    k_new[:, :128] = rotate(k_row[:, :128]).astype(BF16).astype(F32)
    k_new[:, 128:] = k_row[:, 128:].astype(BF16).astype(F32)
    v_new[...] = jnp.dot(normed, wv[...], preferred_element_type=F32).astype(BF16).astype(F32)
    smalls[6].wait()
    for small in smalls[8:]:
        small.start()
    for h in range(HEADS):
        q_row = jnp.dot(normed, wq[:, h * HEAD_DIM:(h + 1) * HEAD_DIM], preferred_element_type=F32)
        q_s[:, h, :, :128] = rotate(q_row[:, :128]).reshape(batch // UNIT, UNIT, 128)
        q_s[:, h, :, 128:] = q_row[:, 128:].reshape(batch // UNIT, UNIT, 128)
    smalls[7].wait()
    pl.semaphore_wait(barrier, 2)

    lane = lax.broadcasted_iota(jnp.int32, (UNIT, 128), 1)
    row_seq = lax.broadcasted_iota(jnp.int32, (ROWS, 128), 0) % UNIT

    def scores_of(u, piece):
        keys = k_vm[piece][pl.ds(u * UNIT - piece * span * chunk, UNIT)].reshape(UNIT * slots, HEAD_DIM)
        q_b = q_s[u].reshape(ROWS, HEAD_DIM).astype(BF16)
        return q_b, lax.dot_general(q_b, keys, (((1,), (1,)), ((), ())), preferred_element_type=F32)

    def weights_of(u, q_b, all_scores):
        seqs = pl.ds(u * UNIT, UNIT)
        scores = all_scores[:, :slots]
        for s in range(1, UNIT):
            scores = jnp.where(row_seq == s, all_scores[:, s * slots:(s + 1) * slots], scores)
        p_now = pos_b[seqs, :].astype(jnp.int32)
        slot = (p_now & (window - 1)) - me * slots
        hit = lane == slot
        held = jnp.where(hit, p_now, sp[seqs, :])
        sp_new[seqs, :] = held
        age = p_now - held
        usable = (held >= 0) & (age >= 0) & (age < window)
        fresh = jnp.sum(q_b.astype(F32).reshape(HEADS, UNIT, HEAD_DIM) * k_new[seqs, :][None], axis=-1, keepdims=True)
        scores = jnp.where(hit[None], fresh, scores.reshape(HEADS, UNIT, slots)) * SCORE_SCALE
        scores = jnp.where(usable[None], scores, NEG_LARGE)
        top = jnp.max(scores, axis=-1, keepdims=True)
        weights = jnp.where(usable[None], jnp.exp(scores - top), 0.0)
        total = jnp.sum(weights, axis=-1, keepdims=True)
        fresh_weight = jnp.sum(jnp.where(hit[None], weights, 0.0), axis=-1, keepdims=True)
        kept = jnp.where(hit[None], 0.0, weights).reshape(ROWS, slots)
        spread = jnp.concatenate([jnp.where(row_seq == s, kept, 0.0).astype(BF16) for s in range(UNIT)], axis=1)
        return top, total, fresh_weight, spread

    def sums_of(u, piece, fresh_weight, spread):
        values = v_vm[piece][pl.ds(u * UNIT - piece * span * chunk, UNIT)].reshape(UNIT * slots, HEAD_DIM)
        sums = jnp.dot(spread, values, preferred_element_type=F32).reshape(HEADS, UNIT, HEAD_DIM)
        sums = sums + fresh_weight.astype(BF16).astype(F32) * v_new[pl.ds(u * UNIT, UNIT), :][None]
        return sums.reshape(ROWS, HEAD_DIM)

    def attend(j, piece):
        units = [j * CHUNK_UNITS + i for i in range(CHUNK_UNITS)]
        scored = [scores_of(u, piece) for u in units]
        weighed = [weights_of(u, *pair) for u, pair in zip(units, scored)]
        for i, u in enumerate(units):
            top, total, fresh_weight, spread = weighed[i]
            sums = sums_of(u, piece, fresh_weight, spread)
            pk[j, i, 0:ROWS, :] = sums[:, :128]
            pk[j, i, ROWS:2 * ROWS, :] = sums[:, 128:]
            tile = jnp.zeros((UNIT, 128), F32)
            for h in range(HEADS):
                tile = jnp.where(lane == h, top[h], jnp.where(lane == HEADS + h, total[h], tile))
            pk[j, i, 2 * ROWS:, :] = tile

    def merge(a, b):
        ta, tb = a[2 * ROWS:, :], b[2 * ROWS:, :]
        tile = jnp.maximum(ta, tb)
        ea, eb = jnp.exp(ta - tile), jnp.exp(tb - tile)
        parts, totals = [], []
        for h in range(HEADS):
            fa, fb = ea[:, h:h + 1], eb[:, h:h + 1]
            totals.append(fa * ta[:, HEADS + h:HEADS + h + 1] + fb * tb[:, HEADS + h:HEADS + h + 1])
            parts.append([fa * a[o + h * UNIT:o + (h + 1) * UNIT, :] + fb * b[o + h * UNIT:o + (h + 1) * UNIT, :] for o in (0, ROWS)])
        return tile, parts, totals

    def first_copy(j):
        return pltpu.make_async_remote_copy(pk.at[j, pl.ds(2 * (1 - core), 2)], rc1.at[j], s1.at[j], r1.at[j], device_id=beside, device_id_type=MESH)

    def second_copy(j):
        return pltpu.make_async_remote_copy(cm.at[j, 1 - x_side], rc2.at[j], s2.at[j], r2.at[j], device_id=over, device_id_type=MESH)

    def first_merge(j):
        first_copy(j).wait_recv()
        for i in range(2):
            tile, parts, totals = merge(pk[j, 2 * core + i], rc1[j, i])
            for h in range(HEADS):
                cm[j, i, h * UNIT:(h + 1) * UNIT, :] = parts[h][0]
                cm[j, i, ROWS + h * UNIT:ROWS + (h + 1) * UNIT, :] = parts[h][1]
                tile = jnp.where(lane == HEADS + h, totals[h], tile)
            cm[j, i, 2 * ROWS:, :] = tile
        second_copy(j).start()

    def second_merge(j):
        second_copy(j).wait_recv()
        _, parts, totals = merge(cm[j, x_side], rc2[j])
        rows = pl.ds(j * UNIT, UNIT)
        for h in range(HEADS):
            inverse = 1.0 / totals[h]
            o_s[rows, h * HEAD_DIM:h * HEAD_DIM + 128] = parts[h][0] * inverse
            o_s[rows, h * HEAD_DIM + 128:(h + 1) * HEAD_DIM] = parts[h][1] * inverse

    own_unit = 2 * core + x_side

    def project(first, last):
        rows = pl.ds(first * UNIT, (last - first) * UNIT)
        residual = jnp.concatenate([x_f[pl.ds(j * chunk + own_unit * UNIT, UNIT), :] for j in range(first, last)], axis=0)
        x_own[rows, :] = residual + jnp.dot(o_s[rows, :].astype(BF16), wo[...], preferred_element_type=F32) + bo[...].astype(F32)[None, :]

    def step(piece, j, carry):
        for copy in cache_copy(j, piece):
            copy.wait()
        attend(j, piece)
        first_copy(j).start()

        @pl.when(j >= FIRST_LAG)
        def _():
            first_merge(j - FIRST_LAG)

        @pl.when(j >= SECOND_LAG)
        def _():
            second_merge(j - SECOND_LAG)

        for ahead in range(PIECES):
            @pl.when((j + AHEAD < chunks) & ((j + AHEAD) // span == ahead))
            def _():
                for copy in cache_copy(j + AHEAD, ahead):
                    copy.start()

        return carry

    for piece in range(PIECES):
        lax.fori_loop(piece * span, (piece + 1) * span, functools.partial(step, piece), 0)
    for j in range(chunks - FIRST_LAG, chunks):
        first_merge(j)
    for small in smalls[8:]:
        small.wait()
    for j in range(chunks - SECOND_LAG, chunks - FIRST_LAG):
        second_merge(j)
    project(0, chunks - FIRST_LAG)
    for j in range(chunks - FIRST_LAG, chunks):
        second_merge(j)
    project(chunks - FIRST_LAG, chunks)

    def drain(j, carry):
        first_copy(j).wait_send()
        second_copy(j).wait_send()
        return carry

    lax.fori_loop(0, chunks, drain, 0)


def insert_rows(window, pos, new, held, out, ring, sem):
    me = lax.axis_index('kv')
    part, slots, _ = held[0].shape
    depth, chunk = ring.shape[:2]
    span = part // chunk
    tile_row = lax.broadcasted_iota(jnp.int32, (16, HEAD_DIM), 0)

    def copy_out(j):
        turn = lax.rem(j, depth)
        return pltpu.make_async_copy(ring.at[turn], out.at[pl.ds(j * chunk, chunk)], sem.at[turn])

    def step(piece, j, carry):
        turn = lax.rem(j, depth)

        @pl.when(j >= depth)
        def _():
            copy_out(j - depth).wait()

        def group(i, carry):
            for n in range(8):
                row = i * 8 + n
                b = j * chunk + row
                slot = (pos[b] & (window - 1)) - me * slots
                base = pl.multiple_of((jnp.clip(slot, 0, slots - 1) // 16) * 16, 16)
                ring[turn, row] = held[piece][b - piece * part]
                fresh = jnp.broadcast_to(new[pl.ds(b, 1), :], (16, HEAD_DIM))
                old = held[piece][b - piece * part, pl.ds(base, 16), :].astype(F32)
                ring[turn, row, pl.ds(base, 16), :] = jnp.where(tile_row == slot - base, fresh, old).astype(BF16)
            return carry
        lax.fori_loop(0, chunk // 8, group, 0)
        copy_out(j).start()
        return carry

    for piece in range(PIECES):
        lax.fori_loop(piece * span, (piece + 1) * span, functools.partial(step, piece), 0)
    for j in range(PIECES * span - depth, PIECES * span):
        copy_out(j).wait()


def write_keys_kernel(window, pos, k_new, sp_new, *rest):
    held = rest[:PIECES]
    k_out, sp_out, ring, sem, sp_sem = rest[PIECES:]
    copy = pltpu.make_async_copy(sp_new, sp_out, sp_sem)
    copy.start()
    insert_rows(window, pos, k_new, held, k_out, ring, sem)
    copy.wait()


def write_values_kernel(window, pos, v_new, x_own, x_beside, x_over, x_across, *rest):
    held = rest[:PIECES]
    v_out, x_out, ring, x_rows, x_new, sem, x_sem = rest[PIECES:]
    me = lax.axis_index('kv')
    for flip, rows in enumerate((x_own, x_beside, x_over, x_across)):
        x_side, core = (me // 2 + flip // 2) % 2, (me % 2 + flip % 2) % 2
        unit = 2 * core + x_side
        for j in range(rows.shape[0] // UNIT):
            x_rows[pl.ds(j * UNIT * CHUNK_UNITS + unit * UNIT, UNIT), :] = rows[j * UNIT:(j + 1) * UNIT, :]
    x_new[...] = x_rows[...].astype(BF16)
    copy = pltpu.make_async_copy(x_new, x_out, x_sem)
    copy.start()
    insert_rows(window, pos, v_new, held, v_out, ring, sem)
    copy.wait()


def solution(mesh):
    kv_size = mesh.shape['kv']
    row_spec = P('dp', None)
    cache_spec = P('dp', 'kv', None)
    slot_spec = P('dp', 'kv')
    vec_spec = P(None)
    mat_spec = P(None, None)
    half_dims = ROPE_DIM // 2
    freq_row = np.tile(ROPE_BASE ** (-np.arange(half_dims) / half_dims), 2).astype(np.float32)[None, :]

    def local_step(x_in, positions, k_cache, v_cache, slot_pos, norm_scale, w_q, w_k, w_v, w_o, b_o):
        batch, model = x_in.shape
        slots = k_cache.shape[1]
        window = slots * kv_size
        width = w_q.shape[1]
        chunks = batch // (UNIT * CHUNK_UNITS)
        hbm = pl.BlockSpec(memory_space=pltpu.HBM)
        vmem = pl.BlockSpec(memory_space=pltpu.VMEM)
        smem = pl.BlockSpec(memory_space=pltpu.SMEM)
        dma = pltpu.SemaphoreType.DMA
        per_chunk = [dma((chunks,))] * 4
        *held, x_own, k_new, v_new, sp_new = pl.pallas_call(
            functools.partial(attend_kernel, window),
            out_shape=(*([pltpu.VMEM((batch // PIECES, slots, HEAD_DIM), BF16)] * (2 * PIECES)), pltpu.VMEM((chunks * UNIT, model), F32),
                       pltpu.VMEM((batch, HEAD_DIM), F32), pltpu.VMEM((batch, HEAD_DIM), F32), pltpu.VMEM((batch, slots), jnp.int32)),
            in_specs=[hbm] * 12,
            out_specs=(vmem,) * (2 * PIECES + 4),
            scratch_shapes=[
                pltpu.VMEM((batch // 128, 128), jnp.int32), pltpu.VMEM((1, 128), F32), pltpu.VMEM((batch, model), BF16), pltpu.VMEM((model,), BF16),
                pltpu.VMEM((model, HEAD_DIM), BF16), pltpu.VMEM((model, HEAD_DIM), BF16), pltpu.VMEM((model, width), BF16),
                pltpu.VMEM((batch, slots), jnp.int32), pltpu.VMEM((width, model), BF16), pltpu.VMEM((model,), BF16),
                pltpu.VMEM((batch, 128), F32), pltpu.VMEM((batch, model), F32), pltpu.VMEM((batch // UNIT, HEADS, UNIT, HEAD_DIM), F32),
                pltpu.VMEM((chunks, CHUNK_UNITS, PACKET, 128), F32), pltpu.VMEM((chunks, 2, PACKET, 128), F32),
                pltpu.VMEM((chunks, 2, PACKET, 128), F32), pltpu.VMEM((chunks, PACKET, 128), F32),
                pltpu.VMEM((chunks * UNIT, width), F32),
                dma((10,)), dma((chunks,)), dma((chunks,)), *per_chunk],
            compiler_params=pltpu.CompilerParams(vmem_limit_bytes=16 << 20, collective_id=0, has_side_effects=True),
            name='attend',
        )(*[pltpu.with_memory_space_constraint(a, pltpu.HBM) for a in (
            positions.reshape(batch // 128, 128), jnp.asarray(freq_row), x_in, norm_scale, w_k, w_v, w_q, slot_pos,
            w_o, b_o, k_cache, v_cache)])
        x_beside, x_over, x_across = [lax.ppermute(x_own, 'kv', [(i, i ^ flip) for i in range(kv_size)]) for flip in range(1, kv_size)]
        traffic = pl.CostEstimate(flops=0, bytes_accessed=k_cache.size * 2, transcendentals=0)
        k_out, slot_pos_out = pl.pallas_call(
            functools.partial(write_keys_kernel, window),
            out_shape=(jax.ShapeDtypeStruct(k_cache.shape, BF16), jax.ShapeDtypeStruct((batch, slots), jnp.int32)),
            in_specs=[smem] + [vmem] * (PIECES + 2),
            out_specs=(hbm,) * 2,
            scratch_shapes=[pltpu.VMEM((RING, 16, slots, HEAD_DIM), BF16), dma((RING,)), dma],
            compiler_params=pltpu.CompilerParams(vmem_limit_bytes=7 << 20),
            cost_estimate=traffic,
            name='write_keys',
        )(positions, k_new, sp_new, *held[:PIECES])
        v_out, x_out = pl.pallas_call(
            functools.partial(write_values_kernel, window),
            out_shape=(jax.ShapeDtypeStruct(v_cache.shape, BF16), jax.ShapeDtypeStruct((batch, model), BF16)),
            in_specs=[smem] + [vmem] * (PIECES + 5),
            out_specs=(hbm,) * 2,
            scratch_shapes=[pltpu.VMEM((RING, 16, slots, HEAD_DIM), BF16), pltpu.VMEM((batch, model), F32), pltpu.VMEM((batch, model), BF16), dma((RING,)), dma],
            compiler_params=pltpu.CompilerParams(vmem_limit_bytes=7 << 20),
            cost_estimate=traffic,
            name='write_values',
        )(positions, v_new, x_own, x_beside, x_over, x_across, *held[PIECES:])
        return x_out, k_out, v_out, slot_pos_out

    return jax.shard_map(
        local_step,
        mesh=mesh,
        in_specs=(row_spec, P('dp'), cache_spec, cache_spec, slot_spec, vec_spec, mat_spec, mat_spec, mat_spec, mat_spec, vec_spec),
        out_specs=(row_spec, cache_spec, cache_spec, slot_spec),
        check_vma=False)
```

```python
import functools
import numpy as np
import jax
import jax.numpy as jnp
from jax import lax
from jax.experimental import pallas as pl
from jax.experimental.pallas import tpu as pltpu
from jax.sharding import PartitionSpec as P

HEADS = 4
HEAD_DIM = 256
ROPE_DIM = 128
ROPE_BASE = 10000.0
EPS = 1e-6
NEG_LARGE = -1e30
SCORE_SCALE = HEAD_DIM ** -0.5

UNIT = 8
CHUNK_UNITS = 2
ROWS = UNIT * HEADS
PACKET = 2 * ROWS + 8
SCATTER_GROUPS = ((0, 2), (2, 5))
WHOLE_GROUPS = ((10, 13), (13, 16))
PIECES = 2
FIRST_LAG = 2
SECOND_LAG = 8
SCATTERED = 10
MESH = pl.DeviceIdType.MESH
F32 = jnp.float32
BF16 = jnp.bfloat16


def attend_kernel(window, pos_h, freq_h, x_h, ns_h, wk_h, wv_h, wq_h, sp_h, wo_h, bo_h, k_h, v_h,
                  *rest):
    k_vm, v_vm = rest[:PIECES], rest[PIECES:2 * PIECES]
    (x_new, k_new, v_new, sp_new,
                  pos, freq, x_in, ns, wk, wv, wq, sp, wo, bo,
                  pos_b, x_f, q_s, pk, rc1, ch, o_s, ag, agd,
                  in_sem, k_sem, v_sem, s1, r1, s2, r2, sa, ra, sb, rb, sc, rc, sd, rd) = rest[2 * PIECES:]
    me = lax.axis_index('kv')
    x_side, core = me // 2, me % 2
    over = {'kv': 2 * (1 - x_side) + core}
    beside = {'kv': 2 * x_side + 1 - core}
    over_i = 2 * (1 - x_side) + core
    batch, slots = sp.shape
    chunk = UNIT * CHUNK_UNITS
    chunks = batch // chunk

    barrier = pltpu.get_barrier_semaphore()
    pl.semaphore_signal(barrier, inc=1, device_id=over, device_id_type=MESH)
    pl.semaphore_signal(barrier, inc=1, device_id=beside, device_id_type=MESH)

    smalls = [pltpu.make_async_copy(src, dst, in_sem.at[n]) for n, (src, dst) in enumerate((
        (pos_h, pos), (freq_h, freq), (x_h, x_in), (ns_h, ns), (wk_h, wk), (wv_h, wv), (wq_h, wq), (sp_h, sp), (wo_h, wo), (bo_h, bo)))]

    span = chunks // PIECES

    def cache_copy(j, piece):
        rows, held = pl.ds(j * chunk, chunk), pl.ds((j - piece * span) * chunk, chunk)
        return (pltpu.make_async_copy(k_h.at[rows], k_vm[piece].at[held], k_sem.at[j]),
                pltpu.make_async_copy(v_h.at[rows], v_vm[piece].at[held], v_sem.at[j]))

    def read_ahead(first, last):
        for j in range(first, last):
            for copy in cache_copy(j, j // span):
                copy.start()

    for small in smalls[:8]:
        small.start()
    read_ahead(0, 2)

    smalls[0].wait()
    smalls[1].wait()
    for r in range(batch // 128):
        row = pos[r:r + 1, :].astype(F32)
        pos_b[pl.ds(128 * r, 128), :] = jnp.transpose(jnp.broadcast_to(row, (128, 128)))
    angles = pos_b[...] * freq[...]
    low = lax.broadcasted_iota(jnp.int32, (batch, 128), 1) < ROPE_DIM // 2
    cos_t = jnp.cos(angles)
    sin_t = jnp.sin(angles)
    sin_t = jnp.where(low, -sin_t, sin_t)

    def rotate(first):
        return first * cos_t + pltpu.roll(first, ROPE_DIM // 2, 1) * sin_t

    read_ahead(2, 4)
    smalls[2].wait()
    smalls[3].wait()
    x32 = x_in[...].astype(F32)
    x_f[...] = x32
    mean_sq = jnp.mean(x32 * x32, axis=-1, keepdims=True)
    normed = (x32 * lax.rsqrt(mean_sq + EPS) * (1.0 + ns[...].astype(F32)[None, :])).astype(BF16)
    read_ahead(4, 6)
    smalls[4].wait()
    smalls[5].wait()
    read_ahead(6, 8)
    k_row = jnp.dot(normed, wk[...], preferred_element_type=F32)
    k_new[:, :128] = rotate(k_row[:, :128]).astype(BF16).astype(F32)
    k_new[:, 128:] = k_row[:, 128:].astype(BF16).astype(F32)
    v_new[...] = jnp.dot(normed, wv[...], preferred_element_type=F32).astype(BF16).astype(F32)
    smalls[6].wait()
    read_ahead(8, chunks)
    for small in smalls[8:]:
        small.start()
    for h in range(HEADS):
        q_row = jnp.dot(normed, wq[:, h * HEAD_DIM:(h + 1) * HEAD_DIM], preferred_element_type=F32)
        q_s[:, h, :, :128] = rotate(q_row[:, :128]).reshape(batch // UNIT, UNIT, 128)
        q_s[:, h, :, 128:] = q_row[:, 128:].reshape(batch // UNIT, UNIT, 128)
    smalls[7].wait()
    pl.semaphore_wait(barrier, 2)

    lane = lax.broadcasted_iota(jnp.int32, (UNIT, 128), 1)
    row_seq = lax.broadcasted_iota(jnp.int32, (ROWS, 128), 0) % UNIT

    def scores_of(u, piece):
        keys = k_vm[piece][pl.ds(u * UNIT - piece * span * chunk, UNIT)].reshape(UNIT * slots, HEAD_DIM)
        q_b = q_s[u].reshape(ROWS, HEAD_DIM).astype(BF16)
        return q_b, lax.dot_general(q_b, keys, (((1,), (1,)), ((), ())), preferred_element_type=F32)

    def weights_of(u, q_b, all_scores):
        seqs = pl.ds(u * UNIT, UNIT)
        scores = all_scores[:, :slots]
        for s in range(1, UNIT):
            scores = jnp.where(row_seq == s, all_scores[:, s * slots:(s + 1) * slots], scores)
        p_now = pos_b[seqs, :].astype(jnp.int32)
        slot = (p_now & (window - 1)) - me * slots
        hit = lane == slot
        held = jnp.where(hit, p_now, sp[seqs, :])
        sp_new[seqs, :] = held
        age = p_now - held
        usable = (held >= 0) & (age >= 0) & (age < window)
        fresh = jnp.sum(q_b.astype(F32).reshape(HEADS, UNIT, HEAD_DIM) * k_new[seqs, :][None], axis=-1, keepdims=True)
        scores = jnp.where(hit[None], fresh, scores.reshape(HEADS, UNIT, slots)) * SCORE_SCALE
        scores = jnp.where(usable[None], scores, NEG_LARGE)
        top = jnp.max(scores, axis=-1, keepdims=True)
        weights = jnp.where(usable[None], jnp.exp(scores - top), 0.0)
        total = jnp.sum(weights, axis=-1, keepdims=True)
        fresh_weight = jnp.sum(jnp.where(hit[None], weights, 0.0), axis=-1, keepdims=True)
        kept = jnp.where(hit[None], 0.0, weights).reshape(ROWS, slots)
        spread = jnp.concatenate([jnp.where(row_seq == s, kept, 0.0).astype(BF16) for s in range(UNIT)], axis=1)
        return top, total, fresh_weight, spread

    def sums_of(u, piece, fresh_weight, spread):
        values = v_vm[piece][pl.ds(u * UNIT - piece * span * chunk, UNIT)].reshape(UNIT * slots, HEAD_DIM)
        sums = jnp.dot(spread, values, preferred_element_type=F32).reshape(HEADS, UNIT, HEAD_DIM)
        sums = sums + fresh_weight.astype(BF16).astype(F32) * v_new[pl.ds(u * UNIT, UNIT), :][None]
        return sums.reshape(ROWS, HEAD_DIM)

    def attend(j, piece):
        units = [j * CHUNK_UNITS + i for i in range(CHUNK_UNITS)]
        scored = [scores_of(u, piece) for u in units]
        weighed = [weights_of(u, *pair) for u, pair in zip(units, scored)]
        for i, u in enumerate(units):
            top, total, fresh_weight, spread = weighed[i]
            sums = sums_of(u, piece, fresh_weight, spread)
            pk[j, i, 0:ROWS, :] = sums[:, :128]
            pk[j, i, ROWS:2 * ROWS, :] = sums[:, 128:]
            tile = jnp.zeros((UNIT, 128), F32)
            for h in range(HEADS):
                tile = jnp.where(lane == h, top[h], jnp.where(lane == HEADS + h, total[h], tile))
            pk[j, i, 2 * ROWS:, :] = tile

    def merge(a, b):
        ta, tb = a[2 * ROWS:, :], b[2 * ROWS:, :]
        tile = jnp.maximum(ta, tb)
        ea, eb = jnp.exp(ta - tile), jnp.exp(tb - tile)
        parts, totals = [], []
        for h in range(HEADS):
            fa, fb = ea[:, h:h + 1], eb[:, h:h + 1]
            totals.append(fa * ta[:, HEADS + h:HEADS + h + 1] + fb * tb[:, HEADS + h:HEADS + h + 1])
            parts.append([fa * a[o + h * UNIT:o + (h + 1) * UNIT, :] + fb * b[o + h * UNIT:o + (h + 1) * UNIT, :] for o in (0, ROWS)])
        return tile, parts, totals

    def first_copy(j):
        return pltpu.make_async_remote_copy(pk.at[j, 1 - core], rc1.at[j], s1.at[j], r1.at[j], device_id=beside, device_id_type=MESH)

    def second_copy(j):
        rows = ch.at[j, x_side]
        return pltpu.make_async_remote_copy(rows, rows, s2.at[j], r2.at[j], device_id=over, device_id_type=MESH)

    def first_merge(j):
        first_copy(j).wait_recv()
        tile, parts, totals = merge(pk[j, core], rc1[j])
        for h in range(HEADS):
            ch[j, x_side, h * UNIT:(h + 1) * UNIT, :] = parts[h][0]
            ch[j, x_side, ROWS + h * UNIT:ROWS + (h + 1) * UNIT, :] = parts[h][1]
            tile = jnp.where(lane == HEADS + h, totals[h], tile)
        ch[j, x_side, 2 * ROWS:, :] = tile

        @pl.when((j >= SCATTERED) | (j % 2 != x_side))
        def _():
            second_copy(j).start()

    def final_rows(j):
        return jnp.where(j < SCATTERED, j // 2, j - SCATTERED // 2) * UNIT

    def second_merge(j):
        @pl.when((j >= SCATTERED) | (j % 2 == x_side))
        def _():
            second_copy(j).wait_recv()
            _, parts, totals = merge(ch[j, 0], ch[j, 1])
            rows = pl.ds(pl.multiple_of((j // 2 if j < SCATTERED else j - SCATTERED // 2) * UNIT if isinstance(j, int) else final_rows(j), UNIT), UNIT)
            for h in range(HEADS):
                inverse = 1.0 / totals[h]
                o_s[rows, h * HEAD_DIM:h * HEAD_DIM + 128] = parts[h][0] * inverse
                o_s[rows, h * HEAD_DIM + 128:(h + 1) * HEAD_DIM] = parts[h][1] * inverse

    def project(first, residual):
        rows = pl.ds(first, residual.shape[0])
        return residual + jnp.dot(o_s[rows, :].astype(BF16), wo[...], preferred_element_type=F32) + bo[...].astype(F32)[None, :]

    def gather_copy(g, owner, target, send, recv):
        first, last = SCATTER_GROUPS[g]
        rows = ag.at[owner, pl.ds(first * UNIT, (last - first) * UNIT)]
        return pltpu.make_async_remote_copy(rows, rows, send.at[g], recv.at[g], device_id=target, device_id_type=MESH)

    def project_scattered(g):
        first, last = SCATTER_GROUPS[g]
        residual = jnp.concatenate([x_f[pl.ds((2 * i + x_side) * chunk + core * UNIT, UNIT), :] for i in range(first, last)], axis=0)
        ag[me, first * UNIT:last * UNIT, :] = project(first * UNIT, residual)
        gather_copy(g, me, over, sa, ra).start()
        gather_copy(g, me, beside, sb, rb).start()

    def forward(g):
        gather_copy(g, me, over, sa, ra).wait_recv()
        gather_copy(g, over_i, beside, sc, rc).start()

    def beside_copy(g):
        first, last = WHOLE_GROUPS[g]
        rows = agd.at[core, pl.ds((first - SCATTERED) * UNIT, (last - first) * UNIT)]
        return pltpu.make_async_remote_copy(rows, rows, sd.at[g], rd.at[g], device_id=beside, device_id_type=MESH)

    def project_whole(g):
        first, last = WHOLE_GROUPS[g]
        residual = jnp.concatenate([x_f[pl.ds(j * chunk + core * UNIT, UNIT), :] for j in range(first, last)], axis=0)
        agd[core, (first - SCATTERED) * UNIT:(last - SCATTERED) * UNIT, :] = project((first - SCATTERED // 2) * UNIT, residual)
        beside_copy(g).start()

    def step(piece, j, carry):
        for copy in cache_copy(j, piece):
            copy.wait()
        attend(j, piece)
        first_copy(j).start()

        @pl.when(j >= FIRST_LAG)
        def _():
            first_merge(j - FIRST_LAG)

        @pl.when(j >= SECOND_LAG)
        def _():
            second_merge(j - SECOND_LAG)

        @pl.when(j == 2 * SCATTER_GROUPS[0][1] - 1 + SECOND_LAG)
        def _():
            smalls[8].wait()
            smalls[9].wait()
            project_scattered(0)

        return carry

    for piece in range(PIECES):
        lax.fori_loop(piece * span, (piece + 1) * span, functools.partial(step, piece), 0)
    for j in range(chunks - FIRST_LAG, chunks):
        first_merge(j)
    done = chunks - SECOND_LAG
    for g in range(1, len(SCATTER_GROUPS)):
        for j in range(done, 2 * SCATTER_GROUPS[g][1]):
            second_merge(j)
        done = max(done, 2 * SCATTER_GROUPS[g][1])
        project_scattered(g)
    forward(0)
    for g in range(len(WHOLE_GROUPS)):
        for j in range(done, WHOLE_GROUPS[g][1]):
            second_merge(j)
        done = WHOLE_GROUPS[g][1]
        project_whole(g)
        if g == 0:
            for early in range(1, len(SCATTER_GROUPS)):
                forward(early)
    for g in range(len(SCATTER_GROUPS)):
        gather_copy(g, me, beside, sb, rb).wait_recv()
        gather_copy(g, me, beside, sc, rc).wait_recv()
    for j in range(SCATTERED):
        rows = [ag[2 * (j % 2) + c, j // 2 * UNIT:(j // 2 + 1) * UNIT, :] for c in range(2)]
        x_new[j * chunk:(j + 1) * chunk, :] = jnp.concatenate(rows, axis=0).astype(BF16)
    for g in range(len(WHOLE_GROUPS)):
        beside_copy(g).wait_recv()
        for j in range(*WHOLE_GROUPS[g]):
            rows = [agd[c, (j - SCATTERED) * UNIT:(j - SCATTERED + 1) * UNIT, :] for c in range(2)]
            x_new[j * chunk:(j + 1) * chunk, :] = jnp.concatenate(rows, axis=0).astype(BF16)

    def drain(j, carry):
        first_copy(j).wait_send()

        @pl.when((j >= SCATTERED) | (j % 2 != x_side))
        def _():
            second_copy(j).wait_send()
        return carry

    lax.fori_loop(0, chunks, drain, 0)
    for g in range(len(SCATTER_GROUPS)):
        gather_copy(g, me, over, sa, ra).wait_send()
        gather_copy(g, me, beside, sb, rb).wait_send()
        gather_copy(g, over_i, beside, sc, rc).wait_send()
    for g in range(len(WHOLE_GROUPS)):
        beside_copy(g).wait_send()


def write_kernel(window, pos, k_new, v_new, x_new, sp_new, *rest):
    k_vm, v_vm = rest[:PIECES], rest[PIECES:2 * PIECES]
    x_out, k_out, v_out, sp_out, k_ring, v_ring, sems, k_sem, v_sem = rest[2 * PIECES:]
    me = lax.axis_index('kv')
    part, slots, _ = k_vm[0].shape
    batch = part * PIECES
    depth, chunk = k_ring.shape[:2]
    chunks = batch // chunk
    span = chunks // PIECES
    others = (pltpu.make_async_copy(x_new, x_out, sems.at[0]), pltpu.make_async_copy(sp_new, sp_out, sems.at[1]))
    for copy in others:
        copy.start()
    tile_row = lax.broadcasted_iota(jnp.int32, (16, HEAD_DIM), 0)

    def copies(j):
        rows, ring = pl.ds(j * chunk, chunk), lax.rem(j, depth)
        return (pltpu.make_async_copy(k_ring.at[ring], k_out.at[rows], k_sem.at[ring]),
                pltpu.make_async_copy(v_ring.at[ring], v_out.at[rows], v_sem.at[ring]))

    def step(piece, j, carry):
        ring = lax.rem(j, depth)

        @pl.when(j >= depth)
        def _():
            for copy in copies(j - depth):
                copy.wait()

        def group(i, carry):
            for n in range(8):
                row = i * 8 + n
                b = j * chunk + row
                slot = (pos[b] & (window - 1)) - me * slots
                base = pl.multiple_of((jnp.clip(slot, 0, slots - 1) // 16) * 16, 16)
                for new, cache, out in ((k_new, k_vm[piece], k_ring), (v_new, v_vm[piece], v_ring)):
                    out[ring, row] = cache[b - piece * part]
                    fresh = jnp.broadcast_to(new[pl.ds(b, 1), :], (16, HEAD_DIM))
                    old = cache[b - piece * part, pl.ds(base, 16), :].astype(F32)
                    out[ring, row, pl.ds(base, 16), :] = jnp.where(tile_row == slot - base, fresh, old).astype(BF16)
            return carry
        lax.fori_loop(0, chunk // 8, group, 0)
        for copy in copies(j):
            copy.start()
        return carry

    for piece in range(PIECES):
        lax.fori_loop(piece * span, (piece + 1) * span, functools.partial(step, piece), 0)
    for j in range(chunks - depth, chunks):
        for copy in copies(j):
            copy.wait()
    for copy in others:
        copy.wait()


def solution(mesh):
    kv_size = mesh.shape['kv']
    row_spec = P('dp', None)
    cache_spec = P('dp', 'kv', None)
    slot_spec = P('dp', 'kv')
    vec_spec = P(None)
    mat_spec = P(None, None)
    half_dims = ROPE_DIM // 2
    freq_row = np.tile(ROPE_BASE ** (-np.arange(half_dims) / half_dims), 2).astype(np.float32)[None, :]

    def local_step(x_in, positions, k_cache, v_cache, slot_pos, norm_scale, w_q, w_k, w_v, w_o, b_o):
        batch, model = x_in.shape
        slots = k_cache.shape[1]
        window = slots * kv_size
        width = w_q.shape[1]
        chunks = batch // (UNIT * CHUNK_UNITS)
        hbm = pl.BlockSpec(memory_space=pltpu.HBM)
        vmem = pl.BlockSpec(memory_space=pltpu.VMEM)
        smem = pl.BlockSpec(memory_space=pltpu.SMEM)
        dma = pltpu.SemaphoreType.DMA
        per_chunk = [dma((chunks,))] * 4
        *held, x_new, k_new, v_new, sp_new = pl.pallas_call(
            functools.partial(attend_kernel, window),
            out_shape=(*([pltpu.VMEM((batch // PIECES, slots, HEAD_DIM), BF16)] * (2 * PIECES)), pltpu.VMEM((batch, model), BF16),
                       pltpu.VMEM((batch, HEAD_DIM), F32), pltpu.VMEM((batch, HEAD_DIM), F32), pltpu.VMEM((batch, slots), jnp.int32)),
            in_specs=[hbm] * 12,
            out_specs=(vmem,) * (2 * PIECES + 4),
            scratch_shapes=[
                pltpu.VMEM((batch // 128, 128), jnp.int32), pltpu.VMEM((1, 128), F32), pltpu.VMEM((batch, model), BF16), pltpu.VMEM((model,), BF16),
                pltpu.VMEM((model, HEAD_DIM), BF16), pltpu.VMEM((model, HEAD_DIM), BF16), pltpu.VMEM((model, width), BF16),
                pltpu.VMEM((batch, slots), jnp.int32), pltpu.VMEM((width, model), BF16), pltpu.VMEM((model,), BF16),
                pltpu.VMEM((batch, 128), F32), pltpu.VMEM((batch, model), F32), pltpu.VMEM((batch // UNIT, HEADS, UNIT, HEAD_DIM), F32),
                pltpu.VMEM((chunks, CHUNK_UNITS, PACKET, 128), F32), pltpu.VMEM((chunks, PACKET, 128), F32), pltpu.VMEM((chunks, 2, PACKET, 128), F32),
                pltpu.VMEM(((chunks - SCATTERED // 2) * UNIT, width), F32), pltpu.VMEM((kv_size, SCATTERED // 2 * UNIT, model), F32),
                pltpu.VMEM((2, (chunks - SCATTERED) * UNIT, model), F32),
                dma((10,)), dma((chunks,)), dma((chunks,)), *per_chunk, *([dma((len(SCATTER_GROUPS),))] * 6), *([dma((len(WHOLE_GROUPS),))] * 2)],
            compiler_params=pltpu.CompilerParams(vmem_limit_bytes=16 << 20, collective_id=0, has_side_effects=True),
            name='attend',
        )(*[pltpu.with_memory_space_constraint(a, pltpu.HBM) for a in (
            positions.reshape(batch // 128, 128), jnp.asarray(freq_row), x_in, norm_scale, w_k, w_v, w_q, slot_pos,
            w_o, b_o, k_cache, v_cache)])
        x_out, k_out, v_out, slot_pos_out = pl.pallas_call(
            functools.partial(write_kernel, window),
            out_shape=(jax.ShapeDtypeStruct((batch, model), BF16), jax.ShapeDtypeStruct(k_cache.shape, BF16),
                       jax.ShapeDtypeStruct(v_cache.shape, BF16), jax.ShapeDtypeStruct((batch, slots), jnp.int32)),
            in_specs=[smem] + [vmem] * (2 * PIECES + 4),
            out_specs=(hbm,) * 4,
            scratch_shapes=[pltpu.VMEM((4, 16, slots, HEAD_DIM), BF16), pltpu.VMEM((4, 16, slots, HEAD_DIM), BF16), dma((2,)), dma((4,)), dma((4,))],
            compiler_params=pltpu.CompilerParams(vmem_limit_bytes=9 << 20),
            name='write',
        )(positions, k_new, v_new, x_new, sp_new, *held)
        return x_out, k_out, v_out, slot_pos_out

    return jax.shard_map(
        local_step,
        mesh=mesh,
        in_specs=(row_spec, P('dp'), cache_spec, cache_spec, slot_spec, vec_spec, mat_spec, mat_spec, mat_spec, mat_spec, vec_spec),
        out_specs=(row_spec, cache_spec, cache_spec, slot_spec),
        check_vma=False)
```

```python
import functools
import numpy as np
import jax
import jax.numpy as jnp
from jax import lax
from jax.experimental import pallas as pl
from jax.experimental.pallas import tpu as pltpu
from jax.sharding import PartitionSpec as P

HEADS = 4
HEAD_DIM = 256
ROPE_DIM = 128
ROPE_BASE = 10000.0
EPS = 1e-6
NEG_LARGE = -1e30
SCORE_SCALE = HEAD_DIM ** -0.5

UNIT = 8
CHUNK_UNITS = 2
ROWS = UNIT * HEADS
PACKET = 2 * ROWS + 8
SCATTER_GROUPS = ((0, 2), (2, 5))
WHOLE_GROUPS = ((10, 13), (13, 16))
PIECES = 2
AHEAD = 4
FIRST_LAG = 2
SECOND_LAG = 8
SCATTERED = 10
MESH = pl.DeviceIdType.MESH
F32 = jnp.float32
BF16 = jnp.bfloat16


def attend_kernel(window, pos_h, freq_h, x_h, ns_h, wk_h, wv_h, wq_h, sp_h, wo_h, bo_h, k_h, v_h,
                  *rest):
    k_vm, v_vm = rest[:PIECES], rest[PIECES:2 * PIECES]
    (x_new, k_new, v_new, sp_new,
                  pos, freq, x_in, ns, wk, wv, wq, sp, wo, bo,
                  pos_b, x_f, q_s, pk, rc1, ch, o_s, ag, agd,
                  in_sem, k_sem, v_sem, s1, r1, s2, r2, sa, ra, sb, rb, sc, rc, sd, rd) = rest[2 * PIECES:]
    me = lax.axis_index('kv')
    x_side, core = me // 2, me % 2
    over = {'kv': 2 * (1 - x_side) + core}
    beside = {'kv': 2 * x_side + 1 - core}
    over_i = 2 * (1 - x_side) + core
    batch, slots = sp.shape
    chunk = UNIT * CHUNK_UNITS
    chunks = batch // chunk

    barrier = pltpu.get_barrier_semaphore()
    pl.semaphore_signal(barrier, inc=1, device_id=over, device_id_type=MESH)
    pl.semaphore_signal(barrier, inc=1, device_id=beside, device_id_type=MESH)

    smalls = [pltpu.make_async_copy(src, dst, in_sem.at[n]) for n, (src, dst) in enumerate((
        (pos_h, pos), (freq_h, freq), (x_h, x_in), (ns_h, ns), (wk_h, wk), (wv_h, wv), (wq_h, wq), (sp_h, sp), (wo_h, wo), (bo_h, bo)))]

    span = chunks // PIECES

    def cache_copy(j, piece):
        rows, held = pl.ds(j * chunk, chunk), pl.ds((j - piece * span) * chunk, chunk)
        return (pltpu.make_async_copy(k_h.at[rows], k_vm[piece].at[held], k_sem.at[j]),
                pltpu.make_async_copy(v_h.at[rows], v_vm[piece].at[held], v_sem.at[j]))

    def read_ahead(first, last):
        for j in range(first, last):
            for copy in cache_copy(j, j // span):
                copy.start()

    for small in smalls[:8]:
        small.start()
    read_ahead(0, 2)

    smalls[0].wait()
    smalls[1].wait()
    for r in range(batch // 128):
        row = pos[r:r + 1, :].astype(F32)
        pos_b[pl.ds(128 * r, 128), :] = jnp.transpose(jnp.broadcast_to(row, (128, 128)))
    read_ahead(2, AHEAD)
    angles = pos_b[...] * freq[...]
    low = lax.broadcasted_iota(jnp.int32, (batch, 128), 1) < ROPE_DIM // 2
    cos_t = jnp.cos(angles)
    sin_t = jnp.sin(angles)
    sin_t = jnp.where(low, -sin_t, sin_t)

    def rotate(first):
        return first * cos_t + pltpu.roll(first, ROPE_DIM // 2, 1) * sin_t

    smalls[2].wait()
    smalls[3].wait()
    x32 = x_in[...].astype(F32)
    x_f[...] = x32
    mean_sq = jnp.mean(x32 * x32, axis=-1, keepdims=True)
    normed = (x32 * lax.rsqrt(mean_sq + EPS) * (1.0 + ns[...].astype(F32)[None, :])).astype(BF16)
    smalls[4].wait()
    smalls[5].wait()
    k_row = jnp.dot(normed, wk[...], preferred_element_type=F32)
    k_new[:, :128] = rotate(k_row[:, :128]).astype(BF16).astype(F32)
    k_new[:, 128:] = k_row[:, 128:].astype(BF16).astype(F32)
    v_new[...] = jnp.dot(normed, wv[...], preferred_element_type=F32).astype(BF16).astype(F32)
    smalls[6].wait()
    for small in smalls[8:]:
        small.start()
    for h in range(HEADS):
        q_row = jnp.dot(normed, wq[:, h * HEAD_DIM:(h + 1) * HEAD_DIM], preferred_element_type=F32)
        q_s[:, h, :, :128] = rotate(q_row[:, :128]).reshape(batch // UNIT, UNIT, 128)
        q_s[:, h, :, 128:] = q_row[:, 128:].reshape(batch // UNIT, UNIT, 128)
    smalls[7].wait()
    pl.semaphore_wait(barrier, 2)

    lane = lax.broadcasted_iota(jnp.int32, (UNIT, 128), 1)
    row_seq = lax.broadcasted_iota(jnp.int32, (ROWS, 128), 0) % UNIT

    def scores_of(u, piece):
        keys = k_vm[piece][pl.ds(u * UNIT - piece * span * chunk, UNIT)].reshape(UNIT * slots, HEAD_DIM)
        q_b = q_s[u].reshape(ROWS, HEAD_DIM).astype(BF16)
        return q_b, lax.dot_general(q_b, keys, (((1,), (1,)), ((), ())), preferred_element_type=F32)

    def weights_of(u, q_b, all_scores):
        seqs = pl.ds(u * UNIT, UNIT)
        scores = all_scores[:, :slots]
        for s in range(1, UNIT):
            scores = jnp.where(row_seq == s, all_scores[:, s * slots:(s + 1) * slots], scores)
        p_now = pos_b[seqs, :].astype(jnp.int32)
        slot = (p_now & (window - 1)) - me * slots
        hit = lane == slot
        held = jnp.where(hit, p_now, sp[seqs, :])
        sp_new[seqs, :] = held
        age = p_now - held
        usable = (held >= 0) & (age >= 0) & (age < window)
        fresh = jnp.sum(q_b.astype(F32).reshape(HEADS, UNIT, HEAD_DIM) * k_new[seqs, :][None], axis=-1, keepdims=True)
        scores = jnp.where(hit[None], fresh, scores.reshape(HEADS, UNIT, slots)) * SCORE_SCALE
        scores = jnp.where(usable[None], scores, NEG_LARGE)
        top = jnp.max(scores, axis=-1, keepdims=True)
        weights = jnp.where(usable[None], jnp.exp(scores - top), 0.0)
        total = jnp.sum(weights, axis=-1, keepdims=True)
        fresh_weight = jnp.sum(jnp.where(hit[None], weights, 0.0), axis=-1, keepdims=True)
        kept = jnp.where(hit[None], 0.0, weights).reshape(ROWS, slots)
        spread = jnp.concatenate([jnp.where(row_seq == s, kept, 0.0).astype(BF16) for s in range(UNIT)], axis=1)
        return top, total, fresh_weight, spread

    def sums_of(u, piece, fresh_weight, spread):
        values = v_vm[piece][pl.ds(u * UNIT - piece * span * chunk, UNIT)].reshape(UNIT * slots, HEAD_DIM)
        sums = jnp.dot(spread, values, preferred_element_type=F32).reshape(HEADS, UNIT, HEAD_DIM)
        sums = sums + fresh_weight.astype(BF16).astype(F32) * v_new[pl.ds(u * UNIT, UNIT), :][None]
        return sums.reshape(ROWS, HEAD_DIM)

    def attend(j, piece):
        units = [j * CHUNK_UNITS + i for i in range(CHUNK_UNITS)]
        scored = [scores_of(u, piece) for u in units]
        weighed = [weights_of(u, *pair) for u, pair in zip(units, scored)]
        for i, u in enumerate(units):
            top, total, fresh_weight, spread = weighed[i]
            sums = sums_of(u, piece, fresh_weight, spread)
            pk[j, i, 0:ROWS, :] = sums[:, :128]
            pk[j, i, ROWS:2 * ROWS, :] = sums[:, 128:]
            tile = jnp.zeros((UNIT, 128), F32)
            for h in range(HEADS):
                tile = jnp.where(lane == h, top[h], jnp.where(lane == HEADS + h, total[h], tile))
            pk[j, i, 2 * ROWS:, :] = tile

    def merge(a, b):
        ta, tb = a[2 * ROWS:, :], b[2 * ROWS:, :]
        tile = jnp.maximum(ta, tb)
        ea, eb = jnp.exp(ta - tile), jnp.exp(tb - tile)
        parts, totals = [], []
        for h in range(HEADS):
            fa, fb = ea[:, h:h + 1], eb[:, h:h + 1]
            totals.append(fa * ta[:, HEADS + h:HEADS + h + 1] + fb * tb[:, HEADS + h:HEADS + h + 1])
            parts.append([fa * a[o + h * UNIT:o + (h + 1) * UNIT, :] + fb * b[o + h * UNIT:o + (h + 1) * UNIT, :] for o in (0, ROWS)])
        return tile, parts, totals

    def first_copy(j):
        return pltpu.make_async_remote_copy(pk.at[j, 1 - core], rc1.at[j], s1.at[j], r1.at[j], device_id=beside, device_id_type=MESH)

    def second_copy(j):
        rows = ch.at[j, x_side]
        return pltpu.make_async_remote_copy(rows, rows, s2.at[j], r2.at[j], device_id=over, device_id_type=MESH)

    def first_merge(j):
        first_copy(j).wait_recv()
        tile, parts, totals = merge(pk[j, core], rc1[j])
        for h in range(HEADS):
            ch[j, x_side, h * UNIT:(h + 1) * UNIT, :] = parts[h][0]
            ch[j, x_side, ROWS + h * UNIT:ROWS + (h + 1) * UNIT, :] = parts[h][1]
            tile = jnp.where(lane == HEADS + h, totals[h], tile)
        ch[j, x_side, 2 * ROWS:, :] = tile

        @pl.when((j >= SCATTERED) | (j % 2 != x_side))
        def _():
            second_copy(j).start()

    def final_rows(j):
        return jnp.where(j < SCATTERED, j // 2, j - SCATTERED // 2) * UNIT

    def second_merge(j):
        @pl.when((j >= SCATTERED) | (j % 2 == x_side))
        def _():
            second_copy(j).wait_recv()
            _, parts, totals = merge(ch[j, 0], ch[j, 1])
            rows = pl.ds(pl.multiple_of((j // 2 if j < SCATTERED else j - SCATTERED // 2) * UNIT if isinstance(j, int) else final_rows(j), UNIT), UNIT)
            for h in range(HEADS):
                inverse = 1.0 / totals[h]
                o_s[rows, h * HEAD_DIM:h * HEAD_DIM + 128] = parts[h][0] * inverse
                o_s[rows, h * HEAD_DIM + 128:(h + 1) * HEAD_DIM] = parts[h][1] * inverse

    def project(first, residual):
        rows = pl.ds(first, residual.shape[0])
        return residual + jnp.dot(o_s[rows, :].astype(BF16), wo[...], preferred_element_type=F32) + bo[...].astype(F32)[None, :]

    def gather_copy(g, owner, target, send, recv):
        first, last = SCATTER_GROUPS[g]
        rows = ag.at[owner, pl.ds(first * UNIT, (last - first) * UNIT)]
        return pltpu.make_async_remote_copy(rows, rows, send.at[g], recv.at[g], device_id=target, device_id_type=MESH)

    def project_scattered(g):
        first, last = SCATTER_GROUPS[g]
        residual = jnp.concatenate([x_f[pl.ds((2 * i + x_side) * chunk + core * UNIT, UNIT), :] for i in range(first, last)], axis=0)
        ag[me, first * UNIT:last * UNIT, :] = project(first * UNIT, residual)
        gather_copy(g, me, over, sa, ra).start()
        gather_copy(g, me, beside, sb, rb).start()

    def forward(g):
        gather_copy(g, me, over, sa, ra).wait_recv()
        gather_copy(g, over_i, beside, sc, rc).start()

    def beside_copy(g):
        first, last = WHOLE_GROUPS[g]
        rows = agd.at[core, pl.ds((first - SCATTERED) * UNIT, (last - first) * UNIT)]
        return pltpu.make_async_remote_copy(rows, rows, sd.at[g], rd.at[g], device_id=beside, device_id_type=MESH)

    def project_whole(g):
        first, last = WHOLE_GROUPS[g]
        residual = jnp.concatenate([x_f[pl.ds(j * chunk + core * UNIT, UNIT), :] for j in range(first, last)], axis=0)
        agd[core, (first - SCATTERED) * UNIT:(last - SCATTERED) * UNIT, :] = project((first - SCATTERED // 2) * UNIT, residual)
        beside_copy(g).start()

    def step(piece, j, carry):
        for copy in cache_copy(j, piece):
            copy.wait()
        attend(j, piece)
        first_copy(j).start()

        @pl.when(j >= FIRST_LAG)
        def _():
            first_merge(j - FIRST_LAG)

        @pl.when(j >= SECOND_LAG)
        def _():
            second_merge(j - SECOND_LAG)

        @pl.when(j == 2 * SCATTER_GROUPS[0][1] - 1 + SECOND_LAG)
        def _():
            smalls[8].wait()
            smalls[9].wait()
            project_scattered(0)

        for ahead in range(PIECES):
            @pl.when((j + AHEAD < chunks) & ((j + AHEAD) // span == ahead))
            def _():
                for copy in cache_copy(j + AHEAD, ahead):
                    copy.start()

        return carry

    for piece in range(PIECES):
        lax.fori_loop(piece * span, (piece + 1) * span, functools.partial(step, piece), 0)
    for j in range(chunks - FIRST_LAG, chunks):
        first_merge(j)
    done = chunks - SECOND_LAG
    for g in range(1, len(SCATTER_GROUPS)):
        for j in range(done, 2 * SCATTER_GROUPS[g][1]):
            second_merge(j)
        done = max(done, 2 * SCATTER_GROUPS[g][1])
        project_scattered(g)
    forward(0)
    for g in range(len(WHOLE_GROUPS)):
        for j in range(done, WHOLE_GROUPS[g][1]):
            second_merge(j)
        done = WHOLE_GROUPS[g][1]
        project_whole(g)
        if g == 0:
            for early in range(1, len(SCATTER_GROUPS)):
                forward(early)
    for g in range(len(SCATTER_GROUPS)):
        gather_copy(g, me, beside, sb, rb).wait_recv()
        gather_copy(g, me, beside, sc, rc).wait_recv()
    for j in range(SCATTERED):
        rows = [ag[2 * (j % 2) + c, j // 2 * UNIT:(j // 2 + 1) * UNIT, :] for c in range(2)]
        x_new[j * chunk:(j + 1) * chunk, :] = jnp.concatenate(rows, axis=0).astype(BF16)
    for g in range(len(WHOLE_GROUPS)):
        beside_copy(g).wait_recv()
        for j in range(*WHOLE_GROUPS[g]):
            rows = [agd[c, (j - SCATTERED) * UNIT:(j - SCATTERED + 1) * UNIT, :] for c in range(2)]
            x_new[j * chunk:(j + 1) * chunk, :] = jnp.concatenate(rows, axis=0).astype(BF16)

    def drain(j, carry):
        first_copy(j).wait_send()

        @pl.when((j >= SCATTERED) | (j % 2 != x_side))
        def _():
            second_copy(j).wait_send()
        return carry

    lax.fori_loop(0, chunks, drain, 0)
    for g in range(len(SCATTER_GROUPS)):
        gather_copy(g, me, over, sa, ra).wait_send()
        gather_copy(g, me, beside, sb, rb).wait_send()
        gather_copy(g, over_i, beside, sc, rc).wait_send()
    for g in range(len(WHOLE_GROUPS)):
        beside_copy(g).wait_send()


def write_kernel(window, pos, k_new, v_new, x_new, sp_new, *rest):
    k_vm, v_vm = rest[:PIECES], rest[PIECES:2 * PIECES]
    x_out, k_out, v_out, sp_out, k_ring, v_ring, sems, k_sem, v_sem = rest[2 * PIECES:]
    me = lax.axis_index('kv')
    part, slots, _ = k_vm[0].shape
    batch = part * PIECES
    depth, chunk = k_ring.shape[:2]
    chunks = batch // chunk
    span = chunks // PIECES
    others = (pltpu.make_async_copy(x_new, x_out, sems.at[0]), pltpu.make_async_copy(sp_new, sp_out, sems.at[1]))
    for copy in others:
        copy.start()
    tile_row = lax.broadcasted_iota(jnp.int32, (16, HEAD_DIM), 0)

    def copies(j):
        rows, ring = pl.ds(j * chunk, chunk), lax.rem(j, depth)
        return (pltpu.make_async_copy(k_ring.at[ring], k_out.at[rows], k_sem.at[ring]),
                pltpu.make_async_copy(v_ring.at[ring], v_out.at[rows], v_sem.at[ring]))

    def step(piece, j, carry):
        ring = lax.rem(j, depth)

        @pl.when(j >= depth)
        def _():
            for copy in copies(j - depth):
                copy.wait()

        def group(i, carry):
            for n in range(8):
                row = i * 8 + n
                b = j * chunk + row
                slot = (pos[b] & (window - 1)) - me * slots
                base = pl.multiple_of((jnp.clip(slot, 0, slots - 1) // 16) * 16, 16)
                for new, cache, out in ((k_new, k_vm[piece], k_ring), (v_new, v_vm[piece], v_ring)):
                    out[ring, row] = cache[b - piece * part]
                    fresh = jnp.broadcast_to(new[pl.ds(b, 1), :], (16, HEAD_DIM))
                    old = cache[b - piece * part, pl.ds(base, 16), :].astype(F32)
                    out[ring, row, pl.ds(base, 16), :] = jnp.where(tile_row == slot - base, fresh, old).astype(BF16)
            return carry
        lax.fori_loop(0, chunk // 8, group, 0)
        for copy in copies(j):
            copy.start()
        return carry

    for piece in range(PIECES):
        lax.fori_loop(piece * span, (piece + 1) * span, functools.partial(step, piece), 0)
    for j in range(chunks - depth, chunks):
        for copy in copies(j):
            copy.wait()
    for copy in others:
        copy.wait()


def solution(mesh):
    kv_size = mesh.shape['kv']
    row_spec = P('dp', None)
    cache_spec = P('dp', 'kv', None)
    slot_spec = P('dp', 'kv')
    vec_spec = P(None)
    mat_spec = P(None, None)
    half_dims = ROPE_DIM // 2
    freq_row = np.tile(ROPE_BASE ** (-np.arange(half_dims) / half_dims), 2).astype(np.float32)[None, :]

    def local_step(x_in, positions, k_cache, v_cache, slot_pos, norm_scale, w_q, w_k, w_v, w_o, b_o):
        batch, model = x_in.shape
        slots = k_cache.shape[1]
        window = slots * kv_size
        width = w_q.shape[1]
        chunks = batch // (UNIT * CHUNK_UNITS)
        hbm = pl.BlockSpec(memory_space=pltpu.HBM)
        vmem = pl.BlockSpec(memory_space=pltpu.VMEM)
        smem = pl.BlockSpec(memory_space=pltpu.SMEM)
        dma = pltpu.SemaphoreType.DMA
        per_chunk = [dma((chunks,))] * 4
        *held, x_new, k_new, v_new, sp_new = pl.pallas_call(
            functools.partial(attend_kernel, window),
            out_shape=(*([pltpu.VMEM((batch // PIECES, slots, HEAD_DIM), BF16)] * (2 * PIECES)), pltpu.VMEM((batch, model), BF16),
                       pltpu.VMEM((batch, HEAD_DIM), F32), pltpu.VMEM((batch, HEAD_DIM), F32), pltpu.VMEM((batch, slots), jnp.int32)),
            in_specs=[hbm] * 12,
            out_specs=(vmem,) * (2 * PIECES + 4),
            scratch_shapes=[
                pltpu.VMEM((batch // 128, 128), jnp.int32), pltpu.VMEM((1, 128), F32), pltpu.VMEM((batch, model), BF16), pltpu.VMEM((model,), BF16),
                pltpu.VMEM((model, HEAD_DIM), BF16), pltpu.VMEM((model, HEAD_DIM), BF16), pltpu.VMEM((model, width), BF16),
                pltpu.VMEM((batch, slots), jnp.int32), pltpu.VMEM((width, model), BF16), pltpu.VMEM((model,), BF16),
                pltpu.VMEM((batch, 128), F32), pltpu.VMEM((batch, model), F32), pltpu.VMEM((batch // UNIT, HEADS, UNIT, HEAD_DIM), F32),
                pltpu.VMEM((chunks, CHUNK_UNITS, PACKET, 128), F32), pltpu.VMEM((chunks, PACKET, 128), F32), pltpu.VMEM((chunks, 2, PACKET, 128), F32),
                pltpu.VMEM(((chunks - SCATTERED // 2) * UNIT, width), F32), pltpu.VMEM((kv_size, SCATTERED // 2 * UNIT, model), F32),
                pltpu.VMEM((2, (chunks - SCATTERED) * UNIT, model), F32),
                dma((10,)), dma((chunks,)), dma((chunks,)), *per_chunk, *([dma((len(SCATTER_GROUPS),))] * 6), *([dma((len(WHOLE_GROUPS),))] * 2)],
            compiler_params=pltpu.CompilerParams(vmem_limit_bytes=16 << 20, collective_id=0, has_side_effects=True),
            name='attend',
        )(*[pltpu.with_memory_space_constraint(a, pltpu.HBM) for a in (
            positions.reshape(batch // 128, 128), jnp.asarray(freq_row), x_in, norm_scale, w_k, w_v, w_q, slot_pos,
            w_o, b_o, k_cache, v_cache)])
        x_out, k_out, v_out, slot_pos_out = pl.pallas_call(
            functools.partial(write_kernel, window),
            out_shape=(jax.ShapeDtypeStruct((batch, model), BF16), jax.ShapeDtypeStruct(k_cache.shape, BF16),
                       jax.ShapeDtypeStruct(v_cache.shape, BF16), jax.ShapeDtypeStruct((batch, slots), jnp.int32)),
            in_specs=[smem] + [vmem] * (2 * PIECES + 4),
            out_specs=(hbm,) * 4,
            scratch_shapes=[pltpu.VMEM((4, 16, slots, HEAD_DIM), BF16), pltpu.VMEM((4, 16, slots, HEAD_DIM), BF16), dma((2,)), dma((4,)), dma((4,))],
            compiler_params=pltpu.CompilerParams(vmem_limit_bytes=9 << 20),
            name='write',
        )(positions, k_new, v_new, x_new, sp_new, *held)
        return x_out, k_out, v_out, slot_pos_out

    return jax.shard_map(
        local_step,
        mesh=mesh,
        in_specs=(row_spec, P('dp'), cache_spec, cache_spec, slot_spec, vec_spec, mat_spec, mat_spec, mat_spec, mat_spec, vec_spec),
        out_specs=(row_spec, cache_spec, cache_spec, slot_spec),
        check_vma=False)
```

```python
import functools
import numpy as np
import jax
import jax.numpy as jnp
from jax import lax
from jax.experimental import pallas as pl
from jax.experimental.pallas import tpu as pltpu
from jax.sharding import PartitionSpec as P

HEADS = 4
HEAD_DIM = 256
ROPE_DIM = 128
ROPE_BASE = 10000.0
EPS = 1e-6
NEG_LARGE = -1e30
SCORE_SCALE = HEAD_DIM ** -0.5

UNIT = 8
CHUNK_UNITS = 2
ROWS = UNIT * HEADS
PACKET = 2 * ROWS + 8
WHOLE_GROUPS = ((0, 4), (10, 13), (13, 16))
PIECES = 2
AHEAD = 4
FIRST_LAG = 3
SECOND_LAG = 12
SCATTER_FIRST, SCATTER_LAST = 4, 10
MESH = pl.DeviceIdType.MESH
F32 = jnp.float32
BF16 = jnp.bfloat16


def attend_kernel(window, pos_h, freq_h, x_h, ns_h, wk_h, wv_h, wq_h, sp_h, wo_h, bo_h, k_h, v_h,
                  *rest):
    k_vm, v_vm = rest[:PIECES], rest[PIECES:2 * PIECES]
    (x_new, k_new, v_new, sp_new,
                  pos, freq, x_in, ns, wk, wv, wq, sp, wo, bo,
                  pos_b, x_f, q_s, pk, rc1, ch, o_s, ag, agd,
                  in_sem, k_sem, v_sem, s1, r1, s2, r2, sa, ra, sd, rd) = rest[2 * PIECES:]
    me = lax.axis_index('kv')
    x_side, core = me // 2, me % 2
    over = {'kv': 2 * (1 - x_side) + core}
    beside = {'kv': 2 * x_side + 1 - core}
    over_i = 2 * (1 - x_side) + core
    batch, slots = sp.shape
    chunk = UNIT * CHUNK_UNITS
    chunks = batch // chunk

    barrier = pltpu.get_barrier_semaphore()
    pl.semaphore_signal(barrier, inc=1, device_id=over, device_id_type=MESH)
    pl.semaphore_signal(barrier, inc=1, device_id=beside, device_id_type=MESH)

    smalls = [pltpu.make_async_copy(src, dst, in_sem.at[n]) for n, (src, dst) in enumerate((
        (pos_h, pos), (freq_h, freq), (x_h, x_in), (ns_h, ns), (wk_h, wk), (wv_h, wv), (wq_h, wq), (sp_h, sp), (wo_h, wo), (bo_h, bo)))]

    span = chunks // PIECES

    def cache_copy(j, piece):
        rows, held = pl.ds(j * chunk, chunk), pl.ds((j - piece * span) * chunk, chunk)
        return (pltpu.make_async_copy(k_h.at[rows], k_vm[piece].at[held], k_sem.at[j]),
                pltpu.make_async_copy(v_h.at[rows], v_vm[piece].at[held], v_sem.at[j]))

    def read_ahead(first, last):
        for j in range(first, last):
            for copy in cache_copy(j, j // span):
                copy.start()

    for small in smalls[:8]:
        small.start()
    read_ahead(0, 1)

    smalls[0].wait()
    smalls[1].wait()
    for r in range(batch // 128):
        row = pos[r:r + 1, :].astype(F32)
        pos_b[pl.ds(128 * r, 128), :] = jnp.transpose(jnp.broadcast_to(row, (128, 128)))
    read_ahead(1, 2)
    angles = pos_b[...] * freq[...]
    low = lax.broadcasted_iota(jnp.int32, (batch, 128), 1) < ROPE_DIM // 2
    cos_t = jnp.cos(angles)
    sin_t = jnp.sin(angles)
    sin_t = jnp.where(low, -sin_t, sin_t)

    def rotate(first):
        return first * cos_t + pltpu.roll(first, ROPE_DIM // 2, 1) * sin_t

    smalls[2].wait()
    smalls[3].wait()
    read_ahead(2, AHEAD)
    x32 = x_in[...].astype(F32)
    x_f[...] = x32
    mean_sq = jnp.mean(x32 * x32, axis=-1, keepdims=True)
    normed = (x32 * lax.rsqrt(mean_sq + EPS) * (1.0 + ns[...].astype(F32)[None, :])).astype(BF16)
    smalls[4].wait()
    smalls[5].wait()
    k_row = jnp.dot(normed, wk[...], preferred_element_type=F32)
    k_new[:, :128] = rotate(k_row[:, :128]).astype(BF16).astype(F32)
    k_new[:, 128:] = k_row[:, 128:].astype(BF16).astype(F32)
    v_new[...] = jnp.dot(normed, wv[...], preferred_element_type=F32).astype(BF16).astype(F32)
    smalls[6].wait()
    for small in smalls[8:]:
        small.start()
    for h in range(HEADS):
        q_row = jnp.dot(normed, wq[:, h * HEAD_DIM:(h + 1) * HEAD_DIM], preferred_element_type=F32)
        q_s[:, h, :, :128] = rotate(q_row[:, :128]).reshape(batch // UNIT, UNIT, 128)
        q_s[:, h, :, 128:] = q_row[:, 128:].reshape(batch // UNIT, UNIT, 128)
    smalls[7].wait()
    pl.semaphore_wait(barrier, 2)

    lane = lax.broadcasted_iota(jnp.int32, (UNIT, 128), 1)
    row_seq = lax.broadcasted_iota(jnp.int32, (ROWS, 128), 0) % UNIT

    def scores_of(u, piece):
        keys = k_vm[piece][pl.ds(u * UNIT - piece * span * chunk, UNIT)].reshape(UNIT * slots, HEAD_DIM)
        q_b = q_s[u].reshape(ROWS, HEAD_DIM).astype(BF16)
        return q_b, lax.dot_general(q_b, keys, (((1,), (1,)), ((), ())), preferred_element_type=F32)

    def weights_of(u, q_b, all_scores):
        seqs = pl.ds(u * UNIT, UNIT)
        scores = all_scores[:, :slots]
        for s in range(1, UNIT):
            scores = jnp.where(row_seq == s, all_scores[:, s * slots:(s + 1) * slots], scores)
        p_now = pos_b[seqs, :].astype(jnp.int32)
        slot = (p_now & (window - 1)) - me * slots
        hit = lane == slot
        held = jnp.where(hit, p_now, sp[seqs, :])
        sp_new[seqs, :] = held
        age = p_now - held
        usable = (held >= 0) & (age >= 0) & (age < window)
        fresh = jnp.sum(q_b.astype(F32).reshape(HEADS, UNIT, HEAD_DIM) * k_new[seqs, :][None], axis=-1, keepdims=True)
        scores = jnp.where(hit[None], fresh, scores.reshape(HEADS, UNIT, slots)) * SCORE_SCALE
        scores = jnp.where(usable[None], scores, NEG_LARGE)
        top = jnp.max(scores, axis=-1, keepdims=True)
        weights = jnp.where(usable[None], jnp.exp(scores - top), 0.0)
        total = jnp.sum(weights, axis=-1, keepdims=True)
        fresh_weight = jnp.sum(jnp.where(hit[None], weights, 0.0), axis=-1, keepdims=True)
        kept = jnp.where(hit[None], 0.0, weights).reshape(ROWS, slots)
        spread = jnp.concatenate([jnp.where(row_seq == s, kept, 0.0).astype(BF16) for s in range(UNIT)], axis=1)
        return top, total, fresh_weight, spread

    def sums_of(u, piece, fresh_weight, spread):
        values = v_vm[piece][pl.ds(u * UNIT - piece * span * chunk, UNIT)].reshape(UNIT * slots, HEAD_DIM)
        sums = jnp.dot(spread, values, preferred_element_type=F32).reshape(HEADS, UNIT, HEAD_DIM)
        sums = sums + fresh_weight.astype(BF16).astype(F32) * v_new[pl.ds(u * UNIT, UNIT), :][None]
        return sums.reshape(ROWS, HEAD_DIM)

    def attend(j, piece):
        units = [j * CHUNK_UNITS + i for i in range(CHUNK_UNITS)]
        scored = [scores_of(u, piece) for u in units]
        weighed = [weights_of(u, *pair) for u, pair in zip(units, scored)]
        for i, u in enumerate(units):
            top, total, fresh_weight, spread = weighed[i]
            sums = sums_of(u, piece, fresh_weight, spread)
            pk[j, i, 0:ROWS, :] = sums[:, :128]
            pk[j, i, ROWS:2 * ROWS, :] = sums[:, 128:]
            tile = jnp.zeros((UNIT, 128), F32)
            for h in range(HEADS):
                tile = jnp.where(lane == h, top[h], jnp.where(lane == HEADS + h, total[h], tile))
            pk[j, i, 2 * ROWS:, :] = tile

    def merge(a, b):
        ta, tb = a[2 * ROWS:, :], b[2 * ROWS:, :]
        tile = jnp.maximum(ta, tb)
        ea, eb = jnp.exp(ta - tile), jnp.exp(tb - tile)
        parts, totals = [], []
        for h in range(HEADS):
            fa, fb = ea[:, h:h + 1], eb[:, h:h + 1]
            totals.append(fa * ta[:, HEADS + h:HEADS + h + 1] + fb * tb[:, HEADS + h:HEADS + h + 1])
            parts.append([fa * a[o + h * UNIT:o + (h + 1) * UNIT, :] + fb * b[o + h * UNIT:o + (h + 1) * UNIT, :] for o in (0, ROWS)])
        return tile, parts, totals

    def first_copy(j):
        return pltpu.make_async_remote_copy(pk.at[j, 1 - core], rc1.at[j], s1.at[j], r1.at[j], device_id=beside, device_id_type=MESH)

    def second_copy(j):
        rows = ch.at[j, x_side]
        return pltpu.make_async_remote_copy(rows, rows, s2.at[j], r2.at[j], device_id=over, device_id_type=MESH)

    def first_merge(j):
        first_copy(j).wait_recv()
        tile, parts, totals = merge(pk[j, core], rc1[j])
        for h in range(HEADS):
            ch[j, x_side, h * UNIT:(h + 1) * UNIT, :] = parts[h][0]
            ch[j, x_side, ROWS + h * UNIT:ROWS + (h + 1) * UNIT, :] = parts[h][1]
            tile = jnp.where(lane == HEADS + h, totals[h], tile)
        ch[j, x_side, 2 * ROWS:, :] = tile

        @pl.when((j < SCATTER_FIRST) | (j >= SCATTER_LAST) | (j % 2 != x_side))
        def _():
            second_copy(j).start()

    scattered = (SCATTER_LAST - SCATTER_FIRST) // 2

    def final_block(j):
        if isinstance(j, int):
            return j if j < SCATTER_FIRST else SCATTER_FIRST + (j - SCATTER_FIRST) // 2 if j < SCATTER_LAST else j - scattered
        return jnp.where(j < SCATTER_FIRST, j, jnp.where(j < SCATTER_LAST, SCATTER_FIRST + (j - SCATTER_FIRST) // 2, j - scattered))

    def whole_block(j):
        return j if j < SCATTER_FIRST else j - 2 * scattered

    def second_merge(j):
        @pl.when((j < SCATTER_FIRST) | (j >= SCATTER_LAST) | (j % 2 == x_side))
        def _():
            second_copy(j).wait_recv()
            _, parts, totals = merge(ch[j, 0], ch[j, 1])
            rows = pl.ds(final_block(j) * UNIT, UNIT)
            for h in range(HEADS):
                inverse = 1.0 / totals[h]
                o_s[rows, h * HEAD_DIM:h * HEAD_DIM + 128] = parts[h][0] * inverse
                o_s[rows, h * HEAD_DIM + 128:(h + 1) * HEAD_DIM] = parts[h][1] * inverse

    def project(first, residual):
        rows = pl.ds(first, residual.shape[0])
        return residual + jnp.dot(o_s[rows, :].astype(BF16), wo[...], preferred_element_type=F32) + bo[...].astype(F32)[None, :]

    def gather_copy(owner, target, n):
        rows = ag.at[owner]
        return pltpu.make_async_remote_copy(rows, rows, sa.at[n], ra.at[n], device_id=target, device_id_type=MESH)

    gather_over, gather_beside, gather_on = gather_copy(me, over, 0), gather_copy(me, beside, 1), gather_copy(over_i, beside, 2)

    def project_scattered():
        residual = jnp.concatenate([x_f[pl.ds((SCATTER_FIRST + 2 * i + x_side) * chunk + core * UNIT, UNIT), :] for i in range(scattered)], axis=0)
        ag[me] = project(SCATTER_FIRST * UNIT, residual)
        gather_over.start()
        gather_beside.start()

    def beside_copy(g):
        first, last = WHOLE_GROUPS[g]
        rows = agd.at[core, pl.ds(whole_block(first) * UNIT, (last - first) * UNIT)]
        return pltpu.make_async_remote_copy(rows, rows, sd.at[g], rd.at[g], device_id=beside, device_id_type=MESH)

    def project_whole(g):
        first, last = WHOLE_GROUPS[g]
        residual = jnp.concatenate([x_f[pl.ds(j * chunk + core * UNIT, UNIT), :] for j in range(first, last)], axis=0)
        agd[core, whole_block(first) * UNIT:whole_block(last - 1) * UNIT + UNIT, :] = project(final_block(first) * UNIT, residual)
        beside_copy(g).start()

    def collect_whole(g):
        beside_copy(g).wait_recv()
        for j in range(*WHOLE_GROUPS[g]):
            rows = [agd[c, whole_block(j) * UNIT:(whole_block(j) + 1) * UNIT, :] for c in range(2)]
            x_new[j * chunk:(j + 1) * chunk, :] = jnp.concatenate(rows, axis=0).astype(BF16)

    def step(piece, j, carry):
        for copy in cache_copy(j, piece):
            copy.wait()
        attend(j, piece)
        first_copy(j).start()

        @pl.when(j >= FIRST_LAG)
        def _():
            first_merge(j - FIRST_LAG)

        @pl.when(j >= SECOND_LAG)
        def _():
            second_merge(j - SECOND_LAG)

        for ahead in range(PIECES):
            @pl.when((j + AHEAD < chunks) & ((j + AHEAD) // span == ahead))
            def _():
                for copy in cache_copy(j + AHEAD, ahead):
                    copy.start()

        return carry

    for piece in range(PIECES):
        lax.fori_loop(piece * span, (piece + 1) * span, functools.partial(step, piece), 0)
    for j in range(chunks - FIRST_LAG, chunks):
        first_merge(j)
    for small in smalls[8:]:
        small.wait()
    for j in range(chunks - SECOND_LAG, SCATTER_LAST):
        second_merge(j)
    project_scattered()
    project_whole(0)
    for j in range(*WHOLE_GROUPS[1]):
        second_merge(j)
    project_whole(1)
    collect_whole(0)
    gather_over.wait_recv()
    gather_on.start()
    for g in range(2, len(WHOLE_GROUPS)):
        for j in range(*WHOLE_GROUPS[g]):
            second_merge(j)
        project_whole(g)
    collect_whole(1)
    gather_beside.wait_recv()
    gather_on.wait_recv()
    for j in range(SCATTER_FIRST, SCATTER_LAST):
        i = (j - SCATTER_FIRST) // 2
        rows = [ag[2 * (j % 2) + c, i * UNIT:(i + 1) * UNIT, :] for c in range(2)]
        x_new[j * chunk:(j + 1) * chunk, :] = jnp.concatenate(rows, axis=0).astype(BF16)
    for g in range(2, len(WHOLE_GROUPS)):
        collect_whole(g)

    def drain(j, carry):
        first_copy(j).wait_send()

        @pl.when((j < SCATTER_FIRST) | (j >= SCATTER_LAST) | (j % 2 != x_side))
        def _():
            second_copy(j).wait_send()
        return carry

    lax.fori_loop(0, chunks, drain, 0)
    for gather in (gather_over, gather_beside, gather_on):
        gather.wait_send()
    for g in range(len(WHOLE_GROUPS)):
        beside_copy(g).wait_send()


def write_kernel(window, pos, k_new, v_new, x_new, sp_new, *rest):
    k_vm, v_vm = rest[:PIECES], rest[PIECES:2 * PIECES]
    x_out, k_out, v_out, sp_out, k_ring, v_ring, sems, k_sem, v_sem = rest[2 * PIECES:]
    me = lax.axis_index('kv')
    part, slots, _ = k_vm[0].shape
    batch = part * PIECES
    depth, chunk = k_ring.shape[:2]
    chunks = batch // chunk
    span = chunks // PIECES
    others = (pltpu.make_async_copy(x_new, x_out, sems.at[0]), pltpu.make_async_copy(sp_new, sp_out, sems.at[1]))
    for copy in others:
        copy.start()
    tile_row = lax.broadcasted_iota(jnp.int32, (16, HEAD_DIM), 0)

    def copies(j):
        rows, ring = pl.ds(j * chunk, chunk), lax.rem(j, depth)
        return (pltpu.make_async_copy(k_ring.at[ring], k_out.at[rows], k_sem.at[ring]),
                pltpu.make_async_copy(v_ring.at[ring], v_out.at[rows], v_sem.at[ring]))

    def step(piece, j, carry):
        ring = lax.rem(j, depth)

        @pl.when(j >= depth)
        def _():
            for copy in copies(j - depth):
                copy.wait()

        def group(i, carry):
            for n in range(8):
                row = i * 8 + n
                b = j * chunk + row
                slot = (pos[b] & (window - 1)) - me * slots
                base = pl.multiple_of((jnp.clip(slot, 0, slots - 1) // 16) * 16, 16)
                for new, cache, out in ((k_new, k_vm[piece], k_ring), (v_new, v_vm[piece], v_ring)):
                    out[ring, row] = cache[b - piece * part]
                    fresh = jnp.broadcast_to(new[pl.ds(b, 1), :], (16, HEAD_DIM))
                    old = cache[b - piece * part, pl.ds(base, 16), :].astype(F32)
                    out[ring, row, pl.ds(base, 16), :] = jnp.where(tile_row == slot - base, fresh, old).astype(BF16)
            return carry
        lax.fori_loop(0, chunk // 8, group, 0)
        for copy in copies(j):
            copy.start()
        return carry

    for piece in range(PIECES):
        lax.fori_loop(piece * span, (piece + 1) * span, functools.partial(step, piece), 0)
    for j in range(chunks - depth, chunks):
        for copy in copies(j):
            copy.wait()
    for copy in others:
        copy.wait()


def solution(mesh):
    kv_size = mesh.shape['kv']
    row_spec = P('dp', None)
    cache_spec = P('dp', 'kv', None)
    slot_spec = P('dp', 'kv')
    vec_spec = P(None)
    mat_spec = P(None, None)
    half_dims = ROPE_DIM // 2
    freq_row = np.tile(ROPE_BASE ** (-np.arange(half_dims) / half_dims), 2).astype(np.float32)[None, :]

    def local_step(x_in, positions, k_cache, v_cache, slot_pos, norm_scale, w_q, w_k, w_v, w_o, b_o):
        batch, model = x_in.shape
        slots = k_cache.shape[1]
        window = slots * kv_size
        width = w_q.shape[1]
        chunks = batch // (UNIT * CHUNK_UNITS)
        scattered = (SCATTER_LAST - SCATTER_FIRST) // 2
        hbm = pl.BlockSpec(memory_space=pltpu.HBM)
        vmem = pl.BlockSpec(memory_space=pltpu.VMEM)
        smem = pl.BlockSpec(memory_space=pltpu.SMEM)
        dma = pltpu.SemaphoreType.DMA
        per_chunk = [dma((chunks,))] * 4
        *held, x_new, k_new, v_new, sp_new = pl.pallas_call(
            functools.partial(attend_kernel, window),
            out_shape=(*([pltpu.VMEM((batch // PIECES, slots, HEAD_DIM), BF16)] * (2 * PIECES)), pltpu.VMEM((batch, model), BF16),
                       pltpu.VMEM((batch, HEAD_DIM), F32), pltpu.VMEM((batch, HEAD_DIM), F32), pltpu.VMEM((batch, slots), jnp.int32)),
            in_specs=[hbm] * 12,
            out_specs=(vmem,) * (2 * PIECES + 4),
            scratch_shapes=[
                pltpu.VMEM((batch // 128, 128), jnp.int32), pltpu.VMEM((1, 128), F32), pltpu.VMEM((batch, model), BF16), pltpu.VMEM((model,), BF16),
                pltpu.VMEM((model, HEAD_DIM), BF16), pltpu.VMEM((model, HEAD_DIM), BF16), pltpu.VMEM((model, width), BF16),
                pltpu.VMEM((batch, slots), jnp.int32), pltpu.VMEM((width, model), BF16), pltpu.VMEM((model,), BF16),
                pltpu.VMEM((batch, 128), F32), pltpu.VMEM((batch, model), F32), pltpu.VMEM((batch // UNIT, HEADS, UNIT, HEAD_DIM), F32),
                pltpu.VMEM((chunks, CHUNK_UNITS, PACKET, 128), F32), pltpu.VMEM((chunks, PACKET, 128), F32), pltpu.VMEM((chunks, 2, PACKET, 128), F32),
                pltpu.VMEM(((chunks - scattered) * UNIT, width), F32), pltpu.VMEM((kv_size, scattered * UNIT, model), F32),
                pltpu.VMEM((2, (chunks - 2 * scattered) * UNIT, model), F32),
                dma((10,)), dma((chunks,)), dma((chunks,)), *per_chunk, dma((3,)), dma((3,)), *([dma((len(WHOLE_GROUPS),))] * 2)],
            compiler_params=pltpu.CompilerParams(vmem_limit_bytes=16 << 20, collective_id=0, has_side_effects=True),
            name='attend',
        )(*[pltpu.with_memory_space_constraint(a, pltpu.HBM) for a in (
            positions.reshape(batch // 128, 128), jnp.asarray(freq_row), x_in, norm_scale, w_k, w_v, w_q, slot_pos,
            w_o, b_o, k_cache, v_cache)])
        x_out, k_out, v_out, slot_pos_out = pl.pallas_call(
            functools.partial(write_kernel, window),
            out_shape=(jax.ShapeDtypeStruct((batch, model), BF16), jax.ShapeDtypeStruct(k_cache.shape, BF16),
                       jax.ShapeDtypeStruct(v_cache.shape, BF16), jax.ShapeDtypeStruct((batch, slots), jnp.int32)),
            in_specs=[smem] + [vmem] * (2 * PIECES + 4),
            out_specs=(hbm,) * 4,
            scratch_shapes=[pltpu.VMEM((4, 16, slots, HEAD_DIM), BF16), pltpu.VMEM((4, 16, slots, HEAD_DIM), BF16), dma((2,)), dma((4,)), dma((4,))],
            compiler_params=pltpu.CompilerParams(vmem_limit_bytes=9 << 20),
            name='write',
        )(positions, k_new, v_new, x_new, sp_new, *held)
        return x_out, k_out, v_out, slot_pos_out

    return jax.shard_map(
        local_step,
        mesh=mesh,
        in_specs=(row_spec, P('dp'), cache_spec, cache_spec, slot_spec, vec_spec, mat_spec, mat_spec, mat_spec, mat_spec, vec_spec),
        out_specs=(row_spec, cache_spec, cache_spec, slot_spec),
        check_vma=False)
```

```python
import functools
import numpy as np
import jax
import jax.numpy as jnp
from jax import lax
from jax.experimental import pallas as pl
from jax.experimental.pallas import tpu as pltpu
from jax.sharding import PartitionSpec as P

HEADS = 4
HEAD_DIM = 256
ROPE_DIM = 128
ROPE_BASE = 10000.0
EPS = 1e-6
NEG_LARGE = -1e30
SCORE_SCALE = HEAD_DIM ** -0.5

UNIT = 8
CHUNK_UNITS = 2
ROWS = UNIT * HEADS
PACKET = 2 * ROWS + 8
SCATTER_GROUPS = ((2, 6), (6, 12))
WHOLE_GROUPS = ((0, 2), (12, 14), (14, 16))
PIECES = 2
AHEAD = 6
FIRST_LAG = 2
SECOND_LAG = 10
SCATTER_FIRST, SCATTER_LAST = 2, 12
MESH = pl.DeviceIdType.MESH
F32 = jnp.float32
BF16 = jnp.bfloat16


def attend_kernel(window, pos_h, freq_h, x_h, ns_h, wk_h, wv_h, wq_h, sp_h, wo_h, bo_h, k_h, v_h,
                  *rest):
    k_vm, v_vm = rest[:PIECES], rest[PIECES:2 * PIECES]
    (x_new, k_new, v_new, sp_new,
                  pos, freq, x_in, ns, wk, wv, wq, sp, wo, bo,
                  pos_b, x_f, q_s, pk, rc1, ch, o_s, ag, agd,
                  in_sem, k_sem, v_sem, s1, r1, s2, r2, sa, ra, sd, rd) = rest[2 * PIECES:]
    me = lax.axis_index('kv')
    x_side, core = me // 2, me % 2
    over = {'kv': 2 * (1 - x_side) + core}
    beside = {'kv': 2 * x_side + 1 - core}
    over_i = 2 * (1 - x_side) + core
    batch, slots = sp.shape
    chunk = UNIT * CHUNK_UNITS
    chunks = batch // chunk

    barrier = pltpu.get_barrier_semaphore()
    pl.semaphore_signal(barrier, inc=1, device_id=over, device_id_type=MESH)
    pl.semaphore_signal(barrier, inc=1, device_id=beside, device_id_type=MESH)

    smalls = [pltpu.make_async_copy(src, dst, in_sem.at[n]) for n, (src, dst) in enumerate((
        (pos_h, pos), (freq_h, freq), (x_h, x_in), (ns_h, ns), (wk_h, wk), (wv_h, wv), (wq_h, wq), (sp_h, sp), (wo_h, wo), (bo_h, bo)))]

    span = chunks // PIECES

    def cache_copy(j, piece):
        rows, held = pl.ds(j * chunk, chunk), pl.ds((j - piece * span) * chunk, chunk)
        return (pltpu.make_async_copy(k_h.at[rows], k_vm[piece].at[held], k_sem.at[j]),
                pltpu.make_async_copy(v_h.at[rows], v_vm[piece].at[held], v_sem.at[j]))

    def read_ahead(first, last):
        for j in range(first, last):
            for copy in cache_copy(j, j // span):
                copy.start()

    for small in smalls[:8]:
        small.start()
    read_ahead(0, 1)

    smalls[0].wait()
    smalls[1].wait()
    for r in range(batch // 128):
        row = pos[r:r + 1, :].astype(F32)
        pos_b[pl.ds(128 * r, 128), :] = jnp.transpose(jnp.broadcast_to(row, (128, 128)))
    read_ahead(1, 2)
    angles = pos_b[...] * freq[...]
    low = lax.broadcasted_iota(jnp.int32, (batch, 128), 1) < ROPE_DIM // 2
    cos_t = jnp.cos(angles)
    sin_t = jnp.sin(angles)
    sin_t = jnp.where(low, -sin_t, sin_t)

    def rotate(first):
        return first * cos_t + pltpu.roll(first, ROPE_DIM // 2, 1) * sin_t

    smalls[2].wait()
    smalls[3].wait()
    read_ahead(2, AHEAD)
    x32 = x_in[...].astype(F32)
    x_f[...] = x32
    mean_sq = jnp.mean(x32 * x32, axis=-1, keepdims=True)
    normed = (x32 * lax.rsqrt(mean_sq + EPS) * (1.0 + ns[...].astype(F32)[None, :])).astype(BF16)
    smalls[4].wait()
    smalls[5].wait()
    k_row = jnp.dot(normed, wk[...], preferred_element_type=F32)
    k_new[:, :128] = rotate(k_row[:, :128]).astype(BF16).astype(F32)
    k_new[:, 128:] = k_row[:, 128:].astype(BF16).astype(F32)
    v_new[...] = jnp.dot(normed, wv[...], preferred_element_type=F32).astype(BF16).astype(F32)
    smalls[6].wait()
    for small in smalls[8:]:
        small.start()
    for h in range(HEADS):
        q_row = jnp.dot(normed, wq[:, h * HEAD_DIM:(h + 1) * HEAD_DIM], preferred_element_type=F32)
        q_s[:, h, :, :128] = rotate(q_row[:, :128]).reshape(batch // UNIT, UNIT, 128)
        q_s[:, h, :, 128:] = q_row[:, 128:].reshape(batch // UNIT, UNIT, 128)
    smalls[7].wait()
    pl.semaphore_wait(barrier, 2)

    lane = lax.broadcasted_iota(jnp.int32, (UNIT, 128), 1)
    row_seq = lax.broadcasted_iota(jnp.int32, (ROWS, 128), 0) % UNIT

    def scores_of(u, piece):
        keys = k_vm[piece][pl.ds(u * UNIT - piece * span * chunk, UNIT)].reshape(UNIT * slots, HEAD_DIM)
        q_b = q_s[u].reshape(ROWS, HEAD_DIM).astype(BF16)
        return q_b, lax.dot_general(q_b, keys, (((1,), (1,)), ((), ())), preferred_element_type=F32)

    def weights_of(u, q_b, all_scores):
        seqs = pl.ds(u * UNIT, UNIT)
        scores = all_scores[:, :slots]
        for s in range(1, UNIT):
            scores = jnp.where(row_seq == s, all_scores[:, s * slots:(s + 1) * slots], scores)
        p_now = pos_b[seqs, :].astype(jnp.int32)
        slot = (p_now & (window - 1)) - me * slots
        hit = lane == slot
        held = jnp.where(hit, p_now, sp[seqs, :])
        sp_new[seqs, :] = held
        age = p_now - held
        usable = (held >= 0) & (age >= 0) & (age < window)
        fresh = jnp.sum(q_b.astype(F32).reshape(HEADS, UNIT, HEAD_DIM) * k_new[seqs, :][None], axis=-1, keepdims=True)
        scores = jnp.where(hit[None], fresh, scores.reshape(HEADS, UNIT, slots)) * SCORE_SCALE
        scores = jnp.where(usable[None], scores, NEG_LARGE)
        top = jnp.max(scores, axis=-1, keepdims=True)
        weights = jnp.where(usable[None], jnp.exp(scores - top), 0.0)
        total = jnp.sum(weights, axis=-1, keepdims=True)
        fresh_weight = jnp.sum(jnp.where(hit[None], weights, 0.0), axis=-1, keepdims=True)
        kept = jnp.where(hit[None], 0.0, weights).reshape(ROWS, slots)
        spread = jnp.concatenate([jnp.where(row_seq == s, kept, 0.0).astype(BF16) for s in range(UNIT)], axis=1)
        return top, total, fresh_weight, spread

    def sums_of(u, piece, fresh_weight, spread):
        values = v_vm[piece][pl.ds(u * UNIT - piece * span * chunk, UNIT)].reshape(UNIT * slots, HEAD_DIM)
        sums = jnp.dot(spread, values, preferred_element_type=F32).reshape(HEADS, UNIT, HEAD_DIM)
        sums = sums + fresh_weight.astype(BF16).astype(F32) * v_new[pl.ds(u * UNIT, UNIT), :][None]
        return sums.reshape(ROWS, HEAD_DIM)

    def attend(j, piece):
        units = [j * CHUNK_UNITS + i for i in range(2 * CHUNK_UNITS)]
        scored = [scores_of(u, piece) for u in units]
        weighed = [weights_of(u, *pair) for u, pair in zip(units, scored)]
        for i, u in enumerate(units):
            top, total, fresh_weight, spread = weighed[i]
            sums = sums_of(u, piece, fresh_weight, spread)
            n, i = j + i // CHUNK_UNITS, i % CHUNK_UNITS
            pk[n, i, 0:ROWS, :] = sums[:, :128]
            pk[n, i, ROWS:2 * ROWS, :] = sums[:, 128:]
            tile = jnp.zeros((UNIT, 128), F32)
            for h in range(HEADS):
                tile = jnp.where(lane == h, top[h], jnp.where(lane == HEADS + h, total[h], tile))
            pk[n, i, 2 * ROWS:, :] = tile

    def merge(a, b):
        ta, tb = a[2 * ROWS:, :], b[2 * ROWS:, :]
        tile = jnp.maximum(ta, tb)
        ea, eb = jnp.exp(ta - tile), jnp.exp(tb - tile)
        parts, totals = [], []
        for h in range(HEADS):
            fa, fb = ea[:, h:h + 1], eb[:, h:h + 1]
            totals.append(fa * ta[:, HEADS + h:HEADS + h + 1] + fb * tb[:, HEADS + h:HEADS + h + 1])
            parts.append([fa * a[o + h * UNIT:o + (h + 1) * UNIT, :] + fb * b[o + h * UNIT:o + (h + 1) * UNIT, :] for o in (0, ROWS)])
        return tile, parts, totals

    def first_copy(j):
        return pltpu.make_async_remote_copy(pk.at[j, 1 - core], rc1.at[j], s1.at[j], r1.at[j], device_id=beside, device_id_type=MESH)

    def second_copy(j):
        rows = ch.at[j, x_side]
        return pltpu.make_async_remote_copy(rows, rows, s2.at[j], r2.at[j], device_id=over, device_id_type=MESH)

    def either(condition, yes, no):
        if isinstance(condition, bool):
            return yes() if condition else no()
        pl.when(condition)(yes)
        pl.when(jnp.logical_not(condition))(no)

    def is_whole(j):
        return (j < SCATTER_FIRST or j >= SCATTER_LAST) if isinstance(j, int) else (j < SCATTER_FIRST) | (j >= SCATTER_LAST)

    def first_merge(j):
        pair = (j, j + 1)
        for n in pair:
            first_copy(n).wait_recv()
        merged = [merge(pk[n, core], rc1[n]) for n in pair]
        for n, (tile, parts, totals) in zip(pair, merged):
            for h in range(HEADS):
                ch[n, x_side, h * UNIT:(h + 1) * UNIT, :] = parts[h][0]
                ch[n, x_side, ROWS + h * UNIT:ROWS + (h + 1) * UNIT, :] = parts[h][1]
                tile = jnp.where(lane == HEADS + h, totals[h], tile)
            ch[n, x_side, 2 * ROWS:, :] = tile

        def both():
            for n in pair:
                second_copy(n).start()

        either(is_whole(j), both, lambda: second_copy(j + 1 - x_side).start())

    scattered = (SCATTER_LAST - SCATTER_FIRST) // 2

    def final_block(j):
        if isinstance(j, int):
            return j if j < SCATTER_FIRST else SCATTER_FIRST + (j - SCATTER_FIRST) // 2 if j < SCATTER_LAST else j - scattered
        return jnp.where(j < SCATTER_FIRST, j, jnp.where(j < SCATTER_LAST, SCATTER_FIRST + (j - SCATTER_FIRST) // 2, j - scattered))

    def whole_block(j):
        return j if j < SCATTER_FIRST else j - 2 * scattered

    def finish(*chunk_ids):
        for n in chunk_ids:
            second_copy(n).wait_recv()
        merged = [merge(ch[n, 0], ch[n, 1]) for n in chunk_ids]
        for n, (_, parts, totals) in zip(chunk_ids, merged):
            rows = pl.ds(final_block(n) * UNIT, UNIT)
            for h in range(HEADS):
                inverse = 1.0 / totals[h]
                o_s[rows, h * HEAD_DIM:h * HEAD_DIM + 128] = parts[h][0] * inverse
                o_s[rows, h * HEAD_DIM + 128:(h + 1) * HEAD_DIM] = parts[h][1] * inverse

    def second_merge(j):
        either(is_whole(j), lambda: finish(j, j + 1), lambda: finish(j + x_side))

    def project(first, residual):
        rows = pl.ds(first, residual.shape[0])
        return residual + jnp.dot(o_s[rows, :].astype(BF16), wo[...], preferred_element_type=F32) + bo[...].astype(F32)[None, :]

    def gather_copy(g, owner, target, n):
        first, last = SCATTER_GROUPS[g]
        rows = ag.at[owner, pl.ds((first - SCATTER_FIRST) // 2 * UNIT, (last - first) // 2 * UNIT)]
        return pltpu.make_async_remote_copy(rows, rows, sa.at[g, n], ra.at[g, n], device_id=target, device_id_type=MESH)

    gathers = [(gather_copy(g, me, over, 0), gather_copy(g, me, beside, 1), gather_copy(g, over_i, beside, 2)) for g in range(len(SCATTER_GROUPS))]

    def project_scattered(g):
        first, last = SCATTER_GROUPS[g]
        residual = jnp.concatenate([x_f[pl.ds((n + x_side) * chunk + core * UNIT, UNIT), :] for n in range(first, last, 2)], axis=0)
        start = (first - SCATTER_FIRST) // 2 * UNIT
        ag[me, start:start + residual.shape[0], :] = project(SCATTER_FIRST * UNIT + start, residual)
        gathers[g][0].start()
        gathers[g][1].start()

    def forward(g):
        gathers[g][0].wait_recv()
        gathers[g][2].start()

    def collect_scattered(g):
        gathers[g][1].wait_recv()
        gathers[g][2].wait_recv()
        for j in range(*SCATTER_GROUPS[g]):
            i = (j - SCATTER_FIRST) // 2
            rows = [ag[2 * (j % 2) + c, i * UNIT:(i + 1) * UNIT, :] for c in range(2)]
            x_new[j * chunk:(j + 1) * chunk, :] = jnp.concatenate(rows, axis=0).astype(BF16)

    def beside_copy(g):
        first, last = WHOLE_GROUPS[g]
        rows = agd.at[core, pl.ds(whole_block(first) * UNIT, (last - first) * UNIT)]
        return pltpu.make_async_remote_copy(rows, rows, sd.at[g], rd.at[g], device_id=beside, device_id_type=MESH)

    def project_whole(g):
        first, last = WHOLE_GROUPS[g]
        residual = jnp.concatenate([x_f[pl.ds(j * chunk + core * UNIT, UNIT), :] for j in range(first, last)], axis=0)
        agd[core, whole_block(first) * UNIT:whole_block(last - 1) * UNIT + UNIT, :] = project(final_block(first) * UNIT, residual)
        beside_copy(g).start()

    def collect_whole(g):
        beside_copy(g).wait_recv()
        for j in range(*WHOLE_GROUPS[g]):
            rows = [agd[c, whole_block(j) * UNIT:(whole_block(j) + 1) * UNIT, :] for c in range(2)]
            x_new[j * chunk:(j + 1) * chunk, :] = jnp.concatenate(rows, axis=0).astype(BF16)

    def step(piece, block, carry):
        j = 2 * block
        for n in range(2):
            for copy in cache_copy(j + n, piece):
                copy.wait()
        attend(j, piece)
        for n in range(2):
            first_copy(j + n).start()

        @pl.when(j >= FIRST_LAG)
        def _():
            first_merge(j - FIRST_LAG)

        @pl.when(j >= SECOND_LAG)
        def _():
            second_merge(j - SECOND_LAG)

        for ahead in range(PIECES):
            @pl.when((j + AHEAD < chunks) & ((j + AHEAD) // span == ahead))
            def _():
                for n in range(2):
                    for copy in cache_copy(j + AHEAD + n, ahead):
                        copy.start()

        return carry

    for piece in range(PIECES):
        lax.fori_loop(piece * span // 2, (piece + 1) * span // 2, functools.partial(step, piece), 0)
    for small in smalls[8:]:
        small.wait()
    seconds = list(range(chunks - SECOND_LAG, chunks, 2))
    firsts = list(range(chunks - FIRST_LAG, chunks, 2))

    def second_upto(last):
        while seconds and seconds[0] < last:
            second_merge(seconds.pop(0))

    second_upto(SCATTER_GROUPS[0][1])
    project_scattered(0)
    for j in firsts:
        first_merge(j)
    project_whole(0)
    second_upto(SCATTER_GROUPS[1][1])
    project_scattered(1)
    forward(0)
    collect_whole(0)
    for g in range(1, len(WHOLE_GROUPS)):
        second_upto(WHOLE_GROUPS[g][1])
        project_whole(g)
        if g == 1:
            collect_scattered(0)
    forward(1)
    collect_scattered(1)
    for g in range(1, len(WHOLE_GROUPS)):
        collect_whole(g)

    def drain(j, carry):
        first_copy(j).wait_send()

        @pl.when((j < SCATTER_FIRST) | (j >= SCATTER_LAST) | (j % 2 != x_side))
        def _():
            second_copy(j).wait_send()
        return carry

    lax.fori_loop(0, chunks, drain, 0)
    for group in gathers:
        for gather in group:
            gather.wait_send()
    for g in range(len(WHOLE_GROUPS)):
        beside_copy(g).wait_send()


def write_kernel(window, pos, k_new, v_new, x_new, sp_new, *rest):
    k_vm, v_vm = rest[:PIECES], rest[PIECES:2 * PIECES]
    x_out, k_out, v_out, sp_out, k_ring, v_ring, sems, k_sem, v_sem = rest[2 * PIECES:]
    me = lax.axis_index('kv')
    part, slots, _ = k_vm[0].shape
    batch = part * PIECES
    depth, chunk = k_ring.shape[:2]
    chunks = batch // chunk
    span = chunks // PIECES
    others = (pltpu.make_async_copy(x_new, x_out, sems.at[0]), pltpu.make_async_copy(sp_new, sp_out, sems.at[1]))
    for copy in others:
        copy.start()
    tile_row = lax.broadcasted_iota(jnp.int32, (16, HEAD_DIM), 0)

    def copies(j):
        rows, ring = pl.ds(j * chunk, chunk), lax.rem(j, depth)
        return (pltpu.make_async_copy(k_ring.at[ring], k_out.at[rows], k_sem.at[ring]),
                pltpu.make_async_copy(v_ring.at[ring], v_out.at[rows], v_sem.at[ring]))

    def step(piece, j, carry):
        ring = lax.rem(j, depth)

        @pl.when(j >= depth)
        def _():
            for copy in copies(j - depth):
                copy.wait()

        def group(i, carry):
            for n in range(8):
                row = i * 8 + n
                b = j * chunk + row
                slot = (pos[b] & (window - 1)) - me * slots
                base = pl.multiple_of((jnp.clip(slot, 0, slots - 1) // 16) * 16, 16)
                for new, cache, out in ((k_new, k_vm[piece], k_ring), (v_new, v_vm[piece], v_ring)):
                    out[ring, row] = cache[b - piece * part]
                    fresh = jnp.broadcast_to(new[pl.ds(b, 1), :], (16, HEAD_DIM))
                    old = cache[b - piece * part, pl.ds(base, 16), :].astype(F32)
                    out[ring, row, pl.ds(base, 16), :] = jnp.where(tile_row == slot - base, fresh, old).astype(BF16)
            return carry
        lax.fori_loop(0, chunk // 8, group, 0)
        for copy in copies(j):
            copy.start()
        return carry

    for piece in range(PIECES):
        lax.fori_loop(piece * span, (piece + 1) * span, functools.partial(step, piece), 0)
    for j in range(chunks - depth, chunks):
        for copy in copies(j):
            copy.wait()
    for copy in others:
        copy.wait()


def solution(mesh):
    kv_size = mesh.shape['kv']
    row_spec = P('dp', None)
    cache_spec = P('dp', 'kv', None)
    slot_spec = P('dp', 'kv')
    vec_spec = P(None)
    mat_spec = P(None, None)
    half_dims = ROPE_DIM // 2
    freq_row = np.tile(ROPE_BASE ** (-np.arange(half_dims) / half_dims), 2).astype(np.float32)[None, :]

    def local_step(x_in, positions, k_cache, v_cache, slot_pos, norm_scale, w_q, w_k, w_v, w_o, b_o):
        batch, model = x_in.shape
        slots = k_cache.shape[1]
        window = slots * kv_size
        width = w_q.shape[1]
        chunks = batch // (UNIT * CHUNK_UNITS)
        scattered = (SCATTER_LAST - SCATTER_FIRST) // 2
        hbm = pl.BlockSpec(memory_space=pltpu.HBM)
        vmem = pl.BlockSpec(memory_space=pltpu.VMEM)
        smem = pl.BlockSpec(memory_space=pltpu.SMEM)
        dma = pltpu.SemaphoreType.DMA
        per_chunk = [dma((chunks,))] * 4
        *held, x_new, k_new, v_new, sp_new = pl.pallas_call(
            functools.partial(attend_kernel, window),
            out_shape=(*([pltpu.VMEM((batch // PIECES, slots, HEAD_DIM), BF16)] * (2 * PIECES)), pltpu.VMEM((batch, model), BF16),
                       pltpu.VMEM((batch, HEAD_DIM), F32), pltpu.VMEM((batch, HEAD_DIM), F32), pltpu.VMEM((batch, slots), jnp.int32)),
            in_specs=[hbm] * 12,
            out_specs=(vmem,) * (2 * PIECES + 4),
            scratch_shapes=[
                pltpu.VMEM((batch // 128, 128), jnp.int32), pltpu.VMEM((1, 128), F32), pltpu.VMEM((batch, model), BF16), pltpu.VMEM((model,), BF16),
                pltpu.VMEM((model, HEAD_DIM), BF16), pltpu.VMEM((model, HEAD_DIM), BF16), pltpu.VMEM((model, width), BF16),
                pltpu.VMEM((batch, slots), jnp.int32), pltpu.VMEM((width, model), BF16), pltpu.VMEM((model,), BF16),
                pltpu.VMEM((batch, 128), F32), pltpu.VMEM((batch, model), F32), pltpu.VMEM((batch // UNIT, HEADS, UNIT, HEAD_DIM), F32),
                pltpu.VMEM((chunks, CHUNK_UNITS, PACKET, 128), F32), pltpu.VMEM((chunks, PACKET, 128), F32), pltpu.VMEM((chunks, 2, PACKET, 128), F32),
                pltpu.VMEM(((chunks - scattered) * UNIT, width), F32), pltpu.VMEM((kv_size, scattered * UNIT, model), F32),
                pltpu.VMEM((2, (chunks - 2 * scattered) * UNIT, model), F32),
                dma((10,)), dma((chunks,)), dma((chunks,)), *per_chunk, *([dma((len(SCATTER_GROUPS), 3))] * 2), *([dma((len(WHOLE_GROUPS),))] * 2)],
            compiler_params=pltpu.CompilerParams(vmem_limit_bytes=16 << 20, collective_id=0, has_side_effects=True),
            name='attend',
        )(*[pltpu.with_memory_space_constraint(a, pltpu.HBM) for a in (
            positions.reshape(batch // 128, 128), jnp.asarray(freq_row), x_in, norm_scale, w_k, w_v, w_q, slot_pos,
            w_o, b_o, k_cache, v_cache)])
        x_out, k_out, v_out, slot_pos_out = pl.pallas_call(
            functools.partial(write_kernel, window),
            out_shape=(jax.ShapeDtypeStruct((batch, model), BF16), jax.ShapeDtypeStruct(k_cache.shape, BF16),
                       jax.ShapeDtypeStruct(v_cache.shape, BF16), jax.ShapeDtypeStruct((batch, slots), jnp.int32)),
            in_specs=[smem] + [vmem] * (2 * PIECES + 4),
            out_specs=(hbm,) * 4,
            scratch_shapes=[pltpu.VMEM((4, 16, slots, HEAD_DIM), BF16), pltpu.VMEM((4, 16, slots, HEAD_DIM), BF16), dma((2,)), dma((4,)), dma((4,))],
            compiler_params=pltpu.CompilerParams(vmem_limit_bytes=9 << 20),
            name='write',
        )(positions, k_new, v_new, x_new, sp_new, *held)
        return x_out, k_out, v_out, slot_pos_out

    return jax.shard_map(
        local_step,
        mesh=mesh,
        in_specs=(row_spec, P('dp'), cache_spec, cache_spec, slot_spec, vec_spec, mat_spec, mat_spec, mat_spec, mat_spec, vec_spec),
        out_specs=(row_spec, cache_spec, cache_spec, slot_spec),
        check_vma=False)
```

```python
import functools
import numpy as np
import jax
import jax.numpy as jnp
from jax import lax
from jax.experimental import pallas as pl
from jax.experimental.pallas import tpu as pltpu
from jax.sharding import PartitionSpec as P

HEADS = 4
HEAD_DIM = 256
ROPE_DIM = 128
ROPE_BASE = 10000.0
EPS = 1e-6
NEG_LARGE = -1e30
SCORE_SCALE = HEAD_DIM ** -0.5

UNIT = 8
CHUNK_UNITS = 2
ROWS = UNIT * HEADS
PACKET = 2 * ROWS + 8
SCATTER_GROUPS = ((2, 6), (6, 12))
WHOLE_GROUPS = ((0, 2), (12, 14), (14, 16))
PIECES = 2
AHEAD = 6
FIRST_LAG = 2
SCATTER_FIRST, SCATTER_LAST = 2, 12
MESH = pl.DeviceIdType.MESH
F32 = jnp.float32
BF16 = jnp.bfloat16


def attend_kernel(window, pos_h, freq_h, x_h, ns_h, wk_h, wv_h, wq_h, sp_h, wo_h, bo_h, k_h, v_h,
                  *rest):
    k_vm, v_vm = rest[:PIECES], rest[PIECES:2 * PIECES]
    (x_new, k_new, v_new, sp_new,
                  pos, freq, x_in, ns, wk, wv, wq, sp, wo, bo,
                  pos_b, x_f, q_s, sc_s, pk, rc1, ch, o_s, ag, agd,
                  in_sem, k_sem, v_sem, s1, r1, s2, r2, sa, ra, sd, rd) = rest[2 * PIECES:]
    me = lax.axis_index('kv')
    x_side, core = me // 2, me % 2
    over = {'kv': 2 * (1 - x_side) + core}
    beside = {'kv': 2 * x_side + 1 - core}
    over_i = 2 * (1 - x_side) + core
    batch, slots = sp.shape
    chunk = UNIT * CHUNK_UNITS
    chunks = batch // chunk

    barrier = pltpu.get_barrier_semaphore()
    pl.semaphore_signal(barrier, inc=1, device_id=over, device_id_type=MESH)
    pl.semaphore_signal(barrier, inc=1, device_id=beside, device_id_type=MESH)

    smalls = [pltpu.make_async_copy(src, dst, in_sem.at[n]) for n, (src, dst) in enumerate((
        (pos_h, pos), (freq_h, freq), (x_h, x_in), (ns_h, ns), (wk_h, wk), (wv_h, wv), (wq_h, wq), (sp_h, sp), (wo_h, wo), (bo_h, bo)))]

    span = chunks // PIECES

    def cache_copy(j, piece):
        rows, held = pl.ds(j * chunk, chunk), pl.ds((j - piece * span) * chunk, chunk)
        return (pltpu.make_async_copy(k_h.at[rows], k_vm[piece].at[held], k_sem.at[j]),
                pltpu.make_async_copy(v_h.at[rows], v_vm[piece].at[held], v_sem.at[j]))

    def read_ahead(first, last):
        for j in range(first, last):
            for copy in cache_copy(j, j // span):
                copy.start()

    for small in smalls[:8]:
        small.start()
    read_ahead(0, 1)

    smalls[0].wait()
    smalls[1].wait()
    for r in range(batch // 128):
        row = pos[r:r + 1, :].astype(F32)
        pos_b[pl.ds(128 * r, 128), :] = jnp.transpose(jnp.broadcast_to(row, (128, 128)))
    read_ahead(1, 2)
    angles = pos_b[...] * freq[...]
    low = lax.broadcasted_iota(jnp.int32, (batch, 128), 1) < ROPE_DIM // 2
    cos_t = jnp.cos(angles)
    sin_t = jnp.sin(angles)
    sin_t = jnp.where(low, -sin_t, sin_t)

    def rotate(first):
        return first * cos_t + pltpu.roll(first, ROPE_DIM // 2, 1) * sin_t

    smalls[2].wait()
    smalls[3].wait()
    read_ahead(2, AHEAD)
    x32 = x_in[...].astype(F32)
    x_f[...] = x32
    mean_sq = jnp.mean(x32 * x32, axis=-1, keepdims=True)
    normed = (x32 * lax.rsqrt(mean_sq + EPS) * (1.0 + ns[...].astype(F32)[None, :])).astype(BF16)
    smalls[4].wait()
    smalls[5].wait()
    k_row = jnp.dot(normed, wk[...], preferred_element_type=F32)
    k_new[:, :128] = rotate(k_row[:, :128]).astype(BF16).astype(F32)
    k_new[:, 128:] = k_row[:, 128:].astype(BF16).astype(F32)
    v_new[...] = jnp.dot(normed, wv[...], preferred_element_type=F32).astype(BF16).astype(F32)
    smalls[6].wait()
    for small in smalls[8:]:
        small.start()
    for h in range(HEADS):
        q_row = jnp.dot(normed, wq[:, h * HEAD_DIM:(h + 1) * HEAD_DIM], preferred_element_type=F32)
        q_s[:, h, :, :128] = rotate(q_row[:, :128]).reshape(batch // UNIT, UNIT, 128)
        q_s[:, h, :, 128:] = q_row[:, 128:].reshape(batch // UNIT, UNIT, 128)
    smalls[7].wait()
    pl.semaphore_wait(barrier, 2)

    lane = lax.broadcasted_iota(jnp.int32, (UNIT, 128), 1)
    row_seq = lax.broadcasted_iota(jnp.int32, (ROWS, 128), 0) % UNIT

    def scores_of(u, piece):
        keys = k_vm[piece][pl.ds(u * UNIT - piece * span * chunk, UNIT)].reshape(UNIT * slots, HEAD_DIM)
        q_b = q_s[u].reshape(ROWS, HEAD_DIM).astype(BF16)
        return q_b, lax.dot_general(q_b, keys, (((1,), (1,)), ((), ())), preferred_element_type=F32)

    def score(j, piece):
        for i in range(2 * CHUNK_UNITS):
            _, all_scores = scores_of(j * CHUNK_UNITS + i, piece)
            scores = all_scores[:, :slots]
            for s in range(1, UNIT):
                scores = jnp.where(row_seq == s, all_scores[:, s * slots:(s + 1) * slots], scores)
            sc_s[i] = scores

    def weights_of(u, scores):
        seqs = pl.ds(u * UNIT, UNIT)
        q_b = q_s[u].reshape(ROWS, HEAD_DIM).astype(BF16)
        p_now = pos_b[seqs, :].astype(jnp.int32)
        slot = (p_now & (window - 1)) - me * slots
        hit = lane == slot
        held = jnp.where(hit, p_now, sp[seqs, :])
        sp_new[seqs, :] = held
        age = p_now - held
        usable = (held >= 0) & (age >= 0) & (age < window)
        fresh = jnp.sum(q_b.astype(F32).reshape(HEADS, UNIT, HEAD_DIM) * k_new[seqs, :][None], axis=-1, keepdims=True)
        scores = jnp.where(hit[None], fresh, scores.reshape(HEADS, UNIT, slots)) * SCORE_SCALE
        scores = jnp.where(usable[None], scores, NEG_LARGE)
        top = jnp.max(scores, axis=-1, keepdims=True)
        weights = jnp.where(usable[None], jnp.exp(scores - top), 0.0)
        total = jnp.sum(weights, axis=-1, keepdims=True)
        fresh_weight = jnp.sum(jnp.where(hit[None], weights, 0.0), axis=-1, keepdims=True)
        kept = jnp.where(hit[None], 0.0, weights).reshape(ROWS, slots)
        spread = jnp.concatenate([jnp.where(row_seq == s, kept, 0.0).astype(BF16) for s in range(UNIT)], axis=1)
        return top, total, fresh_weight, spread

    def sums_of(u, piece, fresh_weight, spread):
        values = v_vm[piece][pl.ds(u * UNIT - piece * span * chunk, UNIT)].reshape(UNIT * slots, HEAD_DIM)
        sums = jnp.dot(spread, values, preferred_element_type=F32).reshape(HEADS, UNIT, HEAD_DIM)
        sums = sums + fresh_weight.astype(BF16).astype(F32) * v_new[pl.ds(u * UNIT, UNIT), :][None]
        return sums.reshape(ROWS, HEAD_DIM)

    def attend(j, piece, next_piece):
        units = [j * CHUNK_UNITS + i for i in range(2 * CHUNK_UNITS)]
        scored = [sc_s[i] for i in range(2 * CHUNK_UNITS)]
        weighed = [weights_of(u, scores) for u, scores in zip(units, scored)]
        if next_piece is not None:
            score(j + 2, next_piece)
        for i, u in enumerate(units):
            top, total, fresh_weight, spread = weighed[i]
            sums = sums_of(u, piece, fresh_weight, spread)
            n, i = j + i // CHUNK_UNITS, i % CHUNK_UNITS
            pk[n, i, 0:ROWS, :] = sums[:, :128]
            pk[n, i, ROWS:2 * ROWS, :] = sums[:, 128:]
            tile = jnp.zeros((UNIT, 128), F32)
            for h in range(HEADS):
                tile = jnp.where(lane == h, top[h], jnp.where(lane == HEADS + h, total[h], tile))
            pk[n, i, 2 * ROWS:, :] = tile

    def merge(a, b):
        ta, tb = a[2 * ROWS:, :], b[2 * ROWS:, :]
        tile = jnp.maximum(ta, tb)
        ea, eb = jnp.exp(ta - tile), jnp.exp(tb - tile)
        parts, totals = [], []
        for h in range(HEADS):
            fa, fb = ea[:, h:h + 1], eb[:, h:h + 1]
            totals.append(fa * ta[:, HEADS + h:HEADS + h + 1] + fb * tb[:, HEADS + h:HEADS + h + 1])
            parts.append([fa * a[o + h * UNIT:o + (h + 1) * UNIT, :] + fb * b[o + h * UNIT:o + (h + 1) * UNIT, :] for o in (0, ROWS)])
        return tile, parts, totals

    def first_copy(j):
        return pltpu.make_async_remote_copy(pk.at[j, 1 - core], rc1.at[j], s1.at[j], r1.at[j], device_id=beside, device_id_type=MESH)

    def second_copy(j):
        rows = ch.at[j, x_side]
        return pltpu.make_async_remote_copy(rows, rows, s2.at[j], r2.at[j], device_id=over, device_id_type=MESH)

    def either(condition, yes, no):
        if isinstance(condition, bool):
            return yes() if condition else no()
        pl.when(condition)(yes)
        pl.when(jnp.logical_not(condition))(no)

    def is_whole(j):
        return (j < SCATTER_FIRST or j >= SCATTER_LAST) if isinstance(j, int) else (j < SCATTER_FIRST) | (j >= SCATTER_LAST)

    def first_merge(j):
        pair = (j, j + 1)
        for n in pair:
            first_copy(n).wait_recv()
        merged = [merge(pk[n, core], rc1[n]) for n in pair]
        for n, (tile, parts, totals) in zip(pair, merged):
            for h in range(HEADS):
                ch[n, x_side, h * UNIT:(h + 1) * UNIT, :] = parts[h][0]
                ch[n, x_side, ROWS + h * UNIT:ROWS + (h + 1) * UNIT, :] = parts[h][1]
                tile = jnp.where(lane == HEADS + h, totals[h], tile)
            ch[n, x_side, 2 * ROWS:, :] = tile

        def both():
            for n in pair:
                second_copy(n).start()

        either(is_whole(j), both, lambda: second_copy(j + 1 - x_side).start())

    scattered = (SCATTER_LAST - SCATTER_FIRST) // 2

    def final_block(j):
        if isinstance(j, int):
            return j if j < SCATTER_FIRST else SCATTER_FIRST + (j - SCATTER_FIRST) // 2 if j < SCATTER_LAST else j - scattered
        return jnp.where(j < SCATTER_FIRST, j, jnp.where(j < SCATTER_LAST, SCATTER_FIRST + (j - SCATTER_FIRST) // 2, j - scattered))

    def whole_block(j):
        return j if j < SCATTER_FIRST else j - 2 * scattered

    def finish(*chunk_ids):
        for n in chunk_ids:
            second_copy(n).wait_recv()
        merged = [merge(ch[n, 0], ch[n, 1]) for n in chunk_ids]
        for n, (_, parts, totals) in zip(chunk_ids, merged):
            rows = pl.ds(final_block(n) * UNIT, UNIT)
            for h in range(HEADS):
                inverse = 1.0 / totals[h]
                o_s[rows, h * HEAD_DIM:h * HEAD_DIM + 128] = parts[h][0] * inverse
                o_s[rows, h * HEAD_DIM + 128:(h + 1) * HEAD_DIM] = parts[h][1] * inverse

    def second_merge(j):
        either(is_whole(j), lambda: finish(j, j + 1), lambda: finish(j + x_side))

    def project(first, residual):
        rows = pl.ds(first, residual.shape[0])
        return residual + jnp.dot(o_s[rows, :].astype(BF16), wo[...], preferred_element_type=F32) + bo[...].astype(F32)[None, :]

    def gather_copy(g, owner, target, n):
        first, last = SCATTER_GROUPS[g]
        rows = ag.at[owner, pl.ds((first - SCATTER_FIRST) // 2 * UNIT, (last - first) // 2 * UNIT)]
        return pltpu.make_async_remote_copy(rows, rows, sa.at[g, n], ra.at[g, n], device_id=target, device_id_type=MESH)

    gathers = [(gather_copy(g, me, over, 0), gather_copy(g, me, beside, 1), gather_copy(g, over_i, beside, 2)) for g in range(len(SCATTER_GROUPS))]

    def project_scattered(g):
        first, last = SCATTER_GROUPS[g]
        residual = jnp.concatenate([x_f[pl.ds((n + x_side) * chunk + core * UNIT, UNIT), :] for n in range(first, last, 2)], axis=0)
        start = (first - SCATTER_FIRST) // 2 * UNIT
        ag[me, start:start + residual.shape[0], :] = project(SCATTER_FIRST * UNIT + start, residual)
        gathers[g][0].start()
        gathers[g][1].start()

    def forward(g):
        gathers[g][0].wait_recv()
        gathers[g][2].start()

    def collect_scattered(g):
        gathers[g][1].wait_recv()
        gathers[g][2].wait_recv()
        for j in range(*SCATTER_GROUPS[g]):
            i = (j - SCATTER_FIRST) // 2
            rows = [ag[2 * (j % 2) + c, i * UNIT:(i + 1) * UNIT, :] for c in range(2)]
            x_new[j * chunk:(j + 1) * chunk, :] = jnp.concatenate(rows, axis=0).astype(BF16)

    def beside_copy(g):
        first, last = WHOLE_GROUPS[g]
        rows = agd.at[core, pl.ds(whole_block(first) * UNIT, (last - first) * UNIT)]
        return pltpu.make_async_remote_copy(rows, rows, sd.at[g], rd.at[g], device_id=beside, device_id_type=MESH)

    def project_whole(g):
        first, last = WHOLE_GROUPS[g]
        residual = jnp.concatenate([x_f[pl.ds(j * chunk + core * UNIT, UNIT), :] for j in range(first, last)], axis=0)
        agd[core, whole_block(first) * UNIT:whole_block(last - 1) * UNIT + UNIT, :] = project(final_block(first) * UNIT, residual)
        beside_copy(g).start()

    def collect_whole(g):
        beside_copy(g).wait_recv()
        for j in range(*WHOLE_GROUPS[g]):
            rows = [agd[c, whole_block(j) * UNIT:(whole_block(j) + 1) * UNIT, :] for c in range(2)]
            x_new[j * chunk:(j + 1) * chunk, :] = jnp.concatenate(rows, axis=0).astype(BF16)

    def step(piece, next_piece, block, carry):
        j = 2 * block
        for n in range(2):
            if next_piece is not None:
                cache_copy(j + 2 + n, next_piece)[0].wait()
            cache_copy(j + n, piece)[1].wait()
        attend(j, piece, next_piece)
        for n in range(2):
            first_copy(j + n).start()

        @pl.when(j >= FIRST_LAG)
        def _():
            first_merge(j - FIRST_LAG)

        for ahead in range(PIECES):
            @pl.when((j + AHEAD < chunks) & ((j + AHEAD) // span == ahead))
            def _():
                for n in range(2):
                    for copy in cache_copy(j + AHEAD + n, ahead):
                        copy.start()

        return carry

    for n in range(2):
        cache_copy(n, 0)[0].wait()
    score(0, 0)
    for piece in range(PIECES):
        last = (piece + 1) * span // 2 - 1
        lax.fori_loop(piece * span // 2, last, functools.partial(step, piece, piece), 0)
        lax.fori_loop(last, last + 1, functools.partial(step, piece, piece + 1 if piece + 1 < PIECES else None), 0)
    for small in smalls[8:]:
        small.wait()
    seconds = list(range(0, chunks, 2))
    firsts = list(range(chunks - FIRST_LAG, chunks, 2))

    def second_upto(last):
        while seconds and seconds[0] < last:
            second_merge(seconds.pop(0))

    second_upto(SCATTER_GROUPS[0][1])
    project_scattered(0)
    for j in firsts:
        first_merge(j)
    project_whole(0)
    second_upto(SCATTER_GROUPS[1][1])
    project_scattered(1)
    forward(0)
    collect_whole(0)
    for g in range(1, len(WHOLE_GROUPS)):
        second_upto(WHOLE_GROUPS[g][1])
        project_whole(g)
        if g == 1:
            collect_scattered(0)
    forward(1)
    collect_scattered(1)
    for g in range(1, len(WHOLE_GROUPS)):
        collect_whole(g)

    def drain(j, carry):
        first_copy(j).wait_send()

        @pl.when((j < SCATTER_FIRST) | (j >= SCATTER_LAST) | (j % 2 != x_side))
        def _():
            second_copy(j).wait_send()
        return carry

    lax.fori_loop(0, chunks, drain, 0)
    for group in gathers:
        for gather in group:
            gather.wait_send()
    for g in range(len(WHOLE_GROUPS)):
        beside_copy(g).wait_send()


def write_kernel(window, pos, k_new, v_new, x_new, sp_new, *rest):
    k_vm, v_vm = rest[:PIECES], rest[PIECES:2 * PIECES]
    x_out, k_out, v_out, sp_out, k_ring, v_ring, sems, k_sem, v_sem = rest[2 * PIECES:]
    me = lax.axis_index('kv')
    part, slots, _ = k_vm[0].shape
    batch = part * PIECES
    depth, chunk = k_ring.shape[:2]
    chunks = batch // chunk
    span = chunks // PIECES
    others = (pltpu.make_async_copy(x_new, x_out, sems.at[0]), pltpu.make_async_copy(sp_new, sp_out, sems.at[1]))
    for copy in others:
        copy.start()
    tile_row = lax.broadcasted_iota(jnp.int32, (16, HEAD_DIM), 0)

    def copies(j):
        rows, ring = pl.ds(j * chunk, chunk), lax.rem(j, depth)
        return (pltpu.make_async_copy(k_ring.at[ring], k_out.at[rows], k_sem.at[ring]),
                pltpu.make_async_copy(v_ring.at[ring], v_out.at[rows], v_sem.at[ring]))

    def step(piece, j, carry):
        ring = lax.rem(j, depth)

        @pl.when(j >= depth)
        def _():
            for copy in copies(j - depth):
                copy.wait()

        def group(i, carry):
            for n in range(8):
                row = i * 8 + n
                b = j * chunk + row
                slot = (pos[b] & (window - 1)) - me * slots
                base = pl.multiple_of((jnp.clip(slot, 0, slots - 1) // 16) * 16, 16)
                for new, cache, out in ((k_new, k_vm[piece], k_ring), (v_new, v_vm[piece], v_ring)):
                    out[ring, row] = cache[b - piece * part]
                    fresh = jnp.broadcast_to(new[pl.ds(b, 1), :], (16, HEAD_DIM))
                    old = cache[b - piece * part, pl.ds(base, 16), :].astype(F32)
                    out[ring, row, pl.ds(base, 16), :] = jnp.where(tile_row == slot - base, fresh, old).astype(BF16)
            return carry
        lax.fori_loop(0, chunk // 8, group, 0)
        for copy in copies(j):
            copy.start()
        return carry

    for piece in range(PIECES):
        lax.fori_loop(piece * span, (piece + 1) * span, functools.partial(step, piece), 0)
    for j in range(chunks - depth, chunks):
        for copy in copies(j):
            copy.wait()
    for copy in others:
        copy.wait()


def solution(mesh):
    kv_size = mesh.shape['kv']
    row_spec = P('dp', None)
    cache_spec = P('dp', 'kv', None)
    slot_spec = P('dp', 'kv')
    vec_spec = P(None)
    mat_spec = P(None, None)
    half_dims = ROPE_DIM // 2
    freq_row = np.tile(ROPE_BASE ** (-np.arange(half_dims) / half_dims), 2).astype(np.float32)[None, :]

    def local_step(x_in, positions, k_cache, v_cache, slot_pos, norm_scale, w_q, w_k, w_v, w_o, b_o):
        batch, model = x_in.shape
        slots = k_cache.shape[1]
        window = slots * kv_size
        width = w_q.shape[1]
        chunks = batch // (UNIT * CHUNK_UNITS)
        scattered = (SCATTER_LAST - SCATTER_FIRST) // 2
        hbm = pl.BlockSpec(memory_space=pltpu.HBM)
        vmem = pl.BlockSpec(memory_space=pltpu.VMEM)
        smem = pl.BlockSpec(memory_space=pltpu.SMEM)
        dma = pltpu.SemaphoreType.DMA
        per_chunk = [dma((chunks,))] * 4
        *held, x_new, k_new, v_new, sp_new = pl.pallas_call(
            functools.partial(attend_kernel, window),
            out_shape=(*([pltpu.VMEM((batch // PIECES, slots, HEAD_DIM), BF16)] * (2 * PIECES)), pltpu.VMEM((batch, model), BF16),
                       pltpu.VMEM((batch, HEAD_DIM), F32), pltpu.VMEM((batch, HEAD_DIM), F32), pltpu.VMEM((batch, slots), jnp.int32)),
            in_specs=[hbm] * 12,
            out_specs=(vmem,) * (2 * PIECES + 4),
            scratch_shapes=[
                pltpu.VMEM((batch // 128, 128), jnp.int32), pltpu.VMEM((1, 128), F32), pltpu.VMEM((batch, model), BF16), pltpu.VMEM((model,), BF16),
                pltpu.VMEM((model, HEAD_DIM), BF16), pltpu.VMEM((model, HEAD_DIM), BF16), pltpu.VMEM((model, width), BF16),
                pltpu.VMEM((batch, slots), jnp.int32), pltpu.VMEM((width, model), BF16), pltpu.VMEM((model,), BF16),
                pltpu.VMEM((batch, 128), F32), pltpu.VMEM((batch, model), F32), pltpu.VMEM((batch // UNIT, HEADS, UNIT, HEAD_DIM), F32),
                pltpu.VMEM((2 * CHUNK_UNITS, ROWS, slots), F32),
                pltpu.VMEM((chunks, CHUNK_UNITS, PACKET, 128), F32), pltpu.VMEM((chunks, PACKET, 128), F32), pltpu.VMEM((chunks, 2, PACKET, 128), F32),
                pltpu.VMEM(((chunks - scattered) * UNIT, width), F32), pltpu.VMEM((kv_size, scattered * UNIT, model), F32),
                pltpu.VMEM((2, (chunks - 2 * scattered) * UNIT, model), F32),
                dma((10,)), dma((chunks,)), dma((chunks,)), *per_chunk, *([dma((len(SCATTER_GROUPS), 3))] * 2), *([dma((len(WHOLE_GROUPS),))] * 2)],
            compiler_params=pltpu.CompilerParams(vmem_limit_bytes=16 << 20, collective_id=0, has_side_effects=True),
            name='attend',
        )(*[pltpu.with_memory_space_constraint(a, pltpu.HBM) for a in (
            positions.reshape(batch // 128, 128), jnp.asarray(freq_row), x_in, norm_scale, w_k, w_v, w_q, slot_pos,
            w_o, b_o, k_cache, v_cache)])
        x_out, k_out, v_out, slot_pos_out = pl.pallas_call(
            functools.partial(write_kernel, window),
            out_shape=(jax.ShapeDtypeStruct((batch, model), BF16), jax.ShapeDtypeStruct(k_cache.shape, BF16),
                       jax.ShapeDtypeStruct(v_cache.shape, BF16), jax.ShapeDtypeStruct((batch, slots), jnp.int32)),
            in_specs=[smem] + [vmem] * (2 * PIECES + 4),
            out_specs=(hbm,) * 4,
            scratch_shapes=[pltpu.VMEM((4, 16, slots, HEAD_DIM), BF16), pltpu.VMEM((4, 16, slots, HEAD_DIM), BF16), dma((2,)), dma((4,)), dma((4,))],
            compiler_params=pltpu.CompilerParams(vmem_limit_bytes=9 << 20),
            name='write',
        )(positions, k_new, v_new, x_new, sp_new, *held)
        return x_out, k_out, v_out, slot_pos_out

    return jax.shard_map(
        local_step,
        mesh=mesh,
        in_specs=(row_spec, P('dp'), cache_spec, cache_spec, slot_spec, vec_spec, mat_spec, mat_spec, mat_spec, mat_spec, vec_spec),
        out_specs=(row_spec, cache_spec, cache_spec, slot_spec),
        check_vma=False)
```

```python
import functools
import numpy as np
import jax
import jax.numpy as jnp
from jax import lax
from jax.experimental import pallas as pl
from jax.experimental.pallas import tpu as pltpu
from jax.sharding import PartitionSpec as P

HEADS = 4
HEAD_DIM = 256
ROPE_DIM = 128
ROPE_BASE = 10000.0
EPS = 1e-6
NEG_LARGE = -1e30
SCORE_SCALE = HEAD_DIM ** -0.5

UNIT = 8
CHUNK_UNITS = 2
ROWS = UNIT * HEADS
PACKET = 2 * ROWS + 8
SCATTER_GROUPS = ((4, 8), (8, 12))
WHOLE_GROUPS = ((0, 4), (12, 14), (14, 16))
PIECES = 2
AHEAD = 6
FIRST_LAG = 2
SECOND_LAG = 10
SCATTER_FIRST, SCATTER_LAST = 4, 12
MESH = pl.DeviceIdType.MESH
F32 = jnp.float32
BF16 = jnp.bfloat16


def attend_kernel(window, pos_h, freq_h, x_h, ns_h, wk_h, wv_h, wq_h, sp_h, wo_h, bo_h, k_h, v_h,
                  *rest):
    k_vm, v_vm = rest[:PIECES], rest[PIECES:2 * PIECES]
    (x_new, k_new, v_new, sp_new,
                  pos, freq, x_in, ns, wk, wv, wq, sp, wo, bo,
                  pos_b, x_f, q_s, pk, rc1, ch, o_s, ag, agd,
                  in_sem, k_sem, v_sem, s1, r1, s2, r2, sa, ra, sd, rd) = rest[2 * PIECES:]
    me = lax.axis_index('kv')
    x_side, core = me // 2, me % 2
    over = {'kv': 2 * (1 - x_side) + core}
    beside = {'kv': 2 * x_side + 1 - core}
    over_i = 2 * (1 - x_side) + core
    batch, slots = sp.shape
    chunk = UNIT * CHUNK_UNITS
    chunks = batch // chunk

    barrier = pltpu.get_barrier_semaphore()
    pl.semaphore_signal(barrier, inc=1, device_id=over, device_id_type=MESH)
    pl.semaphore_signal(barrier, inc=1, device_id=beside, device_id_type=MESH)

    smalls = [pltpu.make_async_copy(src, dst, in_sem.at[n]) for n, (src, dst) in enumerate((
        (pos_h, pos), (freq_h, freq), (x_h, x_in), (ns_h, ns), (wk_h, wk), (wv_h, wv), (wq_h, wq), (sp_h, sp), (wo_h, wo), (bo_h, bo)))]

    span = chunks // PIECES

    def cache_copy(j, piece):
        rows, held = pl.ds(j * chunk, chunk), pl.ds((j - piece * span) * chunk, chunk)
        return (pltpu.make_async_copy(k_h.at[rows], k_vm[piece].at[held], k_sem.at[j]),
                pltpu.make_async_copy(v_h.at[rows], v_vm[piece].at[held], v_sem.at[j]))

    def read_ahead(first, last):
        for j in range(first, last):
            for copy in cache_copy(j, j // span):
                copy.start()

    for small in smalls[:8]:
        small.start()
    read_ahead(0, 1)

    smalls[0].wait()
    smalls[1].wait()
    for r in range(batch // 128):
        row = pos[r:r + 1, :].astype(F32)
        pos_b[pl.ds(128 * r, 128), :] = jnp.transpose(jnp.broadcast_to(row, (128, 128)))
    read_ahead(1, 2)
    angles = pos_b[...] * freq[...]
    low = lax.broadcasted_iota(jnp.int32, (batch, 128), 1) < ROPE_DIM // 2
    cos_t = jnp.cos(angles)
    sin_t = jnp.sin(angles)
    sin_t = jnp.where(low, -sin_t, sin_t)

    def rotate(first):
        return first * cos_t + pltpu.roll(first, ROPE_DIM // 2, 1) * sin_t

    smalls[2].wait()
    smalls[3].wait()
    read_ahead(2, AHEAD)
    x32 = x_in[...].astype(F32)
    x_f[...] = x32
    mean_sq = jnp.mean(x32 * x32, axis=-1, keepdims=True)
    normed = (x32 * lax.rsqrt(mean_sq + EPS) * (1.0 + ns[...].astype(F32)[None, :])).astype(BF16)
    smalls[4].wait()
    smalls[5].wait()
    k_row = jnp.dot(normed, wk[...], preferred_element_type=F32)
    k_new[:, :128] = rotate(k_row[:, :128]).astype(BF16).astype(F32)
    k_new[:, 128:] = k_row[:, 128:].astype(BF16).astype(F32)
    v_new[...] = jnp.dot(normed, wv[...], preferred_element_type=F32).astype(BF16).astype(F32)
    smalls[6].wait()
    for small in smalls[8:]:
        small.start()
    for h in range(HEADS):
        q_row = jnp.dot(normed, wq[:, h * HEAD_DIM:(h + 1) * HEAD_DIM], preferred_element_type=F32)
        q_s[:, h, :, :128] = rotate(q_row[:, :128]).reshape(batch // UNIT, UNIT, 128)
        q_s[:, h, :, 128:] = q_row[:, 128:].reshape(batch // UNIT, UNIT, 128)
    smalls[7].wait()
    pl.semaphore_wait(barrier, 2)

    lane = lax.broadcasted_iota(jnp.int32, (UNIT, 128), 1)
    row_seq = lax.broadcasted_iota(jnp.int32, (ROWS, 128), 0) % UNIT

    def scores_of(u, piece):
        keys = k_vm[piece][pl.ds(u * UNIT - piece * span * chunk, UNIT)].reshape(UNIT * slots, HEAD_DIM)
        q_b = q_s[u].reshape(ROWS, HEAD_DIM).astype(BF16)
        return q_b, lax.dot_general(q_b, keys, (((1,), (1,)), ((), ())), preferred_element_type=F32)

    def weights_of(u, q_b, all_scores):
        seqs = pl.ds(u * UNIT, UNIT)
        scores = all_scores[:, :slots]
        for s in range(1, UNIT):
            scores = jnp.where(row_seq == s, all_scores[:, s * slots:(s + 1) * slots], scores)
        p_now = pos_b[seqs, :].astype(jnp.int32)
        slot = (p_now & (window - 1)) - me * slots
        hit = lane == slot
        held = jnp.where(hit, p_now, sp[seqs, :])
        sp_new[seqs, :] = held
        age = p_now - held
        usable = (held >= 0) & (age >= 0) & (age < window)
        fresh = jnp.sum(q_b.astype(F32).reshape(HEADS, UNIT, HEAD_DIM) * k_new[seqs, :][None], axis=-1, keepdims=True)
        scores = jnp.where(hit[None], fresh, scores.reshape(HEADS, UNIT, slots)) * SCORE_SCALE
        scores = jnp.where(usable[None], scores, NEG_LARGE)
        top = jnp.max(scores, axis=-1, keepdims=True)
        weights = jnp.where(usable[None], jnp.exp(scores - top), 0.0)
        total = jnp.sum(weights, axis=-1, keepdims=True)
        fresh_weight = jnp.sum(jnp.where(hit[None], weights, 0.0), axis=-1, keepdims=True)
        kept = jnp.where(hit[None], 0.0, weights).reshape(ROWS, slots)
        spread = jnp.concatenate([jnp.where(row_seq == s, kept, 0.0).astype(BF16) for s in range(UNIT)], axis=1)
        return top, total, fresh_weight, spread

    def sums_of(u, piece, fresh_weight, spread):
        values = v_vm[piece][pl.ds(u * UNIT - piece * span * chunk, UNIT)].reshape(UNIT * slots, HEAD_DIM)
        sums = jnp.dot(spread, values, preferred_element_type=F32).reshape(HEADS, UNIT, HEAD_DIM)
        sums = sums + fresh_weight.astype(BF16).astype(F32) * v_new[pl.ds(u * UNIT, UNIT), :][None]
        return sums.reshape(ROWS, HEAD_DIM)

    def attend(j, piece):
        units = [j * CHUNK_UNITS + i for i in range(2 * CHUNK_UNITS)]
        scored = [scores_of(u, piece) for u in units]
        weighed = [weights_of(u, *pair) for u, pair in zip(units, scored)]
        for i, u in enumerate(units):
            top, total, fresh_weight, spread = weighed[i]
            sums = sums_of(u, piece, fresh_weight, spread)
            n, i = j + i // CHUNK_UNITS, i % CHUNK_UNITS
            pk[n, i, 0:ROWS, :] = sums[:, :128]
            pk[n, i, ROWS:2 * ROWS, :] = sums[:, 128:]
            tile = jnp.zeros((UNIT, 128), F32)
            for h in range(HEADS):
                tile = jnp.where(lane == h, top[h], jnp.where(lane == HEADS + h, total[h], tile))
            pk[n, i, 2 * ROWS:, :] = tile

    def merge(a, b):
        ta, tb = a[2 * ROWS:, :], b[2 * ROWS:, :]
        tile = jnp.maximum(ta, tb)
        ea, eb = jnp.exp(ta - tile), jnp.exp(tb - tile)
        parts, totals = [], []
        for h in range(HEADS):
            fa, fb = ea[:, h:h + 1], eb[:, h:h + 1]
            totals.append(fa * ta[:, HEADS + h:HEADS + h + 1] + fb * tb[:, HEADS + h:HEADS + h + 1])
            parts.append([fa * a[o + h * UNIT:o + (h + 1) * UNIT, :] + fb * b[o + h * UNIT:o + (h + 1) * UNIT, :] for o in (0, ROWS)])
        return tile, parts, totals

    sequence = lax.broadcasted_iota(jnp.int32, (UNIT, 128), 0)

    def pack(tile, totals):
        spots = jnp.zeros((UNIT, 128), F32)
        for h in range(HEADS):
            spots = jnp.where(lane == h * UNIT + sequence, tile[:, h:h + 1], spots)
            spots = jnp.where(lane == ROWS + h * UNIT + sequence, totals[h], spots)
        return jnp.sum(spots, axis=0, keepdims=True)

    def unpack(row):
        spots = jnp.broadcast_to(row, (UNIT, 128))
        columns = [jnp.sum(jnp.where(lane == n * UNIT + sequence, spots, 0.0), axis=1, keepdims=True) for n in range(2 * HEADS)]
        return columns[:HEADS], columns[HEADS:]

    def merge_packed(a, b):
        (tops_a, totals_a), (tops_b, totals_b) = unpack(a[2 * ROWS:2 * ROWS + 1, :]), unpack(b[2 * ROWS:2 * ROWS + 1, :])
        parts, totals = [], []
        for h in range(HEADS):
            top = jnp.maximum(tops_a[h], tops_b[h])
            fa, fb = jnp.exp(tops_a[h] - top), jnp.exp(tops_b[h] - top)
            totals.append(fa * totals_a[h] + fb * totals_b[h])
            parts.append([fa * a[o + h * UNIT:o + (h + 1) * UNIT, :] + fb * b[o + h * UNIT:o + (h + 1) * UNIT, :] for o in (0, ROWS)])
        return parts, totals

    def first_copy(j):
        return pltpu.make_async_remote_copy(pk.at[j, 1 - core], rc1.at[j], s1.at[j], r1.at[j], device_id=beside, device_id_type=MESH)

    def second_copy(j):
        rows = ch.at[j, x_side, pl.ds(0, 2 * ROWS + 1)]
        return pltpu.make_async_remote_copy(rows, rows, s2.at[j], r2.at[j], device_id=over, device_id_type=MESH)

    def either(condition, yes, no):
        if isinstance(condition, bool):
            return yes() if condition else no()
        pl.when(condition)(yes)
        pl.when(jnp.logical_not(condition))(no)

    def is_whole(j):
        return (j < SCATTER_FIRST or j >= SCATTER_LAST) if isinstance(j, int) else (j < SCATTER_FIRST) | (j >= SCATTER_LAST)

    def first_merge(j):
        pair = (j, j + 1)
        for n in pair:
            first_copy(n).wait_recv()
        merged = [merge(pk[n, core], rc1[n]) for n in pair]
        for n, (tile, parts, totals) in zip(pair, merged):
            for h in range(HEADS):
                ch[n, x_side, h * UNIT:(h + 1) * UNIT, :] = parts[h][0]
                ch[n, x_side, ROWS + h * UNIT:ROWS + (h + 1) * UNIT, :] = parts[h][1]
            ch[n, x_side, 2 * ROWS:2 * ROWS + 1, :] = pack(tile, totals)

        def both():
            for n in pair:
                second_copy(n).start()

        either(is_whole(j), both, lambda: second_copy(j + 1 - x_side).start())

    scattered = (SCATTER_LAST - SCATTER_FIRST) // 2

    def final_block(j):
        if isinstance(j, int):
            return j if j < SCATTER_FIRST else SCATTER_FIRST + (j - SCATTER_FIRST) // 2 if j < SCATTER_LAST else j - scattered
        return jnp.where(j < SCATTER_FIRST, j, jnp.where(j < SCATTER_LAST, SCATTER_FIRST + (j - SCATTER_FIRST) // 2, j - scattered))

    def whole_block(j):
        return j if j < SCATTER_FIRST else j - 2 * scattered

    def finish(*chunk_ids):
        for n in chunk_ids:
            second_copy(n).wait_recv()
        merged = [merge_packed(ch[n, 0], ch[n, 1]) for n in chunk_ids]
        for n, (parts, totals) in zip(chunk_ids, merged):
            rows = pl.ds(final_block(n) * UNIT, UNIT)
            for h in range(HEADS):
                inverse = 1.0 / totals[h]
                o_s[rows, h * HEAD_DIM:h * HEAD_DIM + 128] = parts[h][0] * inverse
                o_s[rows, h * HEAD_DIM + 128:(h + 1) * HEAD_DIM] = parts[h][1] * inverse

    def second_merge(j):
        either(is_whole(j), lambda: finish(j, j + 1), lambda: finish(j + x_side))

    def project(first, residual):
        rows = pl.ds(first, residual.shape[0])
        return residual + jnp.dot(o_s[rows, :].astype(BF16), wo[...], preferred_element_type=F32) + bo[...].astype(F32)[None, :]

    def gather_copy(g, owner, target, n):
        first, last = SCATTER_GROUPS[g]
        rows = ag.at[owner, pl.ds((first - SCATTER_FIRST) // 2 * UNIT, (last - first) // 2 * UNIT)]
        return pltpu.make_async_remote_copy(rows, rows, sa.at[g, n], ra.at[g, n], device_id=target, device_id_type=MESH)

    gathers = [(gather_copy(g, me, over, 0), gather_copy(g, me, beside, 1), gather_copy(g, over_i, beside, 2)) for g in range(len(SCATTER_GROUPS))]

    def project_scattered(g):
        first, last = SCATTER_GROUPS[g]
        residual = jnp.concatenate([x_f[pl.ds((n + x_side) * chunk + core * UNIT, UNIT), :] for n in range(first, last, 2)], axis=0)
        start = (first - SCATTER_FIRST) // 2 * UNIT
        ag[me, start:start + residual.shape[0], :] = project(SCATTER_FIRST * UNIT + start, residual)
        gathers[g][0].start()
        gathers[g][1].start()

    def forward(g):
        gathers[g][0].wait_recv()
        gathers[g][2].start()

    def collect_scattered(g):
        gathers[g][1].wait_recv()
        gathers[g][2].wait_recv()
        for j in range(*SCATTER_GROUPS[g]):
            i = (j - SCATTER_FIRST) // 2
            rows = [ag[2 * (j % 2) + c, i * UNIT:(i + 1) * UNIT, :] for c in range(2)]
            x_new[j * chunk:(j + 1) * chunk, :] = jnp.concatenate(rows, axis=0).astype(BF16)

    def beside_copy(g):
        first, last = WHOLE_GROUPS[g]
        rows = agd.at[core, pl.ds(whole_block(first) * UNIT, (last - first) * UNIT)]
        return pltpu.make_async_remote_copy(rows, rows, sd.at[g], rd.at[g], device_id=beside, device_id_type=MESH)

    def project_whole(g):
        first, last = WHOLE_GROUPS[g]
        residual = jnp.concatenate([x_f[pl.ds(j * chunk + core * UNIT, UNIT), :] for j in range(first, last)], axis=0)
        agd[core, whole_block(first) * UNIT:whole_block(last - 1) * UNIT + UNIT, :] = project(final_block(first) * UNIT, residual)
        beside_copy(g).start()

    def collect_whole(g):
        beside_copy(g).wait_recv()
        for j in range(*WHOLE_GROUPS[g]):
            rows = [agd[c, whole_block(j) * UNIT:(whole_block(j) + 1) * UNIT, :] for c in range(2)]
            x_new[j * chunk:(j + 1) * chunk, :] = jnp.concatenate(rows, axis=0).astype(BF16)

    def step(piece, block, carry):
        j = 2 * block
        for n in range(2):
            for copy in cache_copy(j + n, piece):
                copy.wait()
        attend(j, piece)
        for n in range(2):
            first_copy(j + n).start()

        @pl.when(j >= FIRST_LAG)
        def _():
            first_merge(j - FIRST_LAG)

        @pl.when(j >= SECOND_LAG)
        def _():
            second_merge(j - SECOND_LAG)

        for ahead in range(PIECES):
            @pl.when((j + AHEAD < chunks) & ((j + AHEAD) // span == ahead))
            def _():
                for n in range(2):
                    for copy in cache_copy(j + AHEAD + n, ahead):
                        copy.start()

        return carry

    for piece in range(PIECES):
        lax.fori_loop(piece * span // 2, (piece + 1) * span // 2, functools.partial(step, piece), 0)
    for small in smalls[8:]:
        small.wait()
    seconds = list(range(chunks - SECOND_LAG, chunks, 2))
    firsts = list(range(chunks - FIRST_LAG, chunks, 2))

    def second_upto(last):
        while seconds and seconds[0] < last:
            second_merge(seconds.pop(0))

    second_upto(SCATTER_GROUPS[0][1])
    project_scattered(0)
    for j in firsts:
        first_merge(j)
    project_whole(0)
    second_upto(SCATTER_GROUPS[1][1])
    project_scattered(1)
    forward(0)
    collect_whole(0)
    for g in range(1, len(WHOLE_GROUPS)):
        second_upto(WHOLE_GROUPS[g][1])
        project_whole(g)
        if g == 1:
            collect_scattered(0)
    forward(1)
    collect_scattered(1)
    for g in range(1, len(WHOLE_GROUPS)):
        collect_whole(g)

    def drain(j, carry):
        first_copy(j).wait_send()

        @pl.when((j < SCATTER_FIRST) | (j >= SCATTER_LAST) | (j % 2 != x_side))
        def _():
            second_copy(j).wait_send()
        return carry

    lax.fori_loop(0, chunks, drain, 0)
    for group in gathers:
        for gather in group:
            gather.wait_send()
    for g in range(len(WHOLE_GROUPS)):
        beside_copy(g).wait_send()


def write_kernel(window, pos, k_new, v_new, x_new, sp_new, *rest):
    k_vm, v_vm = rest[:PIECES], rest[PIECES:2 * PIECES]
    x_out, k_out, v_out, sp_out, k_ring, v_ring, sems, k_sem, v_sem = rest[2 * PIECES:]
    me = lax.axis_index('kv')
    part, slots, _ = k_vm[0].shape
    batch = part * PIECES
    depth, chunk = k_ring.shape[:2]
    chunks = batch // chunk
    span = chunks // PIECES
    others = (pltpu.make_async_copy(x_new, x_out, sems.at[0]), pltpu.make_async_copy(sp_new, sp_out, sems.at[1]))
    for copy in others:
        copy.start()
    tile_row = lax.broadcasted_iota(jnp.int32, (16, HEAD_DIM), 0)

    def copies(j):
        rows, ring = pl.ds(j * chunk, chunk), lax.rem(j, depth)
        return (pltpu.make_async_copy(k_ring.at[ring], k_out.at[rows], k_sem.at[ring]),
                pltpu.make_async_copy(v_ring.at[ring], v_out.at[rows], v_sem.at[ring]))

    def step(piece, j, carry):
        ring = lax.rem(j, depth)

        @pl.when(j >= depth)
        def _():
            for copy in copies(j - depth):
                copy.wait()

        def group(i, carry):
            for n in range(8):
                row = i * 8 + n
                b = j * chunk + row
                slot = (pos[b] & (window - 1)) - me * slots
                base = pl.multiple_of((jnp.clip(slot, 0, slots - 1) // 16) * 16, 16)
                for new, cache, out in ((k_new, k_vm[piece], k_ring), (v_new, v_vm[piece], v_ring)):
                    out[ring, row] = cache[b - piece * part]
                    fresh = jnp.broadcast_to(new[pl.ds(b, 1), :], (16, HEAD_DIM))
                    old = cache[b - piece * part, pl.ds(base, 16), :].astype(F32)
                    out[ring, row, pl.ds(base, 16), :] = jnp.where(tile_row == slot - base, fresh, old).astype(BF16)
            return carry
        lax.fori_loop(0, chunk // 8, group, 0)
        for copy in copies(j):
            copy.start()
        return carry

    for piece in range(PIECES):
        lax.fori_loop(piece * span, (piece + 1) * span, functools.partial(step, piece), 0)
    for j in range(chunks - depth, chunks):
        for copy in copies(j):
            copy.wait()
    for copy in others:
        copy.wait()


def solution(mesh):
    kv_size = mesh.shape['kv']
    row_spec = P('dp', None)
    cache_spec = P('dp', 'kv', None)
    slot_spec = P('dp', 'kv')
    vec_spec = P(None)
    mat_spec = P(None, None)
    half_dims = ROPE_DIM // 2
    freq_row = np.tile(ROPE_BASE ** (-np.arange(half_dims) / half_dims), 2).astype(np.float32)[None, :]

    def local_step(x_in, positions, k_cache, v_cache, slot_pos, norm_scale, w_q, w_k, w_v, w_o, b_o):
        batch, model = x_in.shape
        slots = k_cache.shape[1]
        window = slots * kv_size
        width = w_q.shape[1]
        chunks = batch // (UNIT * CHUNK_UNITS)
        scattered = (SCATTER_LAST - SCATTER_FIRST) // 2
        hbm = pl.BlockSpec(memory_space=pltpu.HBM)
        vmem = pl.BlockSpec(memory_space=pltpu.VMEM)
        smem = pl.BlockSpec(memory_space=pltpu.SMEM)
        dma = pltpu.SemaphoreType.DMA
        per_chunk = [dma((chunks,))] * 4
        *held, x_new, k_new, v_new, sp_new = pl.pallas_call(
            functools.partial(attend_kernel, window),
            out_shape=(*([pltpu.VMEM((batch // PIECES, slots, HEAD_DIM), BF16)] * (2 * PIECES)), pltpu.VMEM((batch, model), BF16),
                       pltpu.VMEM((batch, HEAD_DIM), F32), pltpu.VMEM((batch, HEAD_DIM), F32), pltpu.VMEM((batch, slots), jnp.int32)),
            in_specs=[hbm] * 12,
            out_specs=(vmem,) * (2 * PIECES + 4),
            scratch_shapes=[
                pltpu.VMEM((batch // 128, 128), jnp.int32), pltpu.VMEM((1, 128), F32), pltpu.VMEM((batch, model), BF16), pltpu.VMEM((model,), BF16),
                pltpu.VMEM((model, HEAD_DIM), BF16), pltpu.VMEM((model, HEAD_DIM), BF16), pltpu.VMEM((model, width), BF16),
                pltpu.VMEM((batch, slots), jnp.int32), pltpu.VMEM((width, model), BF16), pltpu.VMEM((model,), BF16),
                pltpu.VMEM((batch, 128), F32), pltpu.VMEM((batch, model), F32), pltpu.VMEM((batch // UNIT, HEADS, UNIT, HEAD_DIM), F32),
                pltpu.VMEM((chunks, CHUNK_UNITS, PACKET, 128), F32), pltpu.VMEM((chunks, PACKET, 128), F32), pltpu.VMEM((chunks, 2, PACKET, 128), F32),
                pltpu.VMEM(((chunks - scattered) * UNIT, width), F32), pltpu.VMEM((kv_size, scattered * UNIT, model), F32),
                pltpu.VMEM((2, (chunks - 2 * scattered) * UNIT, model), F32),
                dma((10,)), dma((chunks,)), dma((chunks,)), *per_chunk, *([dma((len(SCATTER_GROUPS), 3))] * 2), *([dma((len(WHOLE_GROUPS),))] * 2)],
            compiler_params=pltpu.CompilerParams(vmem_limit_bytes=16 << 20, collective_id=0, has_side_effects=True),
            name='attend',
        )(*[pltpu.with_memory_space_constraint(a, pltpu.HBM) for a in (
            positions.reshape(batch // 128, 128), jnp.asarray(freq_row), x_in, norm_scale, w_k, w_v, w_q, slot_pos,
            w_o, b_o, k_cache, v_cache)])
        x_out, k_out, v_out, slot_pos_out = pl.pallas_call(
            functools.partial(write_kernel, window),
            out_shape=(jax.ShapeDtypeStruct((batch, model), BF16), jax.ShapeDtypeStruct(k_cache.shape, BF16),
                       jax.ShapeDtypeStruct(v_cache.shape, BF16), jax.ShapeDtypeStruct((batch, slots), jnp.int32)),
            in_specs=[smem] + [vmem] * (2 * PIECES + 4),
            out_specs=(hbm,) * 4,
            scratch_shapes=[pltpu.VMEM((4, 16, slots, HEAD_DIM), BF16), pltpu.VMEM((4, 16, slots, HEAD_DIM), BF16), dma((2,)), dma((4,)), dma((4,))],
            compiler_params=pltpu.CompilerParams(vmem_limit_bytes=9 << 20),
            name='write',
        )(positions, k_new, v_new, x_new, sp_new, *held)
        return x_out, k_out, v_out, slot_pos_out

    return jax.shard_map(
        local_step,
        mesh=mesh,
        in_specs=(row_spec, P('dp'), cache_spec, cache_spec, slot_spec, vec_spec, mat_spec, mat_spec, mat_spec, mat_spec, vec_spec),
        out_specs=(row_spec, cache_spec, cache_spec, slot_spec),
        check_vma=False)
```

```python
import functools
import numpy as np
import jax
import jax.numpy as jnp
from jax import lax
from jax.experimental import pallas as pl
from jax.experimental.pallas import tpu as pltpu
from jax.sharding import PartitionSpec as P

HEADS = 4
HEAD_DIM = 256
ROPE_DIM = 128
ROPE_BASE = 10000.0
EPS = 1e-6
NEG_LARGE = -1e30
SCORE_SCALE = HEAD_DIM ** -0.5

UNIT = 8
CHUNK_UNITS = 2
ROWS = UNIT * HEADS
PACKET = 2 * ROWS + 8
SCATTER_GROUPS = ((4, 8), (8, 12))
WHOLE_GROUPS = ((0, 4), (12, 14), (14, 16))
PIECES = 2
AHEAD = 6
FIRST_LAG = 2
SCATTER_FIRST, SCATTER_LAST = 4, 12
MESH = pl.DeviceIdType.MESH
F32 = jnp.float32
BF16 = jnp.bfloat16


def attend_kernel(window, pos_h, freq_h, x_h, ns_h, wk_h, wv_h, wq_h, sp_h, wo_h, bo_h, k_h, v_h,
                  *rest):
    k_vm, v_vm = rest[:PIECES], rest[PIECES:2 * PIECES]
    (x_new, k_new, v_new, sp_new,
                  pos, freq, x_in, ns, wk, wv, wq, sp, wo, bo,
                  pos_b, x_f, q_s, pk, rc1, ch, o_s, ag, agd,
                  in_sem, k_sem, v_sem, s1, r1, s2, r2, sa, ra, sd, rd) = rest[2 * PIECES:]
    me = lax.axis_index('kv')
    x_side, core = me // 2, me % 2
    over = {'kv': 2 * (1 - x_side) + core}
    beside = {'kv': 2 * x_side + 1 - core}
    over_i = 2 * (1 - x_side) + core
    batch, slots = sp.shape
    chunk = UNIT * CHUNK_UNITS
    chunks = batch // chunk

    barrier = pltpu.get_barrier_semaphore()
    pl.semaphore_signal(barrier, inc=1, device_id=over, device_id_type=MESH)
    pl.semaphore_signal(barrier, inc=1, device_id=beside, device_id_type=MESH)

    smalls = [pltpu.make_async_copy(src, dst, in_sem.at[n]) for n, (src, dst) in enumerate((
        (pos_h, pos), (freq_h, freq), (x_h, x_in), (ns_h, ns), (wk_h, wk), (wv_h, wv), (wq_h, wq), (sp_h, sp), (wo_h, wo), (bo_h, bo)))]

    span = chunks // PIECES

    def cache_copy(j, piece):
        rows, held = pl.ds(j * chunk, chunk), pl.ds((j - piece * span) * chunk, chunk)
        return (pltpu.make_async_copy(k_h.at[rows], k_vm[piece].at[held], k_sem.at[j]),
                pltpu.make_async_copy(v_h.at[rows], v_vm[piece].at[held], v_sem.at[j]))

    def read_ahead(first, last):
        for j in range(first, last):
            for copy in cache_copy(j, j // span):
                copy.start()

    for small in smalls[:8]:
        small.start()
    read_ahead(0, 1)

    smalls[0].wait()
    smalls[1].wait()
    for r in range(batch // 128):
        row = pos[r:r + 1, :].astype(F32)
        pos_b[pl.ds(128 * r, 128), :] = jnp.transpose(jnp.broadcast_to(row, (128, 128)))
    read_ahead(1, 2)
    angles = pos_b[...] * freq[...]
    low = lax.broadcasted_iota(jnp.int32, (batch, 128), 1) < ROPE_DIM // 2
    cos_t = jnp.cos(angles)
    sin_t = jnp.sin(angles)
    sin_t = jnp.where(low, -sin_t, sin_t)

    def rotate(first):
        return first * cos_t + pltpu.roll(first, ROPE_DIM // 2, 1) * sin_t

    smalls[2].wait()
    smalls[3].wait()
    read_ahead(2, AHEAD)
    x32 = x_in[...].astype(F32)
    x_f[...] = x32
    mean_sq = jnp.mean(x32 * x32, axis=-1, keepdims=True)
    normed = (x32 * lax.rsqrt(mean_sq + EPS) * (1.0 + ns[...].astype(F32)[None, :])).astype(BF16)
    smalls[4].wait()
    smalls[5].wait()
    k_row = jnp.dot(normed, wk[...], preferred_element_type=F32)
    k_new[:, :128] = rotate(k_row[:, :128]).astype(BF16).astype(F32)
    k_new[:, 128:] = k_row[:, 128:].astype(BF16).astype(F32)
    v_new[...] = jnp.dot(normed, wv[...], preferred_element_type=F32).astype(BF16).astype(F32)
    smalls[6].wait()
    for small in smalls[8:]:
        small.start()
    for h in range(HEADS):
        q_row = jnp.dot(normed, wq[:, h * HEAD_DIM:(h + 1) * HEAD_DIM], preferred_element_type=F32)
        q_s[:, h, :, :128] = rotate(q_row[:, :128]).reshape(batch // UNIT, UNIT, 128)
        q_s[:, h, :, 128:] = q_row[:, 128:].reshape(batch // UNIT, UNIT, 128)
    smalls[7].wait()
    pl.semaphore_wait(barrier, 2)

    lane = lax.broadcasted_iota(jnp.int32, (UNIT, 128), 1)
    row_seq = lax.broadcasted_iota(jnp.int32, (ROWS, 128), 0) % UNIT

    def scores_of(u, piece):
        keys = k_vm[piece][pl.ds(u * UNIT - piece * span * chunk, UNIT)].reshape(UNIT * slots, HEAD_DIM)
        q_b = q_s[u].reshape(ROWS, HEAD_DIM).astype(BF16)
        return q_b, lax.dot_general(q_b, keys, (((1,), (1,)), ((), ())), preferred_element_type=F32)

    def weights_of(u, q_b, all_scores):
        seqs = pl.ds(u * UNIT, UNIT)
        scores = all_scores[:, :slots]
        for s in range(1, UNIT):
            scores = jnp.where(row_seq == s, all_scores[:, s * slots:(s + 1) * slots], scores)
        p_now = pos_b[seqs, :].astype(jnp.int32)
        slot = (p_now & (window - 1)) - me * slots
        hit = lane == slot
        held = jnp.where(hit, p_now, sp[seqs, :])
        sp_new[seqs, :] = held
        age = p_now - held
        usable = (held >= 0) & (age >= 0) & (age < window)
        fresh = jnp.sum(q_b.astype(F32).reshape(HEADS, UNIT, HEAD_DIM) * k_new[seqs, :][None], axis=-1, keepdims=True)
        scores = jnp.where(hit[None], fresh, scores.reshape(HEADS, UNIT, slots)) * SCORE_SCALE
        scores = jnp.where(usable[None], scores, NEG_LARGE)
        top = jnp.max(scores, axis=-1, keepdims=True)
        weights = jnp.where(usable[None], jnp.exp(scores - top), 0.0)
        total = jnp.sum(weights, axis=-1, keepdims=True)
        fresh_weight = jnp.sum(jnp.where(hit[None], weights, 0.0), axis=-1, keepdims=True)
        kept = jnp.where(hit[None], 0.0, weights).reshape(ROWS, slots)
        spread = jnp.concatenate([jnp.where(row_seq == s, kept, 0.0).astype(BF16) for s in range(UNIT)], axis=1)
        return top, total, fresh_weight, spread

    def sums_of(u, piece, fresh_weight, spread):
        values = v_vm[piece][pl.ds(u * UNIT - piece * span * chunk, UNIT)].reshape(UNIT * slots, HEAD_DIM)
        sums = jnp.dot(spread, values, preferred_element_type=F32).reshape(HEADS, UNIT, HEAD_DIM)
        sums = sums + fresh_weight.astype(BF16).astype(F32) * v_new[pl.ds(u * UNIT, UNIT), :][None]
        return sums.reshape(ROWS, HEAD_DIM)

    def attend(j, piece):
        units = [j * CHUNK_UNITS + i for i in range(2 * CHUNK_UNITS)]
        scored = [scores_of(u, piece) for u in units]
        weighed = [weights_of(u, *pair) for u, pair in zip(units, scored)]
        for i, u in enumerate(units):
            top, total, fresh_weight, spread = weighed[i]
            sums = sums_of(u, piece, fresh_weight, spread)
            n, i = j + i // CHUNK_UNITS, i % CHUNK_UNITS
            pk[n, i, 0:ROWS, :] = sums[:, :128]
            pk[n, i, ROWS:2 * ROWS, :] = sums[:, 128:]
            tile = jnp.zeros((UNIT, 128), F32)
            for h in range(HEADS):
                tile = jnp.where(lane == h, top[h], jnp.where(lane == HEADS + h, total[h], tile))
            pk[n, i, 2 * ROWS:, :] = tile

    def merge(a, b):
        ta, tb = a[2 * ROWS:, :], b[2 * ROWS:, :]
        tile = jnp.maximum(ta, tb)
        ea, eb = jnp.exp(ta - tile), jnp.exp(tb - tile)
        parts, totals = [], []
        for h in range(HEADS):
            fa, fb = ea[:, h:h + 1], eb[:, h:h + 1]
            totals.append(fa * ta[:, HEADS + h:HEADS + h + 1] + fb * tb[:, HEADS + h:HEADS + h + 1])
            parts.append([fa * a[o + h * UNIT:o + (h + 1) * UNIT, :] + fb * b[o + h * UNIT:o + (h + 1) * UNIT, :] for o in (0, ROWS)])
        return tile, parts, totals

    sequence = lax.broadcasted_iota(jnp.int32, (UNIT, 128), 0)

    def pack(tile, totals):
        spots = jnp.zeros((UNIT, 128), F32)
        for h in range(HEADS):
            spots = jnp.where(lane == h * UNIT + sequence, tile[:, h:h + 1], spots)
            spots = jnp.where(lane == ROWS + h * UNIT + sequence, totals[h], spots)
        return jnp.sum(spots, axis=0, keepdims=True)

    def unpack(row):
        spots = jnp.broadcast_to(row, (UNIT, 128))
        columns = [jnp.sum(jnp.where(lane == n * UNIT + sequence, spots, 0.0), axis=1, keepdims=True) for n in range(2 * HEADS)]
        return columns[:HEADS], columns[HEADS:]

    def merge_packed(a, b):
        (tops_a, totals_a), (tops_b, totals_b) = unpack(a[2 * ROWS:2 * ROWS + 1, :]), unpack(b[2 * ROWS:2 * ROWS + 1, :])
        parts, totals = [], []
        for h in range(HEADS):
            top = jnp.maximum(tops_a[h], tops_b[h])
            fa, fb = jnp.exp(tops_a[h] - top), jnp.exp(tops_b[h] - top)
            totals.append(fa * totals_a[h] + fb * totals_b[h])
            parts.append([fa * a[o + h * UNIT:o + (h + 1) * UNIT, :] + fb * b[o + h * UNIT:o + (h + 1) * UNIT, :] for o in (0, ROWS)])
        return parts, totals

    def first_copy(j):
        return pltpu.make_async_remote_copy(pk.at[j, 1 - core], rc1.at[j], s1.at[j], r1.at[j], device_id=beside, device_id_type=MESH)

    def second_copy(j):
        rows = ch.at[j, x_side, pl.ds(0, 2 * ROWS + 1)]
        return pltpu.make_async_remote_copy(rows, rows, s2.at[j], r2.at[j], device_id=over, device_id_type=MESH)

    def either(condition, yes, no):
        if isinstance(condition, bool):
            return yes() if condition else no()
        pl.when(condition)(yes)
        pl.when(jnp.logical_not(condition))(no)

    def is_whole(j):
        return (j < SCATTER_FIRST or j >= SCATTER_LAST) if isinstance(j, int) else (j < SCATTER_FIRST) | (j >= SCATTER_LAST)

    def first_merge(j):
        pair = (j, j + 1)
        for n in pair:
            first_copy(n).wait_recv()
        merged = [merge(pk[n, core], rc1[n]) for n in pair]
        for n, (tile, parts, totals) in zip(pair, merged):
            for h in range(HEADS):
                ch[n, x_side, h * UNIT:(h + 1) * UNIT, :] = parts[h][0]
                ch[n, x_side, ROWS + h * UNIT:ROWS + (h + 1) * UNIT, :] = parts[h][1]
            ch[n, x_side, 2 * ROWS:2 * ROWS + 1, :] = pack(tile, totals)

        def both():
            for n in pair:
                second_copy(n).start()

        either(is_whole(j), both, lambda: second_copy(j + 1 - x_side).start())

    scattered = (SCATTER_LAST - SCATTER_FIRST) // 2

    def final_block(j):
        if isinstance(j, int):
            return j if j < SCATTER_FIRST else SCATTER_FIRST + (j - SCATTER_FIRST) // 2 if j < SCATTER_LAST else j - scattered
        return jnp.where(j < SCATTER_FIRST, j, jnp.where(j < SCATTER_LAST, SCATTER_FIRST + (j - SCATTER_FIRST) // 2, j - scattered))

    def whole_block(j):
        return j if j < SCATTER_FIRST else j - 2 * scattered

    def finish(*chunk_ids):
        for n in chunk_ids:
            second_copy(n).wait_recv()
        merged = [merge_packed(ch[n, 0], ch[n, 1]) for n in chunk_ids]
        for n, (parts, totals) in zip(chunk_ids, merged):
            rows = pl.ds(final_block(n) * UNIT, UNIT)
            for h in range(HEADS):
                inverse = 1.0 / totals[h]
                o_s[rows, h * HEAD_DIM:h * HEAD_DIM + 128] = parts[h][0] * inverse
                o_s[rows, h * HEAD_DIM + 128:(h + 1) * HEAD_DIM] = parts[h][1] * inverse

    def second_merge(j):
        either(is_whole(j), lambda: finish(j, j + 1), lambda: finish(j + x_side))

    def project(first, residual):
        rows = pl.ds(first, residual.shape[0])
        return residual + jnp.dot(o_s[rows, :].astype(BF16), wo[...], preferred_element_type=F32) + bo[...].astype(F32)[None, :]

    def gather_copy(g, owner, target, n):
        first, last = SCATTER_GROUPS[g]
        rows = ag.at[owner, pl.ds((first - SCATTER_FIRST) // 2 * UNIT, (last - first) // 2 * UNIT)]
        return pltpu.make_async_remote_copy(rows, rows, sa.at[g, n], ra.at[g, n], device_id=target, device_id_type=MESH)

    gathers = [(gather_copy(g, me, over, 0), gather_copy(g, me, beside, 1), gather_copy(g, over_i, beside, 2)) for g in range(len(SCATTER_GROUPS))]

    def project_scattered(g):
        first, last = SCATTER_GROUPS[g]
        residual = jnp.concatenate([x_f[pl.ds((n + x_side) * chunk + core * UNIT, UNIT), :] for n in range(first, last, 2)], axis=0)
        start = (first - SCATTER_FIRST) // 2 * UNIT
        ag[me, start:start + residual.shape[0], :] = project(SCATTER_FIRST * UNIT + start, residual)
        gathers[g][0].start()
        gathers[g][1].start()

    def forward(g):
        gathers[g][0].wait_recv()
        gathers[g][2].start()

    def collect_scattered(g):
        gathers[g][1].wait_recv()
        gathers[g][2].wait_recv()
        for j in range(*SCATTER_GROUPS[g]):
            i = (j - SCATTER_FIRST) // 2
            rows = [ag[2 * (j % 2) + c, i * UNIT:(i + 1) * UNIT, :] for c in range(2)]
            x_new[j * chunk:(j + 1) * chunk, :] = jnp.concatenate(rows, axis=0).astype(BF16)

    def beside_copy(g):
        first, last = WHOLE_GROUPS[g]
        rows = agd.at[core, pl.ds(whole_block(first) * UNIT, (last - first) * UNIT)]
        return pltpu.make_async_remote_copy(rows, rows, sd.at[g], rd.at[g], device_id=beside, device_id_type=MESH)

    def project_whole(g):
        first, last = WHOLE_GROUPS[g]
        residual = jnp.concatenate([x_f[pl.ds(j * chunk + core * UNIT, UNIT), :] for j in range(first, last)], axis=0)
        agd[core, whole_block(first) * UNIT:whole_block(last - 1) * UNIT + UNIT, :] = project(final_block(first) * UNIT, residual)
        beside_copy(g).start()

    def collect_whole(g):
        beside_copy(g).wait_recv()
        for j in range(*WHOLE_GROUPS[g]):
            rows = [agd[c, whole_block(j) * UNIT:(whole_block(j) + 1) * UNIT, :] for c in range(2)]
            x_new[j * chunk:(j + 1) * chunk, :] = jnp.concatenate(rows, axis=0).astype(BF16)

    def step(piece, block, carry):
        j = 2 * block
        for n in range(2):
            for copy in cache_copy(j + n, piece):
                copy.wait()
        attend(j, piece)
        for n in range(2):
            first_copy(j + n).start()

        @pl.when(j >= FIRST_LAG)
        def _():
            first_merge(j - FIRST_LAG)

        for ahead in range(PIECES):
            @pl.when((j + AHEAD < chunks) & ((j + AHEAD) // span == ahead))
            def _():
                for n in range(2):
                    for copy in cache_copy(j + AHEAD + n, ahead):
                        copy.start()

        return carry

    for piece in range(PIECES):
        lax.fori_loop(piece * span // 2, (piece + 1) * span // 2, functools.partial(step, piece), 0)
    for small in smalls[8:]:
        small.wait()
    def second_merges(first, last):
        for j in range(first, last, 2):
            second_merge(j)

    def drain(j, carry):
        first_copy(j).wait_send()

        @pl.when((j < SCATTER_FIRST) | (j >= SCATTER_LAST) | (j % 2 != x_side))
        def _():
            second_copy(j).wait_send()
        return carry

    second_merges(*SCATTER_GROUPS[0])
    project_scattered(0)
    for j in range(chunks - FIRST_LAG, chunks, 2):
        first_merge(j)
    second_merges(*WHOLE_GROUPS[0])
    project_whole(0)
    second_merges(*SCATTER_GROUPS[1])
    project_scattered(1)
    forward(0)
    collect_whole(0)
    second_merges(*WHOLE_GROUPS[1])
    project_whole(1)
    collect_scattered(0)
    lax.fori_loop(0, chunks, drain, 0)
    second_merges(*WHOLE_GROUPS[2])
    project_whole(2)
    forward(1)
    collect_whole(1)
    collect_scattered(1)
    collect_whole(2)
    for group in gathers:
        for gather in group:
            gather.wait_send()
    for g in range(len(WHOLE_GROUPS)):
        beside_copy(g).wait_send()


def write_kernel(window, pos, k_new, v_new, x_new, sp_new, *rest):
    k_vm, v_vm = rest[:PIECES], rest[PIECES:2 * PIECES]
    x_out, k_out, v_out, sp_out, k_ring, v_ring, sems, k_sem, v_sem = rest[2 * PIECES:]
    me = lax.axis_index('kv')
    part, slots, _ = k_vm[0].shape
    batch = part * PIECES
    depth, chunk = k_ring.shape[:2]
    chunks = batch // chunk
    span = chunks // PIECES
    others = (pltpu.make_async_copy(x_new, x_out, sems.at[0]), pltpu.make_async_copy(sp_new, sp_out, sems.at[1]))
    for copy in others:
        copy.start()
    tile_row = lax.broadcasted_iota(jnp.int32, (16, HEAD_DIM), 0)

    def copies(j):
        rows, ring = pl.ds(j * chunk, chunk), lax.rem(j, depth)
        return (pltpu.make_async_copy(k_ring.at[ring], k_out.at[rows], k_sem.at[ring]),
                pltpu.make_async_copy(v_ring.at[ring], v_out.at[rows], v_sem.at[ring]))

    def step(piece, j, carry):
        ring = lax.rem(j, depth)

        @pl.when(j >= depth)
        def _():
            for copy in copies(j - depth):
                copy.wait()

        for n, (new, cache, out) in enumerate(((k_new, k_vm[piece], k_ring), (v_new, v_vm[piece], v_ring))):
            def group(i, carry):
                for m in range(8):
                    row = i * 8 + m
                    b = j * chunk + row
                    slot = (pos[b] & (window - 1)) - me * slots
                    base = pl.multiple_of((jnp.clip(slot, 0, slots - 1) // 16) * 16, 16)
                    out[ring, row] = cache[b - piece * part]
                    fresh = jnp.broadcast_to(new[pl.ds(b, 1), :], (16, HEAD_DIM))
                    old = cache[b - piece * part, pl.ds(base, 16), :].astype(F32)
                    out[ring, row, pl.ds(base, 16), :] = jnp.where(tile_row == slot - base, fresh, old).astype(BF16)
                return carry
            lax.fori_loop(0, chunk // 8, group, 0)
            copies(j)[n].start()
        return carry

    for piece in range(PIECES):
        lax.fori_loop(piece * span, (piece + 1) * span, functools.partial(step, piece), 0)
    for j in range(chunks - depth, chunks):
        for copy in copies(j):
            copy.wait()
    for copy in others:
        copy.wait()


def solution(mesh):
    kv_size = mesh.shape['kv']
    row_spec = P('dp', None)
    cache_spec = P('dp', 'kv', None)
    slot_spec = P('dp', 'kv')
    vec_spec = P(None)
    mat_spec = P(None, None)
    half_dims = ROPE_DIM // 2
    freq_row = np.tile(ROPE_BASE ** (-np.arange(half_dims) / half_dims), 2).astype(np.float32)[None, :]

    def local_step(x_in, positions, k_cache, v_cache, slot_pos, norm_scale, w_q, w_k, w_v, w_o, b_o):
        batch, model = x_in.shape
        slots = k_cache.shape[1]
        window = slots * kv_size
        width = w_q.shape[1]
        chunks = batch // (UNIT * CHUNK_UNITS)
        scattered = (SCATTER_LAST - SCATTER_FIRST) // 2
        hbm = pl.BlockSpec(memory_space=pltpu.HBM)
        vmem = pl.BlockSpec(memory_space=pltpu.VMEM)
        smem = pl.BlockSpec(memory_space=pltpu.SMEM)
        dma = pltpu.SemaphoreType.DMA
        per_chunk = [dma((chunks,))] * 4
        *held, x_new, k_new, v_new, sp_new = pl.pallas_call(
            functools.partial(attend_kernel, window),
            out_shape=(*([pltpu.VMEM((batch // PIECES, slots, HEAD_DIM), BF16)] * (2 * PIECES)), pltpu.VMEM((batch, model), BF16),
                       pltpu.VMEM((batch, HEAD_DIM), F32), pltpu.VMEM((batch, HEAD_DIM), F32), pltpu.VMEM((batch, slots), jnp.int32)),
            in_specs=[hbm] * 12,
            out_specs=(vmem,) * (2 * PIECES + 4),
            scratch_shapes=[
                pltpu.VMEM((batch // 128, 128), jnp.int32), pltpu.VMEM((1, 128), F32), pltpu.VMEM((batch, model), BF16), pltpu.VMEM((model,), BF16),
                pltpu.VMEM((model, HEAD_DIM), BF16), pltpu.VMEM((model, HEAD_DIM), BF16), pltpu.VMEM((model, width), BF16),
                pltpu.VMEM((batch, slots), jnp.int32), pltpu.VMEM((width, model), BF16), pltpu.VMEM((model,), BF16),
                pltpu.VMEM((batch, 128), F32), pltpu.VMEM((batch, model), F32), pltpu.VMEM((batch // UNIT, HEADS, UNIT, HEAD_DIM), F32),
                pltpu.VMEM((chunks, CHUNK_UNITS, PACKET, 128), F32), pltpu.VMEM((chunks, PACKET, 128), F32), pltpu.VMEM((chunks, 2, PACKET, 128), F32),
                pltpu.VMEM(((chunks - scattered) * UNIT, width), F32), pltpu.VMEM((kv_size, scattered * UNIT, model), F32),
                pltpu.VMEM((2, (chunks - 2 * scattered) * UNIT, model), F32),
                dma((10,)), dma((chunks,)), dma((chunks,)), *per_chunk, *([dma((len(SCATTER_GROUPS), 3))] * 2), *([dma((len(WHOLE_GROUPS),))] * 2)],
            compiler_params=pltpu.CompilerParams(vmem_limit_bytes=16 << 20, collective_id=0, has_side_effects=True),
            name='attend',
        )(*[pltpu.with_memory_space_constraint(a, pltpu.HBM) for a in (
            positions.reshape(batch // 128, 128), jnp.asarray(freq_row), x_in, norm_scale, w_k, w_v, w_q, slot_pos,
            w_o, b_o, k_cache, v_cache)])
        x_out, k_out, v_out, slot_pos_out = pl.pallas_call(
            functools.partial(write_kernel, window),
            out_shape=(jax.ShapeDtypeStruct((batch, model), BF16), jax.ShapeDtypeStruct(k_cache.shape, BF16),
                       jax.ShapeDtypeStruct(v_cache.shape, BF16), jax.ShapeDtypeStruct((batch, slots), jnp.int32)),
            in_specs=[smem] + [vmem] * (2 * PIECES + 4),
            out_specs=(hbm,) * 4,
            scratch_shapes=[pltpu.VMEM((4, 16, slots, HEAD_DIM), BF16), pltpu.VMEM((4, 16, slots, HEAD_DIM), BF16), dma((2,)), dma((4,)), dma((4,))],
            compiler_params=pltpu.CompilerParams(vmem_limit_bytes=9 << 20),
            name='write',
        )(positions, k_new, v_new, x_new, sp_new, *held)
        return x_out, k_out, v_out, slot_pos_out

    return jax.shard_map(
        local_step,
        mesh=mesh,
        in_specs=(row_spec, P('dp'), cache_spec, cache_spec, slot_spec, vec_spec, mat_spec, mat_spec, mat_spec, mat_spec, vec_spec),
        out_specs=(row_spec, cache_spec, cache_spec, slot_spec),
        check_vma=False)
```

```python
import functools
import numpy as np
import jax
import jax.numpy as jnp
from jax import lax
from jax.experimental import pallas as pl
from jax.experimental.pallas import tpu as pltpu
from jax.sharding import PartitionSpec as P

HEADS = 4
HEAD_DIM = 256
ROPE_DIM = 128
ROPE_BASE = 10000.0
EPS = 1e-6
NEG_LARGE = -1e30
SCORE_SCALE = HEAD_DIM ** -0.5

UNIT = 8
CHUNK_UNITS = 2
ROWS = UNIT * HEADS
PACKET = 2 * ROWS + 8
SCATTER_GROUPS = ((4, 8), (8, 12))
WHOLE_GROUPS = ((0, 4), (12, 14), (14, 16))
PIECES = 2
AHEAD = 6
FIRST_LAG = 2
SCATTER_FIRST, SCATTER_LAST = 4, 12
MESH = pl.DeviceIdType.MESH
F32 = jnp.float32
BF16 = jnp.bfloat16


def attend_kernel(window, pos_h, freq_h, x_h, ns_h, wk_h, wv_h, wq_h, sp_h, wo_h, bo_h, k_h, v_h,
                  *rest):
    k_vm, v_vm = rest[:PIECES], rest[PIECES:2 * PIECES]
    (x_new, k_new, v_new, sp_new,
                  pos, freq, x_in, ns, wk, wv, wq, sp, wo, bo,
                  pos_b, x_f, q_s, pk, rc1, ch, o_s, ag, agd,
                  in_sem, k_sem, v_sem, s1, r1, s2, r2, sa, ra, sd, rd) = rest[2 * PIECES:]
    me = lax.axis_index('kv')
    x_side, core = me // 2, me % 2
    over = {'kv': 2 * (1 - x_side) + core}
    beside = {'kv': 2 * x_side + 1 - core}
    over_i = 2 * (1 - x_side) + core
    batch, slots = sp.shape
    chunk = UNIT * CHUNK_UNITS
    chunks = batch // chunk

    barrier = pltpu.get_barrier_semaphore()
    pl.semaphore_signal(barrier, inc=1, device_id=over, device_id_type=MESH)
    pl.semaphore_signal(barrier, inc=1, device_id=beside, device_id_type=MESH)

    smalls = [pltpu.make_async_copy(src, dst, in_sem.at[n]) for n, (src, dst) in enumerate((
        (pos_h, pos), (freq_h, freq), (x_h, x_in), (ns_h, ns), (wk_h, wk), (wv_h, wv), (wq_h, wq), (sp_h, sp), (wo_h, wo), (bo_h, bo)))]

    span = chunks // PIECES

    def cache_copy(j, piece):
        rows, held = pl.ds(j * chunk, chunk), pl.ds((j - piece * span) * chunk, chunk)
        return (pltpu.make_async_copy(k_h.at[rows], k_vm[piece].at[held], k_sem.at[j]),
                pltpu.make_async_copy(v_h.at[rows], v_vm[piece].at[held], v_sem.at[j]))

    def read_ahead(first, last):
        for j in range(first, last):
            for copy in cache_copy(j, j // span):
                copy.start()

    for small in smalls[:8]:
        small.start()
    read_ahead(0, 1)

    smalls[0].wait()
    smalls[1].wait()
    for r in range(batch // 128):
        row = pos[r:r + 1, :].astype(F32)
        pos_b[pl.ds(128 * r, 128), :] = jnp.transpose(jnp.broadcast_to(row, (128, 128)))
    read_ahead(1, 2)
    half = batch // 2
    low = lax.broadcasted_iota(jnp.int32, (half, 128), 1) < ROPE_DIM // 2
    angles = jnp.where(low, pos_b[:half, :], pos_b[half:, :]) * freq[...]

    def spread_halves(table, sign):
        turned = pltpu.roll(table, ROPE_DIM // 2, 1)
        return jnp.concatenate([jnp.where(low, sign * table, turned), jnp.where(low, sign * turned, table)], axis=0)

    cos_t = spread_halves(jnp.cos(angles), 1.0)
    sin_t = spread_halves(jnp.sin(angles), -1.0)

    def rotate(first):
        return first * cos_t + pltpu.roll(first, ROPE_DIM // 2, 1) * sin_t

    smalls[2].wait()
    smalls[3].wait()
    read_ahead(2, AHEAD)
    x32 = x_in[...].astype(F32)
    x_f[...] = x32
    mean_sq = jnp.mean(x32 * x32, axis=-1, keepdims=True)
    normed = (x32 * lax.rsqrt(mean_sq + EPS) * (1.0 + ns[...].astype(F32)[None, :])).astype(BF16)
    smalls[4].wait()
    smalls[5].wait()
    k_row = jnp.dot(normed, wk[...], preferred_element_type=F32)
    k_new[:, :128] = rotate(k_row[:, :128]).astype(BF16).astype(F32)
    k_new[:, 128:] = k_row[:, 128:].astype(BF16).astype(F32)
    v_new[...] = jnp.dot(normed, wv[...], preferred_element_type=F32).astype(BF16).astype(F32)
    smalls[6].wait()
    for small in smalls[8:]:
        small.start()
    for h in range(HEADS):
        q_row = jnp.dot(normed, wq[:, h * HEAD_DIM:(h + 1) * HEAD_DIM], preferred_element_type=F32)
        q_s[:, h, :, :128] = rotate(q_row[:, :128]).reshape(batch // UNIT, UNIT, 128)
        q_s[:, h, :, 128:] = q_row[:, 128:].reshape(batch // UNIT, UNIT, 128)
    smalls[7].wait()
    pl.semaphore_wait(barrier, 2)

    lane = lax.broadcasted_iota(jnp.int32, (UNIT, 128), 1)
    row_seq = lax.broadcasted_iota(jnp.int32, (ROWS, 128), 0) % UNIT

    def scores_of(u, piece):
        keys = k_vm[piece][pl.ds(u * UNIT - piece * span * chunk, UNIT)].reshape(UNIT * slots, HEAD_DIM)
        q_b = q_s[u].reshape(ROWS, HEAD_DIM).astype(BF16)
        return q_b, lax.dot_general(q_b, keys, (((1,), (1,)), ((), ())), preferred_element_type=F32)

    def weights_of(u, q_b, all_scores):
        seqs = pl.ds(u * UNIT, UNIT)
        scores = all_scores[:, :slots]
        for s in range(1, UNIT):
            scores = jnp.where(row_seq == s, all_scores[:, s * slots:(s + 1) * slots], scores)
        p_now = pos_b[seqs, :].astype(jnp.int32)
        slot = (p_now & (window - 1)) - me * slots
        hit = lane == slot
        held = jnp.where(hit, p_now, sp[seqs, :])
        sp_new[seqs, :] = held
        age = p_now - held
        usable = (held >= 0) & (age >= 0) & (age < window)
        fresh = jnp.sum(q_b.astype(F32).reshape(HEADS, UNIT, HEAD_DIM) * k_new[seqs, :][None], axis=-1, keepdims=True)
        scores = jnp.where(hit[None], fresh, scores.reshape(HEADS, UNIT, slots)) * SCORE_SCALE
        scores = jnp.where(usable[None], scores, NEG_LARGE)
        top = jnp.max(scores, axis=-1, keepdims=True)
        weights = jnp.where(usable[None], jnp.exp(scores - top), 0.0)
        total = jnp.sum(weights, axis=-1, keepdims=True)
        fresh_weight = jnp.sum(jnp.where(hit[None], weights, 0.0), axis=-1, keepdims=True)
        kept = jnp.where(hit[None], 0.0, weights).reshape(ROWS, slots)
        spread = jnp.concatenate([jnp.where(row_seq == s, kept, 0.0).astype(BF16) for s in range(UNIT)], axis=1)
        return top, total, fresh_weight, spread

    def sums_of(u, piece, fresh_weight, spread):
        values = v_vm[piece][pl.ds(u * UNIT - piece * span * chunk, UNIT)].reshape(UNIT * slots, HEAD_DIM)
        sums = jnp.dot(spread, values, preferred_element_type=F32).reshape(HEADS, UNIT, HEAD_DIM)
        sums = sums + fresh_weight.astype(BF16).astype(F32) * v_new[pl.ds(u * UNIT, UNIT), :][None]
        return sums.reshape(ROWS, HEAD_DIM)

    def attend(j, piece):
        units = [j * CHUNK_UNITS + i for i in range(2 * CHUNK_UNITS)]
        scored = [scores_of(u, piece) for u in units]
        weighed = [weights_of(u, *pair) for u, pair in zip(units, scored)]
        for i, u in enumerate(units):
            top, total, fresh_weight, spread = weighed[i]
            sums = sums_of(u, piece, fresh_weight, spread)
            n, i = j + i // CHUNK_UNITS, i % CHUNK_UNITS
            pk[n, i, 0:ROWS, :] = sums[:, :128]
            pk[n, i, ROWS:2 * ROWS, :] = sums[:, 128:]
            tile = jnp.zeros((UNIT, 128), F32)
            for h in range(HEADS):
                tile = jnp.where(lane == h, top[h], jnp.where(lane == HEADS + h, total[h], tile))
            pk[n, i, 2 * ROWS:, :] = tile

    def merge(a, b):
        ta, tb = a[2 * ROWS:, :], b[2 * ROWS:, :]
        tile = jnp.maximum(ta, tb)
        ea, eb = jnp.exp(ta - tile), jnp.exp(tb - tile)
        parts, totals = [], []
        for h in range(HEADS):
            fa, fb = ea[:, h:h + 1], eb[:, h:h + 1]
            totals.append(fa * ta[:, HEADS + h:HEADS + h + 1] + fb * tb[:, HEADS + h:HEADS + h + 1])
            parts.append([fa * a[o + h * UNIT:o + (h + 1) * UNIT, :] + fb * b[o + h * UNIT:o + (h + 1) * UNIT, :] for o in (0, ROWS)])
        return tile, parts, totals

    sequence = lax.broadcasted_iota(jnp.int32, (UNIT, 128), 0)

    def pack(tile, totals):
        spots = jnp.zeros((UNIT, 128), F32)
        for h in range(HEADS):
            spots = jnp.where(lane == h * UNIT + sequence, tile[:, h:h + 1], spots)
            spots = jnp.where(lane == ROWS + h * UNIT + sequence, totals[h], spots)
        return jnp.sum(spots, axis=0, keepdims=True)

    def unpack(row):
        spots = jnp.broadcast_to(row, (UNIT, 128))
        columns = [jnp.sum(jnp.where(lane == n * UNIT + sequence, spots, 0.0), axis=1, keepdims=True) for n in range(2 * HEADS)]
        return columns[:HEADS], columns[HEADS:]

    def merge_packed(a, b):
        (tops_a, totals_a), (tops_b, totals_b) = unpack(a[2 * ROWS:2 * ROWS + 1, :]), unpack(b[2 * ROWS:2 * ROWS + 1, :])
        parts, totals = [], []
        for h in range(HEADS):
            top = jnp.maximum(tops_a[h], tops_b[h])
            fa, fb = jnp.exp(tops_a[h] - top), jnp.exp(tops_b[h] - top)
            totals.append(fa * totals_a[h] + fb * totals_b[h])
            parts.append([fa * a[o + h * UNIT:o + (h + 1) * UNIT, :] + fb * b[o + h * UNIT:o + (h + 1) * UNIT, :] for o in (0, ROWS)])
        return parts, totals

    def first_copy(j):
        return pltpu.make_async_remote_copy(pk.at[j, 1 - core], rc1.at[j], s1.at[j], r1.at[j], device_id=beside, device_id_type=MESH)

    def second_copy(j):
        rows = ch.at[j, x_side, pl.ds(0, 2 * ROWS + 1)]
        return pltpu.make_async_remote_copy(rows, rows, s2.at[j], r2.at[j], device_id=over, device_id_type=MESH)

    def either(condition, yes, no):
        if isinstance(condition, bool):
            return yes() if condition else no()
        pl.when(condition)(yes)
        pl.when(jnp.logical_not(condition))(no)

    def is_whole(j):
        return (j < SCATTER_FIRST or j >= SCATTER_LAST) if isinstance(j, int) else (j < SCATTER_FIRST) | (j >= SCATTER_LAST)

    def first_merge(j):
        pair = (j, j + 1)
        for n in pair:
            first_copy(n).wait_recv()
        merged = [merge(pk[n, core], rc1[n]) for n in pair]
        for n, (tile, parts, totals) in zip(pair, merged):
            for h in range(HEADS):
                ch[n, x_side, h * UNIT:(h + 1) * UNIT, :] = parts[h][0]
                ch[n, x_side, ROWS + h * UNIT:ROWS + (h + 1) * UNIT, :] = parts[h][1]
            ch[n, x_side, 2 * ROWS:2 * ROWS + 1, :] = pack(tile, totals)

        def both():
            for n in pair:
                second_copy(n).start()

        either(is_whole(j), both, lambda: second_copy(j + 1 - x_side).start())

    scattered = (SCATTER_LAST - SCATTER_FIRST) // 2

    def final_block(j):
        if isinstance(j, int):
            return j if j < SCATTER_FIRST else SCATTER_FIRST + (j - SCATTER_FIRST) // 2 if j < SCATTER_LAST else j - scattered
        return jnp.where(j < SCATTER_FIRST, j, jnp.where(j < SCATTER_LAST, SCATTER_FIRST + (j - SCATTER_FIRST) // 2, j - scattered))

    def whole_block(j):
        return j if j < SCATTER_FIRST else j - 2 * scattered

    def finish(*chunk_ids):
        for n in chunk_ids:
            second_copy(n).wait_recv()
        merged = [merge_packed(ch[n, 0], ch[n, 1]) for n in chunk_ids]
        for n, (parts, totals) in zip(chunk_ids, merged):
            rows = pl.ds(final_block(n) * UNIT, UNIT)
            for h in range(HEADS):
                inverse = 1.0 / totals[h]
                o_s[rows, h * HEAD_DIM:h * HEAD_DIM + 128] = parts[h][0] * inverse
                o_s[rows, h * HEAD_DIM + 128:(h + 1) * HEAD_DIM] = parts[h][1] * inverse

    def second_merge(j):
        either(is_whole(j), lambda: finish(j, j + 1), lambda: finish(j + x_side))

    def project(first, residual):
        rows = pl.ds(first, residual.shape[0])
        return residual + jnp.dot(o_s[rows, :].astype(BF16), wo[...], preferred_element_type=F32) + bo[...].astype(F32)[None, :]

    def gather_copy(g, owner, target, n):
        first, last = SCATTER_GROUPS[g]
        rows = ag.at[owner, pl.ds((first - SCATTER_FIRST) // 2 * UNIT, (last - first) // 2 * UNIT)]
        return pltpu.make_async_remote_copy(rows, rows, sa.at[g, n], ra.at[g, n], device_id=target, device_id_type=MESH)

    gathers = [(gather_copy(g, me, over, 0), gather_copy(g, me, beside, 1), gather_copy(g, over_i, beside, 2)) for g in range(len(SCATTER_GROUPS))]

    def project_scattered(g):
        first, last = SCATTER_GROUPS[g]
        residual = jnp.concatenate([x_f[pl.ds((n + x_side) * chunk + core * UNIT, UNIT), :] for n in range(first, last, 2)], axis=0)
        start = (first - SCATTER_FIRST) // 2 * UNIT
        ag[me, start:start + residual.shape[0], :] = project(SCATTER_FIRST * UNIT + start, residual)
        gathers[g][0].start()
        gathers[g][1].start()

    def forward(g):
        gathers[g][0].wait_recv()
        gathers[g][2].start()

    def collect_scattered(g):
        gathers[g][1].wait_recv()
        gathers[g][2].wait_recv()
        for j in range(*SCATTER_GROUPS[g]):
            i = (j - SCATTER_FIRST) // 2
            rows = [ag[2 * (j % 2) + c, i * UNIT:(i + 1) * UNIT, :] for c in range(2)]
            x_new[j * chunk:(j + 1) * chunk, :] = jnp.concatenate(rows, axis=0).astype(BF16)

    def beside_copy(g):
        first, last = WHOLE_GROUPS[g]
        rows = agd.at[core, pl.ds(whole_block(first) * UNIT, (last - first) * UNIT)]
        return pltpu.make_async_remote_copy(rows, rows, sd.at[g], rd.at[g], device_id=beside, device_id_type=MESH)

    def project_whole(g):
        first, last = WHOLE_GROUPS[g]
        residual = jnp.concatenate([x_f[pl.ds(j * chunk + core * UNIT, UNIT), :] for j in range(first, last)], axis=0)
        agd[core, whole_block(first) * UNIT:whole_block(last - 1) * UNIT + UNIT, :] = project(final_block(first) * UNIT, residual)
        beside_copy(g).start()

    def collect_whole(g):
        beside_copy(g).wait_recv()
        for j in range(*WHOLE_GROUPS[g]):
            rows = [agd[c, whole_block(j) * UNIT:(whole_block(j) + 1) * UNIT, :] for c in range(2)]
            x_new[j * chunk:(j + 1) * chunk, :] = jnp.concatenate(rows, axis=0).astype(BF16)

    def step(piece, block, carry):
        j = 2 * block
        for n in range(2):
            for copy in cache_copy(j + n, piece):
                copy.wait()
        attend(j, piece)
        for n in range(2):
            first_copy(j + n).start()

        @pl.when(j >= FIRST_LAG)
        def _():
            first_merge(j - FIRST_LAG)

        for ahead in range(PIECES):
            @pl.when((j + AHEAD < chunks) & ((j + AHEAD) // span == ahead))
            def _():
                for n in range(2):
                    for copy in cache_copy(j + AHEAD + n, ahead):
                        copy.start()

        return carry

    for piece in range(PIECES):
        lax.fori_loop(piece * span // 2, (piece + 1) * span // 2, functools.partial(step, piece), 0)
    for small in smalls[8:]:
        small.wait()
    def second_merges(first, last):
        for j in range(first, last, 2):
            second_merge(j)

    def drain(j, carry):
        first_copy(j).wait_send()

        @pl.when((j < SCATTER_FIRST) | (j >= SCATTER_LAST) | (j % 2 != x_side))
        def _():
            second_copy(j).wait_send()
        return carry

    second_merges(*SCATTER_GROUPS[0])
    project_scattered(0)
    for j in range(chunks - FIRST_LAG, chunks, 2):
        first_merge(j)
    second_merges(*WHOLE_GROUPS[0])
    project_whole(0)
    second_merges(*SCATTER_GROUPS[1])
    project_scattered(1)
    forward(0)
    collect_whole(0)
    second_merges(*WHOLE_GROUPS[1])
    project_whole(1)
    collect_scattered(0)
    lax.fori_loop(0, chunks, drain, 0)
    second_merges(*WHOLE_GROUPS[2])
    project_whole(2)
    forward(1)
    collect_whole(1)
    collect_scattered(1)
    collect_whole(2)
    for group in gathers:
        for gather in group:
            gather.wait_send()
    for g in range(len(WHOLE_GROUPS)):
        beside_copy(g).wait_send()


def write_kernel(window, pos, k_new, v_new, x_new, sp_new, *rest):
    k_vm, v_vm = rest[:PIECES], rest[PIECES:2 * PIECES]
    x_out, k_out, v_out, sp_out, k_ring, v_ring, sems, k_sem, v_sem = rest[2 * PIECES:]
    me = lax.axis_index('kv')
    part, slots, _ = k_vm[0].shape
    batch = part * PIECES
    depth, chunk = k_ring.shape[:2]
    chunks = batch // chunk
    span = chunks // PIECES
    others = (pltpu.make_async_copy(x_new, x_out, sems.at[0]), pltpu.make_async_copy(sp_new, sp_out, sems.at[1]))
    for copy in others:
        copy.start()
    tile_row = lax.broadcasted_iota(jnp.int32, (16, HEAD_DIM), 0)

    def copies(j):
        rows, ring = pl.ds(j * chunk, chunk), lax.rem(j, depth)
        return (pltpu.make_async_copy(k_ring.at[ring], k_out.at[rows], k_sem.at[ring]),
                pltpu.make_async_copy(v_ring.at[ring], v_out.at[rows], v_sem.at[ring]))

    def step(piece, j, carry):
        ring = lax.rem(j, depth)

        @pl.when(j >= depth)
        def _():
            for copy in copies(j - depth):
                copy.wait()

        for n, (new, cache, out) in enumerate(((k_new, k_vm[piece], k_ring), (v_new, v_vm[piece], v_ring))):
            def group(i, carry):
                for m in range(8):
                    row = i * 8 + m
                    b = j * chunk + row
                    slot = (pos[b] & (window - 1)) - me * slots
                    base = pl.multiple_of((jnp.clip(slot, 0, slots - 1) // 16) * 16, 16)
                    out[ring, row] = cache[b - piece * part]
                    fresh = jnp.broadcast_to(new[pl.ds(b, 1), :], (16, HEAD_DIM))
                    old = cache[b - piece * part, pl.ds(base, 16), :].astype(F32)
                    out[ring, row, pl.ds(base, 16), :] = jnp.where(tile_row == slot - base, fresh, old).astype(BF16)
                return carry
            lax.fori_loop(0, chunk // 8, group, 0)
            copies(j)[n].start()
        return carry

    for piece in range(PIECES):
        lax.fori_loop(piece * span, (piece + 1) * span, functools.partial(step, piece), 0)
    for j in range(chunks - depth, chunks):
        for copy in copies(j):
            copy.wait()
    for copy in others:
        copy.wait()


def solution(mesh):
    kv_size = mesh.shape['kv']
    row_spec = P('dp', None)
    cache_spec = P('dp', 'kv', None)
    slot_spec = P('dp', 'kv')
    vec_spec = P(None)
    mat_spec = P(None, None)
    half_dims = ROPE_DIM // 2
    freq_row = np.tile(ROPE_BASE ** (-np.arange(half_dims) / half_dims), 2).astype(np.float32)[None, :]

    def local_step(x_in, positions, k_cache, v_cache, slot_pos, norm_scale, w_q, w_k, w_v, w_o, b_o):
        batch, model = x_in.shape
        slots = k_cache.shape[1]
        window = slots * kv_size
        width = w_q.shape[1]
        chunks = batch // (UNIT * CHUNK_UNITS)
        scattered = (SCATTER_LAST - SCATTER_FIRST) // 2
        hbm = pl.BlockSpec(memory_space=pltpu.HBM)
        vmem = pl.BlockSpec(memory_space=pltpu.VMEM)
        smem = pl.BlockSpec(memory_space=pltpu.SMEM)
        dma = pltpu.SemaphoreType.DMA
        per_chunk = [dma((chunks,))] * 4
        *held, x_new, k_new, v_new, sp_new = pl.pallas_call(
            functools.partial(attend_kernel, window),
            out_shape=(*([pltpu.VMEM((batch // PIECES, slots, HEAD_DIM), BF16)] * (2 * PIECES)), pltpu.VMEM((batch, model), BF16),
                       pltpu.VMEM((batch, HEAD_DIM), F32), pltpu.VMEM((batch, HEAD_DIM), F32), pltpu.VMEM((batch, slots), jnp.int32)),
            in_specs=[hbm] * 12,
            out_specs=(vmem,) * (2 * PIECES + 4),
            scratch_shapes=[
                pltpu.VMEM((batch // 128, 128), jnp.int32), pltpu.VMEM((1, 128), F32), pltpu.VMEM((batch, model), BF16), pltpu.VMEM((model,), BF16),
                pltpu.VMEM((model, HEAD_DIM), BF16), pltpu.VMEM((model, HEAD_DIM), BF16), pltpu.VMEM((model, width), BF16),
                pltpu.VMEM((batch, slots), jnp.int32), pltpu.VMEM((width, model), BF16), pltpu.VMEM((model,), BF16),
                pltpu.VMEM((batch, 128), F32), pltpu.VMEM((batch, model), F32), pltpu.VMEM((batch // UNIT, HEADS, UNIT, HEAD_DIM), F32),
                pltpu.VMEM((chunks, CHUNK_UNITS, PACKET, 128), F32), pltpu.VMEM((chunks, PACKET, 128), F32), pltpu.VMEM((chunks, 2, PACKET, 128), F32),
                pltpu.VMEM(((chunks - scattered) * UNIT, width), F32), pltpu.VMEM((kv_size, scattered * UNIT, model), F32),
                pltpu.VMEM((2, (chunks - 2 * scattered) * UNIT, model), F32),
                dma((10,)), dma((chunks,)), dma((chunks,)), *per_chunk, *([dma((len(SCATTER_GROUPS), 3))] * 2), *([dma((len(WHOLE_GROUPS),))] * 2)],
            compiler_params=pltpu.CompilerParams(vmem_limit_bytes=16 << 20, collective_id=0, has_side_effects=True),
            name='attend',
        )(*[pltpu.with_memory_space_constraint(a, pltpu.HBM) for a in (
            positions.reshape(batch // 128, 128), jnp.asarray(freq_row), x_in, norm_scale, w_k, w_v, w_q, slot_pos,
            w_o, b_o, k_cache, v_cache)])
        x_out, k_out, v_out, slot_pos_out = pl.pallas_call(
            functools.partial(write_kernel, window),
            out_shape=(jax.ShapeDtypeStruct((batch, model), BF16), jax.ShapeDtypeStruct(k_cache.shape, BF16),
                       jax.ShapeDtypeStruct(v_cache.shape, BF16), jax.ShapeDtypeStruct((batch, slots), jnp.int32)),
            in_specs=[smem] + [vmem] * (2 * PIECES + 4),
            out_specs=(hbm,) * 4,
            scratch_shapes=[pltpu.VMEM((4, 16, slots, HEAD_DIM), BF16), pltpu.VMEM((4, 16, slots, HEAD_DIM), BF16), dma((2,)), dma((4,)), dma((4,))],
            compiler_params=pltpu.CompilerParams(vmem_limit_bytes=9 << 20),
            name='write',
        )(positions, k_new, v_new, x_new, sp_new, *held)
        return x_out, k_out, v_out, slot_pos_out

    return jax.shard_map(
        local_step,
        mesh=mesh,
        in_specs=(row_spec, P('dp'), cache_spec, cache_spec, slot_spec, vec_spec, mat_spec, mat_spec, mat_spec, mat_spec, vec_spec),
        out_specs=(row_spec, cache_spec, cache_spec, slot_spec),
        check_vma=False)
```

```python
import functools
import numpy as np
import jax
import jax.numpy as jnp
from jax import lax
from jax.experimental import pallas as pl
from jax.experimental.pallas import tpu as pltpu
from jax.sharding import PartitionSpec as P

HEADS = 4
HEAD_DIM = 256
ROPE_DIM = 128
ROPE_BASE = 10000.0
EPS = 1e-6
NEG_LARGE = -1e30
SCORE_SCALE = HEAD_DIM ** -0.5

UNIT = 8
CHUNK_UNITS = 2
ROWS = UNIT * HEADS
PACKET = 2 * ROWS + 8
SCATTER_GROUPS = ((4, 8), (8, 12))
WHOLE_GROUPS = ((0, 4), (12, 14), (14, 16))
PIECES = 2
AHEAD = 6
FIRST_LAG = 2
SCATTER_FIRST, SCATTER_LAST = 4, 12
MESH = pl.DeviceIdType.MESH
F32 = jnp.float32
BF16 = jnp.bfloat16


def attend_kernel(window, pos_h, freq_h, x_h, ns_h, wk_h, wv_h, wq_h, sp_h, wo_h, bo_h, k_h, v_h,
                  *rest):
    k_vm, v_vm = rest[:PIECES], rest[PIECES:2 * PIECES]
    (x_new, k_new, v_new, sp_new,
                  pos, freq, x_in, ns, wk, wv, wq, sp, wo, bo,
                  pos_b, x_f, q_s, pk, rc1, ch, o_s, ag, agd,
                  in_sem, k_sem, v_sem, s1, r1, s2, r2, sa, ra, sd, rd) = rest[2 * PIECES:]
    me = lax.axis_index('kv')
    x_side, core = me // 2, me % 2
    over = {'kv': 2 * (1 - x_side) + core}
    beside = {'kv': 2 * x_side + 1 - core}
    over_i = 2 * (1 - x_side) + core
    batch, slots = sp.shape
    chunk = UNIT * CHUNK_UNITS
    chunks = batch // chunk

    barrier = pltpu.get_barrier_semaphore()
    pl.semaphore_signal(barrier, inc=1, device_id=over, device_id_type=MESH)
    pl.semaphore_signal(barrier, inc=1, device_id=beside, device_id_type=MESH)

    smalls = [pltpu.make_async_copy(src, dst, in_sem.at[n]) for n, (src, dst) in enumerate((
        (pos_h, pos), (freq_h, freq), (x_h, x_in), (ns_h, ns), (wk_h, wk), (wv_h, wv), (wq_h, wq), (sp_h, sp), (wo_h, wo), (bo_h, bo)))]

    span = chunks // PIECES

    def cache_copy(j, piece):
        rows, held = pl.ds(j * chunk, chunk), pl.ds((j - piece * span) * chunk, chunk)
        return (pltpu.make_async_copy(k_h.at[rows], k_vm[piece].at[held], k_sem.at[j]),
                pltpu.make_async_copy(v_h.at[rows], v_vm[piece].at[held], v_sem.at[j]))

    def read_ahead(first, last):
        for j in range(first, last):
            for copy in cache_copy(j, j // span):
                copy.start()

    for small in smalls[:8]:
        small.start()
    read_ahead(0, 2)

    smalls[0].wait()
    smalls[1].wait()
    for r in range(batch // 128):
        row = pos[r:r + 1, :].astype(F32)
        pos_b[pl.ds(128 * r, 128), :] = jnp.transpose(jnp.broadcast_to(row, (128, 128)))
    half = batch // 2
    low = lax.broadcasted_iota(jnp.int32, (half, 128), 1) < ROPE_DIM // 2
    angles = jnp.where(low, pos_b[:half, :], pos_b[half:, :]) * freq[...]

    def spread_halves(table, sign):
        turned = pltpu.roll(table, ROPE_DIM // 2, 1)
        return jnp.concatenate([jnp.where(low, sign * table, turned), jnp.where(low, sign * turned, table)], axis=0)

    cos_t = spread_halves(jnp.cos(angles), 1.0)
    sin_t = spread_halves(jnp.sin(angles), -1.0)

    def rotate(first):
        return first * cos_t + pltpu.roll(first, ROPE_DIM // 2, 1) * sin_t

    smalls[2].wait()
    smalls[3].wait()
    read_ahead(2, 4)
    x32 = x_in[...].astype(F32)
    x_f[...] = x32
    mean_sq = jnp.mean(x32 * x32, axis=-1, keepdims=True)
    normed = (x32 * lax.rsqrt(mean_sq + EPS) * (1.0 + ns[...].astype(F32)[None, :])).astype(BF16)
    smalls[4].wait()
    smalls[5].wait()
    k_row = jnp.dot(normed, wk[...], preferred_element_type=F32)
    k_new[:, :128] = rotate(k_row[:, :128]).astype(BF16).astype(F32)
    k_new[:, 128:] = k_row[:, 128:].astype(BF16).astype(F32)
    v_new[...] = jnp.dot(normed, wv[...], preferred_element_type=F32).astype(BF16).astype(F32)
    smalls[6].wait()
    read_ahead(4, AHEAD)
    for small in smalls[8:]:
        small.start()
    for h in range(HEADS):
        q_row = jnp.dot(normed, wq[:, h * HEAD_DIM:(h + 1) * HEAD_DIM], preferred_element_type=F32)
        q_s[:, h, :, :128] = rotate(q_row[:, :128]).reshape(batch // UNIT, UNIT, 128)
        q_s[:, h, :, 128:] = q_row[:, 128:].reshape(batch // UNIT, UNIT, 128)
    smalls[7].wait()
    pl.semaphore_wait(barrier, 2)

    lane = lax.broadcasted_iota(jnp.int32, (UNIT, 128), 1)
    row_seq = lax.broadcasted_iota(jnp.int32, (ROWS, 128), 0) % UNIT

    def scores_of(u, piece):
        keys = k_vm[piece][pl.ds(u * UNIT - piece * span * chunk, UNIT)].reshape(UNIT * slots, HEAD_DIM)
        q_b = q_s[u].reshape(ROWS, HEAD_DIM).astype(BF16)
        return q_b, lax.dot_general(q_b, keys, (((1,), (1,)), ((), ())), preferred_element_type=F32)

    def weights_of(u, q_b, all_scores):
        seqs = pl.ds(u * UNIT, UNIT)
        scores = all_scores[:, :slots]
        for s in range(1, UNIT):
            scores = jnp.where(row_seq == s, all_scores[:, s * slots:(s + 1) * slots], scores)
        p_now = pos_b[seqs, :].astype(jnp.int32)
        slot = (p_now & (window - 1)) - me * slots
        hit = lane == slot
        held = jnp.where(hit, p_now, sp[seqs, :])
        sp_new[seqs, :] = held
        age = p_now - held
        usable = (held >= 0) & (age >= 0) & (age < window)
        fresh = jnp.sum(q_b.astype(F32).reshape(HEADS, UNIT, HEAD_DIM) * k_new[seqs, :][None], axis=-1, keepdims=True)
        scores = jnp.where(hit[None], fresh, scores.reshape(HEADS, UNIT, slots)) * SCORE_SCALE
        scores = jnp.where(usable[None], scores, NEG_LARGE)
        top = jnp.max(scores, axis=-1, keepdims=True)
        weights = jnp.where(usable[None], jnp.exp(scores - top), 0.0)
        total = jnp.sum(weights, axis=-1, keepdims=True)
        fresh_weight = jnp.sum(jnp.where(hit[None], weights, 0.0), axis=-1, keepdims=True)
        kept = jnp.where(hit[None], 0.0, weights).reshape(ROWS, slots)
        spread = jnp.concatenate([jnp.where(row_seq == s, kept, 0.0).astype(BF16) for s in range(UNIT)], axis=1)
        return top, total, fresh_weight, spread

    def sums_of(u, piece, fresh_weight, spread):
        values = v_vm[piece][pl.ds(u * UNIT - piece * span * chunk, UNIT)].reshape(UNIT * slots, HEAD_DIM)
        sums = jnp.dot(spread, values, preferred_element_type=F32).reshape(HEADS, UNIT, HEAD_DIM)
        sums = sums + fresh_weight.astype(BF16).astype(F32) * v_new[pl.ds(u * UNIT, UNIT), :][None]
        return sums.reshape(ROWS, HEAD_DIM)

    def attend(j, piece):
        units = [j * CHUNK_UNITS + i for i in range(2 * CHUNK_UNITS)]
        scored = [scores_of(u, piece) for u in units]
        weighed = [weights_of(u, *pair) for u, pair in zip(units, scored)]
        for i, u in enumerate(units):
            top, total, fresh_weight, spread = weighed[i]
            sums = sums_of(u, piece, fresh_weight, spread)
            n, i = j + i // CHUNK_UNITS, i % CHUNK_UNITS
            pk[n, i, 0:ROWS, :] = sums[:, :128]
            pk[n, i, ROWS:2 * ROWS, :] = sums[:, 128:]
            tile = jnp.zeros((UNIT, 128), F32)
            for h in range(HEADS):
                tile = jnp.where(lane == h, top[h], jnp.where(lane == HEADS + h, total[h], tile))
            pk[n, i, 2 * ROWS:, :] = tile

    def merge(a, b):
        ta, tb = a[2 * ROWS:, :], b[2 * ROWS:, :]
        tile = jnp.maximum(ta, tb)
        ea, eb = jnp.exp(ta - tile), jnp.exp(tb - tile)
        parts, totals = [], []
        for h in range(HEADS):
            fa, fb = ea[:, h:h + 1], eb[:, h:h + 1]
            totals.append(fa * ta[:, HEADS + h:HEADS + h + 1] + fb * tb[:, HEADS + h:HEADS + h + 1])
            parts.append([fa * a[o + h * UNIT:o + (h + 1) * UNIT, :] + fb * b[o + h * UNIT:o + (h + 1) * UNIT, :] for o in (0, ROWS)])
        return tile, parts, totals

    sequence = lax.broadcasted_iota(jnp.int32, (UNIT, 128), 0)

    def pack(tile, totals):
        spots = jnp.zeros((UNIT, 128), F32)
        for h in range(HEADS):
            spots = jnp.where(lane == h * UNIT + sequence, tile[:, h:h + 1], spots)
            spots = jnp.where(lane == ROWS + h * UNIT + sequence, totals[h], spots)
        return jnp.sum(spots, axis=0, keepdims=True)

    def unpack(row):
        spots = jnp.broadcast_to(row, (UNIT, 128))
        columns = [jnp.sum(jnp.where(lane == n * UNIT + sequence, spots, 0.0), axis=1, keepdims=True) for n in range(2 * HEADS)]
        return columns[:HEADS], columns[HEADS:]

    def merge_packed(a, b):
        (tops_a, totals_a), (tops_b, totals_b) = unpack(a[2 * ROWS:2 * ROWS + 1, :]), unpack(b[2 * ROWS:2 * ROWS + 1, :])
        parts, totals = [], []
        for h in range(HEADS):
            top = jnp.maximum(tops_a[h], tops_b[h])
            fa, fb = jnp.exp(tops_a[h] - top), jnp.exp(tops_b[h] - top)
            totals.append(fa * totals_a[h] + fb * totals_b[h])
            parts.append([fa * a[o + h * UNIT:o + (h + 1) * UNIT, :] + fb * b[o + h * UNIT:o + (h + 1) * UNIT, :] for o in (0, ROWS)])
        return parts, totals

    def first_copy(j):
        return pltpu.make_async_remote_copy(pk.at[j, 1 - core], rc1.at[j], s1.at[j], r1.at[j], device_id=beside, device_id_type=MESH)

    def second_copy(j):
        rows = ch.at[j, x_side, pl.ds(0, 2 * ROWS + 1)]
        return pltpu.make_async_remote_copy(rows, rows, s2.at[j], r2.at[j], device_id=over, device_id_type=MESH)

    def either(condition, yes, no):
        if isinstance(condition, bool):
            return yes() if condition else no()
        pl.when(condition)(yes)
        pl.when(jnp.logical_not(condition))(no)

    def is_whole(j):
        return (j < SCATTER_FIRST or j >= SCATTER_LAST) if isinstance(j, int) else (j < SCATTER_FIRST) | (j >= SCATTER_LAST)

    def first_merge(j):
        pair = (j, j + 1)
        for n in pair:
            first_copy(n).wait_recv()
        merged = [merge(pk[n, core], rc1[n]) for n in pair]
        for n, (tile, parts, totals) in zip(pair, merged):
            for h in range(HEADS):
                ch[n, x_side, h * UNIT:(h + 1) * UNIT, :] = parts[h][0]
                ch[n, x_side, ROWS + h * UNIT:ROWS + (h + 1) * UNIT, :] = parts[h][1]
            ch[n, x_side, 2 * ROWS:2 * ROWS + 1, :] = pack(tile, totals)

        def both():
            for n in pair:
                second_copy(n).start()

        either(is_whole(j), both, lambda: second_copy(j + 1 - x_side).start())

    scattered = (SCATTER_LAST - SCATTER_FIRST) // 2

    def final_block(j):
        if isinstance(j, int):
            return j if j < SCATTER_FIRST else SCATTER_FIRST + (j - SCATTER_FIRST) // 2 if j < SCATTER_LAST else j - scattered
        return jnp.where(j < SCATTER_FIRST, j, jnp.where(j < SCATTER_LAST, SCATTER_FIRST + (j - SCATTER_FIRST) // 2, j - scattered))

    def whole_block(j):
        return j if j < SCATTER_FIRST else j - 2 * scattered

    def finish(*chunk_ids):
        for n in chunk_ids:
            second_copy(n).wait_recv()
        merged = [merge_packed(ch[n, 0], ch[n, 1]) for n in chunk_ids]
        for n, (parts, totals) in zip(chunk_ids, merged):
            rows = pl.ds(final_block(n) * UNIT, UNIT)
            for h in range(HEADS):
                inverse = 1.0 / totals[h]
                o_s[rows, h * HEAD_DIM:h * HEAD_DIM + 128] = parts[h][0] * inverse
                o_s[rows, h * HEAD_DIM + 128:(h + 1) * HEAD_DIM] = parts[h][1] * inverse

    def second_merge(j):
        either(is_whole(j), lambda: finish(j, j + 1), lambda: finish(j + x_side))

    def project(first, residual):
        rows = pl.ds(first, residual.shape[0])
        return residual + jnp.dot(o_s[rows, :].astype(BF16), wo[...], preferred_element_type=F32) + bo[...].astype(F32)[None, :]

    def gather_copy(g, owner, target, n):
        first, last = SCATTER_GROUPS[g]
        rows = ag.at[owner, pl.ds((first - SCATTER_FIRST) // 2 * UNIT, (last - first) // 2 * UNIT)]
        return pltpu.make_async_remote_copy(rows, rows, sa.at[g, n], ra.at[g, n], device_id=target, device_id_type=MESH)

    gathers = [(gather_copy(g, me, over, 0), gather_copy(g, me, beside, 1), gather_copy(g, over_i, beside, 2)) for g in range(len(SCATTER_GROUPS))]

    def project_scattered(g):
        first, last = SCATTER_GROUPS[g]
        residual = jnp.concatenate([x_f[pl.ds((n + x_side) * chunk + core * UNIT, UNIT), :] for n in range(first, last, 2)], axis=0)
        start = (first - SCATTER_FIRST) // 2 * UNIT
        ag[me, start:start + residual.shape[0], :] = project(SCATTER_FIRST * UNIT + start, residual)
        gathers[g][0].start()
        gathers[g][1].start()

    def forward(g):
        gathers[g][0].wait_recv()
        gathers[g][2].start()

    def collect_scattered(g):
        gathers[g][1].wait_recv()
        gathers[g][2].wait_recv()
        for j in range(*SCATTER_GROUPS[g]):
            i = (j - SCATTER_FIRST) // 2
            rows = [ag[2 * (j % 2) + c, i * UNIT:(i + 1) * UNIT, :] for c in range(2)]
            x_new[j * chunk:(j + 1) * chunk, :] = jnp.concatenate(rows, axis=0).astype(BF16)

    def beside_copy(g):
        first, last = WHOLE_GROUPS[g]
        rows = agd.at[core, pl.ds(whole_block(first) * UNIT, (last - first) * UNIT)]
        return pltpu.make_async_remote_copy(rows, rows, sd.at[g], rd.at[g], device_id=beside, device_id_type=MESH)

    def project_whole(g):
        first, last = WHOLE_GROUPS[g]
        residual = jnp.concatenate([x_f[pl.ds(j * chunk + core * UNIT, UNIT), :] for j in range(first, last)], axis=0)
        agd[core, whole_block(first) * UNIT:whole_block(last - 1) * UNIT + UNIT, :] = project(final_block(first) * UNIT, residual)
        beside_copy(g).start()

    def collect_whole(g):
        beside_copy(g).wait_recv()
        for j in range(*WHOLE_GROUPS[g]):
            rows = [agd[c, whole_block(j) * UNIT:(whole_block(j) + 1) * UNIT, :] for c in range(2)]
            x_new[j * chunk:(j + 1) * chunk, :] = jnp.concatenate(rows, axis=0).astype(BF16)

    def step(piece, block, carry):
        j = 2 * block
        for n in range(2):
            for copy in cache_copy(j + n, piece):
                copy.wait()
        attend(j, piece)
        for n in range(2):
            first_copy(j + n).start()

        @pl.when(j >= FIRST_LAG)
        def _():
            first_merge(j - FIRST_LAG)

        for ahead in range(PIECES):
            @pl.when((j + AHEAD < chunks) & ((j + AHEAD) // span == ahead))
            def _():
                for n in range(2):
                    for copy in cache_copy(j + AHEAD + n, ahead):
                        copy.start()

        return carry

    for piece in range(PIECES):
        lax.fori_loop(piece * span // 2, (piece + 1) * span // 2, functools.partial(step, piece), 0)
    for small in smalls[8:]:
        small.wait()
    def second_merges(first, last):
        for j in range(first, last, 2):
            second_merge(j)

    def drain(j, carry):
        first_copy(j).wait_send()

        @pl.when((j < SCATTER_FIRST) | (j >= SCATTER_LAST) | (j % 2 != x_side))
        def _():
            second_copy(j).wait_send()
        return carry

    second_merges(*SCATTER_GROUPS[0])
    project_scattered(0)
    for j in range(chunks - FIRST_LAG, chunks, 2):
        first_merge(j)
    second_merges(*WHOLE_GROUPS[0])
    project_whole(0)
    second_merges(*SCATTER_GROUPS[1])
    project_scattered(1)
    forward(0)
    collect_whole(0)
    second_merges(*WHOLE_GROUPS[1])
    project_whole(1)
    collect_scattered(0)
    lax.fori_loop(0, chunks, drain, 0)
    second_merges(*WHOLE_GROUPS[2])
    project_whole(2)
    forward(1)
    collect_whole(1)
    collect_scattered(1)
    collect_whole(2)
    for group in gathers:
        for gather in group:
            gather.wait_send()
    for g in range(len(WHOLE_GROUPS)):
        beside_copy(g).wait_send()


def write_kernel(window, pos, k_new, v_new, x_new, sp_new, *rest):
    k_vm, v_vm = rest[:PIECES], rest[PIECES:2 * PIECES]
    x_out, k_out, v_out, sp_out, k_ring, v_ring, sems, k_sem, v_sem = rest[2 * PIECES:]
    me = lax.axis_index('kv')
    part, slots, _ = k_vm[0].shape
    batch = part * PIECES
    depth, chunk = k_ring.shape[:2]
    chunks = batch // chunk
    span = chunks // PIECES
    others = (pltpu.make_async_copy(x_new, x_out, sems.at[0]), pltpu.make_async_copy(sp_new, sp_out, sems.at[1]))
    for copy in others:
        copy.start()
    tile_row = lax.broadcasted_iota(jnp.int32, (16, HEAD_DIM), 0)

    def copies(j):
        rows, ring = pl.ds(j * chunk, chunk), lax.rem(j, depth)
        return (pltpu.make_async_copy(k_ring.at[ring], k_out.at[rows], k_sem.at[ring]),
                pltpu.make_async_copy(v_ring.at[ring], v_out.at[rows], v_sem.at[ring]))

    def step(piece, j, carry):
        ring = lax.rem(j, depth)

        @pl.when(j >= depth)
        def _():
            for copy in copies(j - depth):
                copy.wait()

        for n, (new, cache, out) in enumerate(((k_new, k_vm[piece], k_ring), (v_new, v_vm[piece], v_ring))):
            def group(i, carry):
                for m in range(8):
                    row = i * 8 + m
                    b = j * chunk + row
                    slot = (pos[b] & (window - 1)) - me * slots
                    base = pl.multiple_of((jnp.clip(slot, 0, slots - 1) // 16) * 16, 16)
                    out[ring, row] = cache[b - piece * part]
                    fresh = jnp.broadcast_to(new[pl.ds(b, 1), :], (16, HEAD_DIM))
                    old = cache[b - piece * part, pl.ds(base, 16), :].astype(F32)
                    out[ring, row, pl.ds(base, 16), :] = jnp.where(tile_row == slot - base, fresh, old).astype(BF16)
                return carry
            lax.fori_loop(0, chunk // 8, group, 0)
            copies(j)[n].start()
        return carry

    for piece in range(PIECES):
        lax.fori_loop(piece * span, (piece + 1) * span, functools.partial(step, piece), 0)
    for j in range(chunks - depth, chunks):
        for copy in copies(j):
            copy.wait()
    for copy in others:
        copy.wait()


def solution(mesh):
    kv_size = mesh.shape['kv']
    row_spec = P('dp', None)
    cache_spec = P('dp', 'kv', None)
    slot_spec = P('dp', 'kv')
    vec_spec = P(None)
    mat_spec = P(None, None)
    half_dims = ROPE_DIM // 2
    freq_row = np.tile(ROPE_BASE ** (-np.arange(half_dims) / half_dims), 2).astype(np.float32)[None, :]

    def local_step(x_in, positions, k_cache, v_cache, slot_pos, norm_scale, w_q, w_k, w_v, w_o, b_o):
        batch, model = x_in.shape
        slots = k_cache.shape[1]
        window = slots * kv_size
        width = w_q.shape[1]
        chunks = batch // (UNIT * CHUNK_UNITS)
        scattered = (SCATTER_LAST - SCATTER_FIRST) // 2
        hbm = pl.BlockSpec(memory_space=pltpu.HBM)
        vmem = pl.BlockSpec(memory_space=pltpu.VMEM)
        smem = pl.BlockSpec(memory_space=pltpu.SMEM)
        dma = pltpu.SemaphoreType.DMA
        per_chunk = [dma((chunks,))] * 4
        *held, x_new, k_new, v_new, sp_new = pl.pallas_call(
            functools.partial(attend_kernel, window),
            out_shape=(*([pltpu.VMEM((batch // PIECES, slots, HEAD_DIM), BF16)] * (2 * PIECES)), pltpu.VMEM((batch, model), BF16),
                       pltpu.VMEM((batch, HEAD_DIM), F32), pltpu.VMEM((batch, HEAD_DIM), F32), pltpu.VMEM((batch, slots), jnp.int32)),
            in_specs=[hbm] * 12,
            out_specs=(vmem,) * (2 * PIECES + 4),
            scratch_shapes=[
                pltpu.VMEM((batch // 128, 128), jnp.int32), pltpu.VMEM((1, 128), F32), pltpu.VMEM((batch, model), BF16), pltpu.VMEM((model,), BF16),
                pltpu.VMEM((model, HEAD_DIM), BF16), pltpu.VMEM((model, HEAD_DIM), BF16), pltpu.VMEM((model, width), BF16),
                pltpu.VMEM((batch, slots), jnp.int32), pltpu.VMEM((width, model), BF16), pltpu.VMEM((model,), BF16),
                pltpu.VMEM((batch, 128), F32), pltpu.VMEM((batch, model), F32), pltpu.VMEM((batch // UNIT, HEADS, UNIT, HEAD_DIM), F32),
                pltpu.VMEM((chunks, CHUNK_UNITS, PACKET, 128), F32), pltpu.VMEM((chunks, PACKET, 128), F32), pltpu.VMEM((chunks, 2, PACKET, 128), F32),
                pltpu.VMEM(((chunks - scattered) * UNIT, width), F32), pltpu.VMEM((kv_size, scattered * UNIT, model), F32),
                pltpu.VMEM((2, (chunks - 2 * scattered) * UNIT, model), F32),
                dma((10,)), dma((chunks,)), dma((chunks,)), *per_chunk, *([dma((len(SCATTER_GROUPS), 3))] * 2), *([dma((len(WHOLE_GROUPS),))] * 2)],
            compiler_params=pltpu.CompilerParams(vmem_limit_bytes=16 << 20, collective_id=0, has_side_effects=True),
            name='attend',
        )(*[pltpu.with_memory_space_constraint(a, pltpu.HBM) for a in (
            positions.reshape(batch // 128, 128), jnp.asarray(freq_row), x_in, norm_scale, w_k, w_v, w_q, slot_pos,
            w_o, b_o, k_cache, v_cache)])
        x_out, k_out, v_out, slot_pos_out = pl.pallas_call(
            functools.partial(write_kernel, window),
            out_shape=(jax.ShapeDtypeStruct((batch, model), BF16), jax.ShapeDtypeStruct(k_cache.shape, BF16),
                       jax.ShapeDtypeStruct(v_cache.shape, BF16), jax.ShapeDtypeStruct((batch, slots), jnp.int32)),
            in_specs=[smem] + [vmem] * (2 * PIECES + 4),
            out_specs=(hbm,) * 4,
            scratch_shapes=[pltpu.VMEM((4, 16, slots, HEAD_DIM), BF16), pltpu.VMEM((4, 16, slots, HEAD_DIM), BF16), dma((2,)), dma((4,)), dma((4,))],
            compiler_params=pltpu.CompilerParams(vmem_limit_bytes=9 << 20),
            name='write',
        )(positions, k_new, v_new, x_new, sp_new, *held)
        return x_out, k_out, v_out, slot_pos_out

    return jax.shard_map(
        local_step,
        mesh=mesh,
        in_specs=(row_spec, P('dp'), cache_spec, cache_spec, slot_spec, vec_spec, mat_spec, mat_spec, mat_spec, mat_spec, vec_spec),
        out_specs=(row_spec, cache_spec, cache_spec, slot_spec),
        check_vma=False)
```
